512 devices in a mesh: gx: 16 (over y, core), gy: 8 (over z), gz: 4 (over x).
Axes of the slice: x: 4, y: 8, z: 8, core: 2. Of those that a mesh axis runs over, the one named last changes fastest.
Arguments:
- charges: float32 [256, 256, 512], P('gx', 'gy', 'gz'), may hold values from -6 to 6
- term_width: float32 [2, 4], replicated, may hold values from 0.8 to 3.5
- term_weight: float32 [2, 4], replicated, may hold values from 0.5 to 2
Outputs:
- potential: float32 [256, 256, 512], P('gx', 'gy', 'gz')
The draws below stay inside these ranges and needn't reach their ends.
All inputs are finite; a program needn't handle non-finite values.
Results may differ from the reference program's by a relative error of at most 0.00025.
Values sent between devices are 32-bit elements; how exact they have to be, the bound alone decides.
No kernel may reach another device: no remote copies, remote signals or barrier semaphores. Data moves between devices by JAX's collectives and lax.ppermute only.
A program may use at most 64 MiB of HBM per device.

```python
import math
import jax
import jax.numpy as jnp
from jax import lax

TERMS = 4
RADIUS = 8
NX = 256
NY = 256
NZ = 512


def draw_charges(key, part):
    return jnp.clip(jax.random.normal(key, (NX, NY, NZ), jnp.float32), -6.0, 6.0)


def setup_inputs(seed: int = 0) -> dict:
    seeds = jax.random.split(jax.random.key(seed), 4)
    charges = draw_charges(jax.random.fold_in(seeds[3], 71), 0)
    term_width = jnp.clip(jnp.exp(jax.random.uniform(seeds[1], (2, TERMS), jnp.float32, math.log(0.8), math.log(3.5))), 0.8, 3.5)
    term_weight = jnp.clip(jax.random.uniform(seeds[2], (2, TERMS), jnp.float32, 0.5, 2.0), 0.5, 2.0)
    return {"charges": charges, "term_width": term_width, "term_weight": term_weight}


screening = 0.01
strength = 4.0


def gaussian_taps(widths):
    offsets = jnp.arange(-RADIUS, RADIUS + 1).astype(widths.dtype)
    values = jnp.exp(-(offsets[None, :] ** 2) / (2.0 * widths[:, None] ** 2))
    return values / jnp.sum(values, axis=1, keepdims=True)


def convolve(padded, taps, axis, length):
    total = taps[0] * lax.slice_in_dim(padded, 0, length, axis=axis)
    for offset in range(1, 2 * RADIUS + 1):
        total = total + taps[offset] * lax.slice_in_dim(padded, offset, offset + length, axis=axis)
    return total


def smooth_level(field, widths, weights):
    taps = gaussian_taps(widths)
    padded = jnp.pad(field, RADIUS, mode="wrap")
    shape = field.shape
    result = None
    for term_index in range(TERMS):
        first_pass = convolve(padded, taps[term_index], 0, shape[0])
        second_pass = convolve(first_pass, taps[term_index], 1, shape[1])
        third_pass = convolve(second_pass, taps[term_index], 2, shape[2])
        contrib = weights[term_index] * third_pass
        result = contrib if result is None else result + contrib
    return result


def restrict(field):
    shape = field.shape
    return field.reshape(shape[0] // 2, 2, shape[1] // 2, 2, shape[2] // 2, 2).mean(axis=(1, 3, 5))


def expand(field):
    return jnp.repeat(jnp.repeat(jnp.repeat(field, 2, axis=0), 2, axis=1), 2, axis=2)


def axis_lam(count, dtype):
    modes = jnp.arange(count).astype(dtype)
    return 2.0 - 2.0 * jnp.cos((2.0 * math.pi / count) * modes)


def solve_top(coarse):
    shape = coarse.shape
    lam = axis_lam(shape[0], coarse.dtype)[:, None, None] + axis_lam(shape[1], coarse.dtype)[None, :, None] + axis_lam(shape[2], coarse.dtype)[None, None, :]
    zeroed = lam <= 0.0
    mult = jnp.where(zeroed, 0.0, strength * jnp.exp(-lam) / (lam + screening))
    spectrum = jnp.fft.fftn(coarse) * mult
    return jnp.real(jnp.fft.ifftn(spectrum)).astype(coarse.dtype)


def reference(charges, term_width, term_weight):
    middle = restrict(charges)
    coarse = restrict(middle)
    near = smooth_level(charges, term_width[0], term_weight[0])
    between = smooth_level(middle, term_width[1], term_weight[1])
    distant = solve_top(coarse)
    return near + expand(between + expand(distant))
```

```python
import math

import jax
import jax.numpy as jnp
import numpy as np
from jax import lax
from jax.experimental import pallas as pl
from jax.experimental.pallas import tpu as pltpu
from jax.sharding import PartitionSpec as P

TERMS = 4
RADIUS = 8
TAPS = RADIUS + 1

HIGHEST = lax.Precision.HIGHEST
F32 = jnp.float32
BF16 = jnp.bfloat16
screening = 0.01
strength = 4.0

BX, BY, BZ = 16, 32, 128
MX, MY, MZ = 8, 16, 64
CX, CY, CZ = 64, 64, 128
EY, EMY = BY + 2 * RADIUS, MY + 2 * RADIUS
GX, GY, GZ = 16, 8, 4
YROWS = BX * 8 + 2 * 8 + 5 * 8
XROWS = 8 * EY + EY + 5 * EMY


def cas_table(count):
    modes = np.arange(count)
    angles = 2.0 * math.pi / count * (np.outer(modes, modes) % count)
    return np.cos(angles) + np.sin(angles)


def constant_tables():
    cas_y, cas_z = cas_table(CY), cas_table(CZ)

    def lam(count):
        return 2.0 - 2.0 * np.cos(2.0 * math.pi / count * np.arange(count))

    total = lam(CX)[:, None, None] + lam(CY)[None, :, None] + lam(CZ)[None, None, :]
    mult = strength * np.exp(-total) / (total + screening)
    mult[0, 0, 0] = 0.0
    shifts = np.arange(CX // 2 + 1)
    cosine = np.cos(2.0 * math.pi / CX * (np.outer(shifts, np.arange(CX)) % CX))
    along_x = np.einsum("dm,myz->dyz", cosine, mult) / (CX * CY * CZ)
    own_z = np.stack([np.tile(cas_z[:, 32 * g : 32 * g + 32], (1, 4)) for g in range(GZ)])
    fine = np.arange(BZ)
    pairs = np.zeros((BZ, BZ))
    pairs[fine, fine // 2] = 1.0 / 8.0
    pairs[fine, 64 + fine // 4] = 1.0 / 64.0
    spread = np.zeros((BZ, 4 * BZ))
    for block in range(4):
        spread[block * 32 + fine // 4, block * BZ + fine] = 1.0
    rows = np.zeros((MY, 8))
    rows[np.arange(MY), np.arange(MY) // 2] = 1.0
    return [np.asarray(t, np.float32) for t in (cas_y, cas_z, along_x, own_z, pairs, spread, rows)]


def lanes(shape):
    return lax.broadcasted_iota(jnp.int32, shape, len(shape) - 1)


def roll(value, shift):
    shift %= 128
    return pltpu.roll(value, shift, 1) if shift else value


def dot(a, b):
    return jnp.dot(a, b, preferred_element_type=F32)


def exact(a, b):
    return jnp.dot(a, b, preferred_element_type=F32, precision=HIGHEST)


def halves(value):
    high = value.astype(BF16)
    return high, (value - high.astype(F32)).astype(BF16)


def weights_kernel(width_ref, weight_ref, gy_ref, gzh_ref, gzl_ref, my_ref, mzh_ref, mzl_ref, cx_ref):
    def scale(level, term):
        width = jnp.full((8, 128), width_ref[level, term], F32)
        inverse = 1.0 / (2.0 * width * width)
        offset = lanes((8, 128)) - RADIUS
        values = jnp.exp(-(offset * offset).astype(F32) * inverse)
        values = jnp.where(offset <= RADIUS, values, 0.0)
        norm = 1.0 / jnp.sum(values, axis=1, keepdims=True)
        return inverse[0:1, 0:1], norm[0:1, 0:1]

    def taps(offset, inverse, norm):
        values = jnp.exp(-(offset * offset).astype(F32) * inverse) * norm
        return jnp.where(jnp.abs(offset) <= RADIUS, values, 0.0)

    def along_y(ref, term, inverse, norm, out, ext):
        shape = (out, 3 * ext)
        column = lanes(shape)
        row = lax.broadcasted_iota(jnp.int32, shape, 0)
        part = (column >= ext).astype(jnp.int32) + (column >= 2 * ext).astype(jnp.int32)
        high, low = halves(taps(column - part * ext - RADIUS - row, inverse, norm))
        ref[term * out : (term + 1) * out, :] = jnp.where(part < 2, high.astype(F32), low.astype(F32)).astype(BF16)

    for term in range(TERMS):
        inverse, norm = scale(0, term)
        along_y(gy_ref, term, inverse, norm, BY, EY)
        shape = (256, 128)
        row = lax.broadcasted_iota(jnp.int32, shape, 0)
        slot = row & 15
        place = jnp.where(row < BZ, row, jnp.where(slot < 8, slot - 8, BZ - 8 + slot))
        high, low = halves(taps(place - lanes(shape), inverse, norm))
        gzh_ref[term] = high
        gzl_ref[term] = low
        for offset in range(TAPS):
            value = jnp.exp(-float(offset * offset) * inverse) * norm * weight_ref[0, term]
            cx_ref[term * TAPS + offset] = jnp.broadcast_to(value, (8, 128))

        inverse, norm = scale(1, term)
        along_y(my_ref, term, inverse, norm, MY, EMY)
        shape = (128, 128)
        row = lax.broadcasted_iota(jnp.int32, shape, 0)
        place = jnp.where(row < MZ, row, jnp.where(row < MZ + 8, row - MZ - 8, row - 8))
        values = taps(place - (lanes(shape) >> 1), inverse, norm)
        high, low = halves(jnp.where(row < MZ + 16, values, 0.0))
        mzh_ref[term] = high
        mzl_ref[term] = low
        for offset in range(TAPS):
            value = jnp.exp(-float(offset * offset) * inverse) * norm * weight_ref[1, term]
            cx_ref[(TERMS + term) * TAPS + offset] = jnp.broadcast_to(value, (8, 128))


def restrict_kernel(f_ref, pairs_ref, coarse_ref, mid_ref, zmsg_ref, half_ref):
    planes = []
    for x in range(MX):
        total = None
        for plane in (2 * x, 2 * x + 1):
            for odd in (0, 1):
                part = f_ref[plane, pl.ds(odd, MY, stride=2), :]
                total = part if total is None else total + part
        planes.append(total)
    half_ref[...] = exact(jnp.concatenate(planes, axis=0), pairs_ref[...])
    lane = lanes((8, 128))
    coarse = jnp.zeros((8, 128), F32)
    for x in range(4):
        part = None
        for row in (2 * x * MY, 2 * x * MY + 1, (2 * x + 1) * MY, (2 * x + 1) * MY + 1):
            piece = half_ref[pl.ds(row, 8, stride=2), :]
            part = piece if part is None else part + piece
        coarse = jnp.where((lane >> 5) == x, roll(part, x * 32 - 64), coarse)
    for target in range(GY * GZ):
        coarse_ref[target] = coarse

    me = lax.axis_index("gz")
    up, down = lax.rem(me + 1, GZ), lax.rem(me + GZ - 1, GZ)
    zmsg_ref[...] = jnp.zeros_like(zmsg_ref)
    slot = lanes((BY, 128)) >> 3
    for group in range(2):
        rising = jnp.zeros((BY, 128), F32)
        falling = jnp.zeros((BY, 128), F32)
        for x in range(8):
            plane = f_ref[group * 8 + x]
            rising = jnp.where(slot == 2 * x, roll(plane, x * 16 - 120), rising)
            falling = jnp.where(slot == 2 * x + 1, roll(plane, x * 16 + 8), falling)
        zmsg_ref[up, group * BY : (group + 1) * BY, :] = rising
        zmsg_ref[down, group * BY : (group + 1) * BY, :] = falling
    slot = lanes((MY, 128)) >> 3
    rising = jnp.zeros((MY, 128), F32)
    falling = jnp.zeros((MY, 128), F32)
    middle = []
    for x in range(MX):
        plane = half_ref[x * MY : (x + 1) * MY, :]
        middle.append(plane)
        rising = jnp.where(slot == 2 * x, roll(plane, x * 16 - 56), rising)
        falling = jnp.where(slot == 2 * x + 1, roll(plane, x * 16 + 8), falling)
    zmsg_ref[up, 2 * BY : 2 * BY + MY, :] = rising
    zmsg_ref[down, 2 * BY : 2 * BY + MY, :] = falling
    for x in range(4):
        mid_ref[x] = jnp.where(slot < 8, middle[x], roll(middle[x + 4], 64))


def modes_kernel(slab_ref, cas_y_ref, cas_z_ref, along_ref, own_z_ref, out_ref):
    rows = [jnp.concatenate([slab_ref[gy * GZ + gz] for gz in range(GZ)], axis=1) for gy in range(GY)]
    by_y = exact(cas_y_ref[...], jnp.concatenate(rows, axis=0))
    lane = lanes((CY, 128)) >> 5
    planes = []
    for x in range(4):
        plane = jnp.zeros((CY, 128), F32)
        for gz in range(GZ):
            plane = jnp.where(lane == gz, roll(by_y[:, gz * 128 : (gz + 1) * 128], (gz - x) * 32), plane)
        planes.append(plane)
    by_z = exact(jnp.concatenate(planes, axis=0), cas_z_ref[...])
    source = [by_z[x * CY : (x + 1) * CY, :] for x in range(4)]
    own_y = cas_y_ref[pl.ds(pl.multiple_of(lax.axis_index("gy") * 8, 8), 8), :]
    own_z = own_z_ref[lax.axis_index("gz")]
    me = lax.axis_index("gx")
    lane = lanes((8, 128)) >> 5
    for block in range(GX):
        outs = []
        for x in range(4):
            total = None
            for other in range(4):
                shift = (block * 4 + x - other) % CX
                part = along_ref[min(shift, CX - shift)] * source[other]
                total = part if total is None else total + part
            outs.append(total)
        back_y = exact(own_y, jnp.concatenate(outs, axis=1))
        back_z = exact(
            jnp.concatenate([back_y[:, x * 128 : (x + 1) * 128] for x in range(4)], axis=0), own_z
        )
        result = back_z[0:8]
        for x in range(1, 4):
            result = jnp.where(lane == x, back_z[x * 8 : (x + 1) * 8], result)
        out_ref[lax.rem(me + block, GX)] = result


def y_message_kernel(f_ref, mid_ref, zrecv_ref, halo_ref, up_ref, down_ref):
    me = lax.axis_index("gz")
    halo = zrecv_ref[lax.rem(me + GZ - 1, GZ)] + zrecv_ref[lax.rem(me + 1, GZ)]
    halo_ref[...] = halo
    for ref, fine, middle in ((up_ref, BY - 8, MY - 8), (down_ref, 0, 0)):
        for x in range(BX):
            ref[x * 8 : x * 8 + 8, :] = f_ref[x, fine : fine + 8, :]
        for group in range(2):
            ref[128 + group * 8 : 136 + group * 8, :] = halo[group * BY + fine : group * BY + fine + 8]
        for x in range(4):
            ref[144 + x * 8 : 152 + x * 8, :] = mid_ref[x, middle : middle + 8, :]
        ref[176:184, :] = halo[2 * BY + middle : 2 * BY + middle + 8]


def own_extended(f_ref, mid_ref, halo_ref, low_ref, high_ref):
    def joined(row, inner):
        return jnp.concatenate([low_ref[row : row + 8, :], inner, high_ref[row : row + 8, :]], axis=0)

    planes = [lambda x=x: joined(x * 8, f_ref[x]) for x in range(BX)]
    sides = [lambda g=g: joined(128 + g * 8, halo_ref[g * BY : (g + 1) * BY, :]) for g in range(2)]
    middle = [lambda x=x: joined(144 + x * 8, mid_ref[x]) for x in range(4)]
    edge = lambda: joined(176, halo_ref[2 * BY : 2 * BY + MY, :])
    return planes, sides, middle, edge


def x_message_kernel(f_ref, mid_ref, halo_ref, low_ref, high_ref, up_ref, down_ref):
    planes, sides, middle, edge = own_extended(f_ref, mid_ref, halo_ref, low_ref, high_ref)
    for ref, first, group in ((up_ref, 8, 1), (down_ref, 0, 0)):
        for x in range(8):
            ref[x * EY : (x + 1) * EY, :] = planes[first + x]()
        ref[8 * EY : 9 * EY, :] = sides[group]()
        for x in range(4):
            ref[9 * EY + x * EMY : 9 * EY + (x + 1) * EMY, :] = middle[x]()
        ref[9 * EY + 4 * EMY : 9 * EY + 5 * EMY, :] = edge()


def filter_yz(planes, sides, gy, gzh_ref, gzl_ref, out_ref, places):
    for group in range(2):
        data = jnp.concatenate([planes[group * 8 + x]() for x in range(8)] + [sides[group]()], axis=1)
        high, low = halves(data)
        by_y = dot(gy, jnp.concatenate([high, low, high], axis=0))
        slot = lanes((BY, 128)) >> 4
        for term in range(TERMS):
            rows = by_y[term * BY : (term + 1) * BY, :]
            side = rows[:, 8 * 128 :]
            left = jnp.concatenate([rows[:, x * 128 : (x + 1) * 128] for x in range(8)], axis=0)
            right = jnp.concatenate([jnp.where(slot == x, side, 0.0) for x in range(8)], axis=0)
            high, low = halves(jnp.concatenate([left, right], axis=1))
            gzh = gzh_ref[term]
            result = dot(high, gzh) + dot(low, gzh) + dot(high, gzl_ref[term])
            for x in range(8):
                out_ref[term, places[group * 8 + x]] = result[x * BY : (x + 1) * BY]


def filter_middle(middle, edge, my, mzh_ref, mzl_ref, out_ref, place):
    slot = lanes((EMY, 128)) >> 3
    rim = edge()
    planes = []
    for x in range(MX):
        plane = middle[x]() if x < 4 else roll(middle[x - 4](), 64)
        rolled = roll(rim, 64 - 16 * x)
        planes.append(jnp.where(slot < 8, plane, jnp.where(slot < 10, rolled, 0.0)))
    high, low = halves(jnp.concatenate(planes, axis=1))
    by_y = dot(my, jnp.concatenate([high, low, high], axis=0))
    for term in range(TERMS):
        rows = by_y[term * MY : (term + 1) * MY, :]
        left = jnp.concatenate([rows[:, x * 128 : (x + 1) * 128] for x in range(MX)], axis=0)
        high, low = halves(left)
        mzh = mzh_ref[term]
        result = dot(high, mzh) + dot(low, mzh) + dot(high, mzl_ref[term])
        for x in range(MX):
            out_ref[term, place + x] = result[x * MY : (x + 1) * MY]


def own_kernel(
    f_ref, mid_ref, halo_ref, low_ref, high_ref, gy_ref, gzh_ref, gzl_ref, my_ref, mzh_ref, mzl_ref, fine_ref, middle_ref
):
    planes, sides, middle, edge = own_extended(f_ref, mid_ref, halo_ref, low_ref, high_ref)
    filter_yz(planes, sides, gy_ref[...], gzh_ref, gzl_ref, fine_ref, list(range(BX)))
    filter_middle(middle, edge, my_ref[...], mzh_ref, mzl_ref, middle_ref, 0)


def final_kernel(
    low_ref, high_ref, fine_ref, middle_ref, top_ref, gy_ref, gzh_ref, gzl_ref, my_ref, mzh_ref, mzl_ref, cx_ref,
    spread_ref, rows_ref, out_ref, ring_ref, small_ref, add_ref,
):
    planes, sides = [], []
    for ref in (low_ref, high_ref):
        planes += [lambda ref=ref, x=x: ref[x * EY : (x + 1) * EY, :] for x in range(8)]
        sides.append(lambda ref=ref: ref[8 * EY : 9 * EY, :])
    filter_yz(planes, sides, gy_ref[...], gzh_ref, gzl_ref, ring_ref, list(range(16)))
    for index, ref in enumerate((low_ref, high_ref)):
        middle = [lambda ref=ref, x=x: ref[9 * EY + x * EMY : 9 * EY + (x + 1) * EMY, :] for x in range(4)]
        edge = lambda ref=ref: ref[9 * EY + 4 * EMY : 9 * EY + 5 * EMY, :]
        filter_middle(middle, edge, my_ref[...], mzh_ref, mzl_ref, small_ref, index * MX)

    top = top_ref[0]
    for source in range(1, GX):
        top = top + top_ref[source]
    top = exact(exact(rows_ref[...], top), spread_ref[...])

    for tile in range(MY // 8):
        sl = slice(tile * 8, tile * 8 + 8)
        acc = [top[sl, (x // 2) * 128 : (x // 2 + 1) * 128] for x in range(MX)]
        for term in range(TERMS):
            for place in range(3 * MX):
                if place < MX:
                    value = small_ref[term, place, sl, :]
                elif place < 2 * MX:
                    value = middle_ref[term, place - MX, sl, :]
                else:
                    value = small_ref[term, place - MX, sl, :]
                for x in range(MX):
                    offset = place - x - RADIUS
                    if abs(offset) <= RADIUS:
                        acc[x] = acc[x] + cx_ref[(TERMS + term) * TAPS + abs(offset)] * value
        for x in range(MX):
            add_ref[x, pl.ds(tile * 16, 8, stride=2), :] = acc[x]
            add_ref[x, pl.ds(tile * 16 + 1, 8, stride=2), :] = acc[x]

    def tile_step(tile, carry):
        sl = pl.ds(pl.multiple_of(tile * 8, 8), 8)
        acc = [add_ref[x // 2, sl, :] for x in range(BX)]
        for term in range(TERMS):
            for place in range(2 * BX):
                if place < 8:
                    value = ring_ref[term, place, sl, :]
                elif place < 24:
                    value = fine_ref[term, place - 8, sl, :]
                else:
                    value = ring_ref[term, place - 16, sl, :]
                for x in range(BX):
                    offset = place - x - RADIUS
                    if abs(offset) <= RADIUS:
                        acc[x] = acc[x] + cx_ref[term * TAPS + abs(offset)] * value
        for x in range(BX):
            out_ref[x, sl, :] = acc[x]
        return carry

    lax.fori_loop(0, BY // 8, tile_step, 0)


def call(kernel, outs, args, scratch=(), flops=0, smem=0):
    vmem = pl.BlockSpec(memory_space=pltpu.VMEM)
    specs = [pl.BlockSpec(memory_space=pltpu.SMEM)] * smem + [vmem] * (len(args) - smem)
    size = sum(a.size * a.dtype.itemsize for a in args)
    return pl.pallas_call(
        kernel,
        out_shape=[jax.ShapeDtypeStruct(shape, dtype) for shape, dtype in outs],
        in_specs=specs,
        out_specs=[vmem] * len(outs),
        scratch_shapes=list(scratch),
        cost_estimate=pl.CostEstimate(flops=flops, bytes_accessed=size, transcendentals=0),
        compiler_params=pltpu.CompilerParams(vmem_limit_bytes=32 * 1024 * 1024),
    )(*args)


def ring(value, axis, step):
    count = lax.axis_size(axis)
    return lax.ppermute(value, axis, [(i, (i + step) % count) for i in range(count)])


def shards(charges, term_width, term_weight):
    cas_y, cas_z, along_x, own_z, pairs, spread, rows = [jnp.asarray(t) for t in constant_tables()]
    coarse, mid, zmsg = call(
        restrict_kernel,
        [((GY * GZ, 8, 128), F32), ((4, MY, 128), F32), ((GZ, 2 * BY + MY, 128), F32)],
        [charges, pairs],
        [pltpu.VMEM((MX * MY, 128), F32)],
        flops=10**7,
    )
    slab = lax.all_to_all(coarse, ("gy", "gz"), 0, 0, tiled=True)
    zrecv = lax.all_to_all(zmsg, "gz", 0, 0, tiled=True)
    gy, gzh, gzl, my, mzh, mzl, cx = call(
        weights_kernel,
        [
            ((TERMS * BY, 3 * EY), BF16),
            ((TERMS, 256, 128), BF16),
            ((TERMS, 256, 128), BF16),
            ((TERMS * MY, 3 * EMY), BF16),
            ((TERMS, 128, 128), BF16),
            ((TERMS, 128, 128), BF16),
            ((2 * TERMS * TAPS, 8, 128), F32),
        ],
        [term_width, term_weight],
        flops=10**7,
        smem=2,
    )
    (partial,) = call(
        modes_kernel, [((GX, 8, 128), F32)], [slab, cas_y, cas_z, along_x, own_z], flops=5 * 10**7
    )
    top = lax.all_to_all(partial, "gx", 0, 0, tiled=True)
    halo, y_up, y_down = call(
        y_message_kernel,
        [((2 * BY + MY, 128), F32), ((YROWS, 128), F32), ((YROWS, 128), F32)],
        [charges, mid, zrecv],
        flops=10**6,
    )
    low, high = ring(y_up, "gy", 1), ring(y_down, "gy", -1)
    x_up, x_down = call(
        x_message_kernel,
        [((XROWS, 128), F32), ((XROWS, 128), F32)],
        [charges, mid, halo, low, high],
        flops=10**6,
    )
    x_low, x_high = ring(x_up, "gx", 1), ring(x_down, "gx", -1)
    fine, middle = call(
        own_kernel,
        [((TERMS, BX, BY, 128), F32), ((TERMS, MX, MY, 128), F32)],
        [charges, mid, halo, low, high, gy, gzh, gzl, my, mzh, mzl],
        flops=10**8,
    )
    (result,) = call(
        final_kernel,
        [((BX, BY, BZ), F32)],
        [x_low, x_high, fine, middle, top, gy, gzh, gzl, my, mzh, mzl, cx, spread, rows],
        [
            pltpu.VMEM((TERMS, 16, BY, 128), F32),
            pltpu.VMEM((TERMS, 16, MY, 128), F32),
            pltpu.VMEM((MX, BY, 128), F32),
        ],
        flops=10**8,
    )
    return result


def solution(mesh):
    placed = (P("gx", "gy", "gz"), P(), P())
    return jax.shard_map(
        shards, mesh=mesh, in_specs=placed, out_specs=P("gx", "gy", "gz"), check_vma=False
    )
```

```python
import math

import jax
import jax.numpy as jnp
import numpy as np
from jax import lax
from jax.experimental import pallas as pl
from jax.experimental.pallas import tpu as pltpu
from jax.sharding import PartitionSpec as P


TERMS = 4
RADIUS = 8
TAPS = RADIUS + 1

HIGHEST = lax.Precision.HIGHEST
F32 = jnp.float32
BF16 = jnp.bfloat16
screening = 0.01
strength = 4.0

BX, BY, BZ = 16, 32, 128
MX, MY, MZ = 8, 16, 64
CX, CY, CZ = 64, 64, 128
EY, EMY = BY + 2 * RADIUS, MY + 2 * RADIUS
GX, GY, GZ = 16, 8, 4
FETCHED = 7
ZROWS = 2 * BY + MY
YROWS = BX * 8 + 2 * 8 + 5 * 8
XROWS = 8 * EY + EY + 5 * EMY


def cas_table(count):
    modes = np.arange(count)
    angles = 2.0 * math.pi / count * (np.outer(modes, modes) % count)
    return np.cos(angles) + np.sin(angles)


def constant_tables():
    cas_y, cas_z = cas_table(CY), cas_table(CZ)

    def lam(count):
        return 2.0 - 2.0 * np.cos(2.0 * math.pi / count * np.arange(count))

    total = lam(CX)[:, None, None] + lam(CY)[None, :, None] + lam(CZ)[None, None, :]
    mult = strength * np.exp(-total) / (total + screening)
    mult[0, 0, 0] = 0.0
    shifts = np.arange(CX // 2 + 1)
    cosine = np.cos(2.0 * math.pi / CX * (np.outer(shifts, np.arange(CX)) % CX))
    along_x = np.einsum("dm,myz->dyz", cosine, mult) / (CX * CY * CZ)
    own_z = np.stack([np.tile(cas_z[:, 32 * g : 32 * g + 32], (1, 4)) for g in range(GZ)])
    return [np.asarray(t, np.float32) for t in (cas_y, cas_z, along_x, own_z)]


def lanes(shape):
    return lax.broadcasted_iota(jnp.int32, shape, len(shape) - 1)


def roll(value, shift):
    shift %= 128
    return pltpu.roll(value, shift, 1) if shift else value


def dot(a, b):
    return jnp.dot(a, b, preferred_element_type=F32)


def exact(a, b):
    return jnp.dot(a, b, preferred_element_type=F32, precision=HIGHEST)


def halves(value):
    high = value.astype(BF16)
    return high, (value - high.astype(F32)).astype(BF16)


def weights_kernel(width_ref, weight_ref, gy_ref, gzh_ref, gzl_ref, my_ref, mzh_ref, mzl_ref, cx_ref):
    def scale(level, term):
        width = jnp.broadcast_to(width_ref[level : level + 1, term : term + 1], (8, 128))
        inverse = 1.0 / (2.0 * width * width)
        offset = lanes((8, 128)) - RADIUS
        values = jnp.exp(-(offset * offset).astype(F32) * inverse)
        values = jnp.where(offset <= RADIUS, values, 0.0)
        norm = 1.0 / jnp.sum(values, axis=1, keepdims=True)
        return inverse[0:1, 0:1], norm[0:1, 0:1]

    def taps(offset, inverse, norm):
        values = jnp.exp(-(offset * offset).astype(F32) * inverse) * norm
        return jnp.where(jnp.abs(offset) <= RADIUS, values, 0.0)

    def along_y(ref, term, inverse, norm, out, ext):
        shape = (out, 3 * ext)
        column = lanes(shape)
        row = lax.broadcasted_iota(jnp.int32, shape, 0)
        part = (column >= ext).astype(jnp.int32) + (column >= 2 * ext).astype(jnp.int32)
        high, low = halves(taps(column - part * ext - RADIUS - row, inverse, norm))
        ref[term * out : (term + 1) * out, :] = jnp.where(part < 2, high.astype(F32), low.astype(F32)).astype(BF16)

    for term in range(TERMS):
        inverse, norm = scale(0, term)
        along_y(gy_ref, term, inverse, norm, BY, EY)
        shape = (256, 128)
        row = lax.broadcasted_iota(jnp.int32, shape, 0)
        slot = row & 15
        place = jnp.where(row < BZ, row, jnp.where(slot < 8, slot - 8, BZ - 8 + slot))
        high, low = halves(taps(place - lanes(shape), inverse, norm))
        gzh_ref[term] = high
        gzl_ref[term] = low
        for offset in range(TAPS):
            value = jnp.exp(-float(offset * offset) * inverse) * norm * weight_ref[0:1, term : term + 1]
            cx_ref[term * TAPS + offset] = jnp.broadcast_to(value, (8, 128))

        inverse, norm = scale(1, term)
        along_y(my_ref, term, inverse, norm, MY, EMY)
        shape = (128, 128)
        row = lax.broadcasted_iota(jnp.int32, shape, 0)
        place = jnp.where(row < MZ, row, jnp.where(row < MZ + 8, row - MZ - 8, row - 8))
        values = taps(place - (lanes(shape) >> 1), inverse, norm)
        high, low = halves(jnp.where(row < MZ + 16, values, 0.0))
        mzh_ref[term] = high
        mzl_ref[term] = low
        for offset in range(TAPS):
            value = jnp.exp(-float(offset * offset) * inverse) * norm * weight_ref[1:2, term : term + 1]
            cx_ref[(TERMS + term) * TAPS + offset] = jnp.broadcast_to(value, (8, 128))


def restrict_kernel(*refs):
    sources, (coarse_ref, mid_ref, up_ref, down_ref), copies = refs[:FETCHED], refs[FETCHED : FETCHED + 4], refs[FETCHED + 4 :]
    copies, half_ref, sems = copies[:FETCHED], copies[FETCHED], copies[FETCHED + 1]
    fetches = [pltpu.make_async_copy(a, b, sems.at[i]) for i, (a, b) in enumerate(zip(sources, copies))]
    for fetch in fetches:
        fetch.start()
    f_ref = copies[0]
    fetches[0].wait()
    planes = []
    for x in range(MX):
        total = None
        for plane in (2 * x, 2 * x + 1):
            for odd in (0, 1):
                part = f_ref[plane, pl.ds(odd, MY, stride=2), :]
                total = part if total is None else total + part
        planes.append(total)
    row, column = lax.broadcasted_iota(jnp.int32, (BZ, 128), 0), lanes((BZ, 128))
    pairs = jnp.where((row >> 1) == column, 1.0 / 8.0, jnp.where((row >> 2) == column - 64, 1.0 / 64.0, 0.0))
    half_ref[...] = exact(jnp.concatenate(planes, axis=0), pairs)
    lane = lanes((8, 128))
    coarse = jnp.zeros((8, 128), F32)
    for x in range(4):
        part = None
        for row in (2 * x * MY, 2 * x * MY + 1, (2 * x + 1) * MY, (2 * x + 1) * MY + 1):
            piece = half_ref[pl.ds(row, 8, stride=2), :]
            part = piece if part is None else part + piece
        coarse = jnp.where((lane >> 5) == x, roll(part, x * 32 - 64), coarse)
    for target in range(GY * GZ):
        coarse_ref[target] = coarse

    slot = lanes((BY, 128)) >> 3
    for group in range(2):
        rising = jnp.zeros((BY, 128), F32)
        falling = jnp.zeros((BY, 128), F32)
        for x in range(8):
            plane = f_ref[group * 8 + x]
            rising = jnp.where(slot == 2 * x, roll(plane, x * 16 - 120), rising)
            falling = jnp.where(slot == 2 * x + 1, roll(plane, x * 16 + 8), falling)
        up_ref[group * BY : (group + 1) * BY, :] = rising
        down_ref[group * BY : (group + 1) * BY, :] = falling
    slot = lanes((MY, 128)) >> 3
    rising = jnp.zeros((MY, 128), F32)
    falling = jnp.zeros((MY, 128), F32)
    middle = []
    for x in range(MX):
        plane = half_ref[x * MY : (x + 1) * MY, :]
        middle.append(plane)
        rising = jnp.where(slot == 2 * x, roll(plane, x * 16 - 56), rising)
        falling = jnp.where(slot == 2 * x + 1, roll(plane, x * 16 + 8), falling)
    up_ref[2 * BY : 2 * BY + MY, :] = rising
    down_ref[2 * BY : 2 * BY + MY, :] = falling
    for x in range(4):
        mid_ref[x] = jnp.where(slot < 8, middle[x], roll(middle[x + 4], 64))
    for fetch in fetches[1:]:
        fetch.wait()


def modes_kernel(slab_ref, cas_y_ref, cas_z_ref, along_ref, own_z_ref, out_ref):
    rows = [jnp.concatenate([slab_ref[gy * GZ + gz] for gz in range(GZ)], axis=1) for gy in range(GY)]
    by_y = exact(cas_y_ref[...], jnp.concatenate(rows, axis=0))
    lane = lanes((CY, 128)) >> 5
    planes = []
    for x in range(4):
        plane = jnp.zeros((CY, 128), F32)
        for gz in range(GZ):
            plane = jnp.where(lane == gz, roll(by_y[:, gz * 128 : (gz + 1) * 128], (gz - x) * 32), plane)
        planes.append(plane)
    by_z = exact(jnp.concatenate(planes, axis=0), cas_z_ref[...])
    source = [by_z[x * CY : (x + 1) * CY, :] for x in range(4)]
    own_y = cas_y_ref[pl.ds(pl.multiple_of(lax.axis_index("gy") * 8, 8), 8), :]
    own_z = own_z_ref[lax.axis_index("gz")]
    me = lax.axis_index("gx")
    lane = lanes((8, 128)) >> 5
    for block in range(GX):
        outs = []
        for x in range(4):
            total = None
            for other in range(4):
                shift = (block * 4 + x - other) % CX
                part = along_ref[min(shift, CX - shift)] * source[other]
                total = part if total is None else total + part
            outs.append(total)
        back_y = exact(own_y, jnp.concatenate(outs, axis=1))
        back_z = exact(
            jnp.concatenate([back_y[:, x * 128 : (x + 1) * 128] for x in range(4)], axis=0), own_z
        )
        result = back_z[0:8]
        for x in range(1, 4):
            result = jnp.where(lane == x, back_z[x * 8 : (x + 1) * 8], result)
        out_ref[lax.rem(me + block, GX)] = result


def y_message_kernel(f_ref, mid_ref, zlow_ref, zhigh_ref, halo_ref, up_ref, down_ref):
    halo = zlow_ref[...] + zhigh_ref[...]
    halo_ref[...] = halo
    for ref, fine, middle in ((up_ref, BY - 8, MY - 8), (down_ref, 0, 0)):
        for x in range(BX):
            ref[x * 8 : x * 8 + 8, :] = f_ref[x, fine : fine + 8, :]
        for group in range(2):
            ref[128 + group * 8 : 136 + group * 8, :] = halo[group * BY + fine : group * BY + fine + 8]
        for x in range(4):
            ref[144 + x * 8 : 152 + x * 8, :] = mid_ref[x, middle : middle + 8, :]
        ref[176:184, :] = halo[2 * BY + middle : 2 * BY + middle + 8]


def own_extended(f_ref, mid_ref, halo_ref, low_ref, high_ref):
    def joined(row, inner):
        return jnp.concatenate([low_ref[row : row + 8, :], inner, high_ref[row : row + 8, :]], axis=0)

    planes = [lambda x=x: joined(x * 8, f_ref[x]) for x in range(BX)]
    sides = [lambda g=g: joined(128 + g * 8, halo_ref[g * BY : (g + 1) * BY, :]) for g in range(2)]
    middle = [lambda x=x: joined(144 + x * 8, mid_ref[x]) for x in range(4)]
    edge = lambda: joined(176, halo_ref[2 * BY : 2 * BY + MY, :])
    return planes, sides, middle, edge


def x_message_kernel(f_ref, mid_ref, halo_ref, low_ref, high_ref, up_ref, down_ref):
    planes, sides, middle, edge = own_extended(f_ref, mid_ref, halo_ref, low_ref, high_ref)
    for ref, first, group in ((up_ref, 8, 1), (down_ref, 0, 0)):
        for x in range(8):
            ref[x * EY : (x + 1) * EY, :] = planes[first + x]()
        ref[8 * EY : 9 * EY, :] = sides[group]()
        for x in range(4):
            ref[9 * EY + x * EMY : 9 * EY + (x + 1) * EMY, :] = middle[x]()
        ref[9 * EY + 4 * EMY : 9 * EY + 5 * EMY, :] = edge()


def filter_yz(planes, sides, gy, gzh_ref, gzl_ref, out_ref, places):
    for group in range(2):
        data = jnp.concatenate([planes[group * 8 + x]() for x in range(8)] + [sides[group]()], axis=1)
        high, low = halves(data)
        by_y = dot(gy, jnp.concatenate([high, low, high], axis=0))
        slot = lanes((BY, 128)) >> 4
        for term in range(TERMS):
            rows = by_y[term * BY : (term + 1) * BY, :]
            side = rows[:, 8 * 128 :]
            left = jnp.concatenate([rows[:, x * 128 : (x + 1) * 128] for x in range(8)], axis=0)
            right = jnp.concatenate([jnp.where(slot == x, side, 0.0) for x in range(8)], axis=0)
            high, low = halves(jnp.concatenate([left, right], axis=1))
            gzh = gzh_ref[term]
            result = dot(high, gzh) + dot(low, gzh) + dot(high, gzl_ref[term])
            for x in range(8):
                out_ref[term, places[group * 8 + x]] = result[x * BY : (x + 1) * BY]


def filter_middle(middle, edge, my, mzh_ref, mzl_ref, out_ref, place):
    slot = lanes((EMY, 128)) >> 3
    rim = edge()
    planes = []
    for x in range(MX):
        plane = middle[x]() if x < 4 else roll(middle[x - 4](), 64)
        rolled = roll(rim, 64 - 16 * x)
        planes.append(jnp.where(slot < 8, plane, jnp.where(slot < 10, rolled, 0.0)))
    high, low = halves(jnp.concatenate(planes, axis=1))
    by_y = dot(my, jnp.concatenate([high, low, high], axis=0))
    for term in range(TERMS):
        rows = by_y[term * MY : (term + 1) * MY, :]
        left = jnp.concatenate([rows[:, x * 128 : (x + 1) * 128] for x in range(MX)], axis=0)
        high, low = halves(left)
        mzh = mzh_ref[term]
        result = dot(high, mzh) + dot(low, mzh) + dot(high, mzl_ref[term])
        for x in range(MX):
            out_ref[term, place + x] = result[x * MY : (x + 1) * MY]


def own_kernel(
    f_ref, mid_ref, halo_ref, low_ref, high_ref, gy_ref, gzh_ref, gzl_ref, my_ref, mzh_ref, mzl_ref, fine_ref, middle_ref
):
    planes, sides, middle, edge = own_extended(f_ref, mid_ref, halo_ref, low_ref, high_ref)
    filter_yz(planes, sides, gy_ref[...], gzh_ref, gzl_ref, fine_ref, list(range(BX)))
    filter_middle(middle, edge, my_ref[...], mzh_ref, mzl_ref, middle_ref, 0)


def near_kernel(
    low_ref, high_ref, fine_ref, middle_ref, gy_ref, gzh_ref, gzl_ref, my_ref, mzh_ref, mzl_ref, cx_ref,
    out_ref, ring_ref, small_ref, add_ref,
):
    planes, sides = [], []
    for ref in (low_ref, high_ref):
        planes += [lambda ref=ref, x=x: ref[x * EY : (x + 1) * EY, :] for x in range(8)]
        sides.append(lambda ref=ref: ref[8 * EY : 9 * EY, :])
    filter_yz(planes, sides, gy_ref[...], gzh_ref, gzl_ref, ring_ref, list(range(16)))
    for index, ref in enumerate((low_ref, high_ref)):
        middle = [lambda ref=ref, x=x: ref[9 * EY + x * EMY : 9 * EY + (x + 1) * EMY, :] for x in range(4)]
        edge = lambda ref=ref: ref[9 * EY + 4 * EMY : 9 * EY + 5 * EMY, :]
        filter_middle(middle, edge, my_ref[...], mzh_ref, mzl_ref, small_ref, index * MX)

    for tile in range(MY // 8):
        sl = slice(tile * 8, tile * 8 + 8)
        acc = [None] * MX
        for term in range(TERMS):
            for place in range(3 * MX):
                if place < MX:
                    value = small_ref[term, place, sl, :]
                elif place < 2 * MX:
                    value = middle_ref[term, place - MX, sl, :]
                else:
                    value = small_ref[term, place - MX, sl, :]
                for x in range(MX):
                    offset = place - x - RADIUS
                    if abs(offset) <= RADIUS:
                        part = cx_ref[(TERMS + term) * TAPS + abs(offset)] * value
                        acc[x] = part if acc[x] is None else acc[x] + part
        for x in range(MX):
            add_ref[x, pl.ds(tile * 16, 8, stride=2), :] = acc[x]
            add_ref[x, pl.ds(tile * 16 + 1, 8, stride=2), :] = acc[x]

    def tile_step(tile, carry):
        sl = pl.ds(pl.multiple_of(tile * 8, 8), 8)
        acc = [add_ref[x // 2, sl, :] for x in range(BX)]
        for term in range(TERMS):
            for place in range(2 * BX):
                if place < 8:
                    value = ring_ref[term, place, sl, :]
                elif place < 24:
                    value = fine_ref[term, place - 8, sl, :]
                else:
                    value = ring_ref[term, place - 16, sl, :]
                for x in range(BX):
                    offset = place - x - RADIUS
                    if abs(offset) <= RADIUS:
                        acc[x] = acc[x] + cx_ref[term * TAPS + abs(offset)] * value
        for x in range(BX):
            out_ref[x, sl, :] = acc[x]
        return carry

    lax.fori_loop(0, BY // 8, tile_step, 0)


def add_kernel(near_ref, top_ref, out_ref, wide_ref):
    top = top_ref[0]
    for source in range(1, GX):
        top = top + top_ref[source]
    shape = (BZ, 4 * BZ)
    row, column = lax.broadcasted_iota(jnp.int32, shape, 0), lanes(shape)
    spread = jnp.where(row == (column >> 7) * 32 + ((column & 127) >> 2), 1.0, 0.0).astype(BF16)
    high, rest = halves(top)
    rest = top - high.astype(F32)
    mid, low = halves(rest)
    parts = dot(jnp.concatenate([high.astype(F32), mid.astype(F32), low.astype(F32)], axis=0).astype(BF16), spread)
    wide = parts[0:8] + parts[8:16] + parts[16:24]
    for row in range(4):
        wide_ref[pl.ds(row, 8, stride=4), :] = wide[:, :128]
        wide_ref[pl.ds(BY + row, 8, stride=4), :] = wide[:, 128:256]
        wide_ref[pl.ds(2 * BY + row, 8, stride=4), :] = wide[:, 256:384]
        wide_ref[pl.ds(3 * BY + row, 8, stride=4), :] = wide[:, 384:512]
    for x in range(BX):
        out_ref[x] = near_ref[x] + wide_ref[(x // 4) * BY : (x // 4 + 1) * BY, :]


def call(kernel, outs, args, scratch=(), flops=0, hbm=False, limit=4):
    vmem = pl.BlockSpec(memory_space=pltpu.VMEM)
    specs = [pl.BlockSpec(memory_space=pltpu.HBM) if hbm else vmem] * len(args)
    if hbm:
        args = [pltpu.with_memory_space_constraint(a, pltpu.HBM) for a in args]
    size = sum(a.size * a.dtype.itemsize for a in args)
    return pl.pallas_call(
        kernel,
        out_shape=[jax.ShapeDtypeStruct(shape, dtype) for shape, dtype in outs],
        in_specs=specs,
        out_specs=[vmem] * len(outs),
        scratch_shapes=list(scratch),
        cost_estimate=pl.CostEstimate(flops=flops, bytes_accessed=size, transcendentals=0),
        compiler_params=pltpu.CompilerParams(vmem_limit_bytes=limit * 1024 * 1024),
    )(*args)


def ring(value, axis, step):
    count = lax.axis_size(axis)
    return lax.ppermute(value, axis, [(i, (i + step) % count) for i in range(count)])


def exchange(value, axis):
    return lax.all_to_all(value, axis, 0, 0, tiled=True)


def potential(charges, term_width, term_weight):
    sources = [charges, term_width, term_weight] + [jnp.asarray(t) for t in constant_tables()]
    coarse, mid, z_up, z_down, charges, term_width, term_weight, cas_y, cas_z, along_x, own_z = call(
        restrict_kernel,
        [((GY * GZ, 8, 128), F32), ((4, MY, 128), F32), ((ZROWS, 128), F32), ((ZROWS, 128), F32)]
        + [(a.shape, a.dtype) for a in sources],
        sources,
        [pltpu.VMEM((MX * MY, 128), F32), pltpu.SemaphoreType.DMA((FETCHED,))],
        flops=10**7,
        hbm=True,
        limit=4,
    )
    slab = exchange(coarse, ("gy", "gz"))
    z_low, z_high = ring(z_up, "gz", 1), ring(z_down, "gz", -1)
    gy, gzh, gzl, my, mzh, mzl, cx = call(
        weights_kernel,
        [
            ((TERMS * BY, 3 * EY), BF16),
            ((TERMS, 256, 128), BF16),
            ((TERMS, 256, 128), BF16),
            ((TERMS * MY, 3 * EMY), BF16),
            ((TERMS, 128, 128), BF16),
            ((TERMS, 128, 128), BF16),
            ((2 * TERMS * TAPS, 8, 128), F32),
        ],
        [term_width, term_weight],
        flops=10**7,
    )
    bands = [gy, gzh, gzl, my, mzh, mzl]
    halo, y_up, y_down = call(
        y_message_kernel,
        [((ZROWS, 128), F32), ((YROWS, 128), F32), ((YROWS, 128), F32)],
        [charges, mid, z_low, z_high],
        flops=10**6,
    )
    low, high = ring(y_up, "gy", 1), ring(y_down, "gy", -1)
    (partial,) = call(
        modes_kernel, [((GX, 8, 128), F32)], [slab, cas_y, cas_z, along_x, own_z], flops=5 * 10**7, limit=8
    )
    top = exchange(partial, "gx")
    x_up, x_down = call(
        x_message_kernel, [((XROWS, 128), F32), ((XROWS, 128), F32)], [charges, mid, halo, low, high], flops=10**6
    )
    x_low, x_high = ring(x_up, "gx", 1), ring(x_down, "gx", -1)
    fine, middle = call(
        own_kernel,
        [((TERMS, BX, BY, 128), F32), ((TERMS, MX, MY, 128), F32)],
        [charges, mid, halo, low, high] + bands,
        flops=10**8,
        limit=8,
    )
    (near,) = call(
        near_kernel,
        [((BX, BY, BZ), F32)],
        [x_low, x_high, fine, middle] + bands + [cx],
        [
            pltpu.VMEM((TERMS, 16, BY, 128), F32),
            pltpu.VMEM((TERMS, 16, MY, 128), F32),
            pltpu.VMEM((MX, BY, 128), F32),
        ],
        flops=10**8,
        limit=10,
    )
    (result,) = call(add_kernel, [((BX, BY, BZ), F32)], [near, top], [pltpu.VMEM((4 * BY, 128), F32)], flops=10**6)
    return result


def solution(mesh):
    placed = (P("gx", "gy", "gz"), P(), P())
    return jax.shard_map(potential, mesh=mesh, in_specs=placed, out_specs=P("gx", "gy", "gz"), check_vma=False)
```

```python
import math

import jax
import jax.numpy as jnp
import numpy as np
from jax import lax
from jax.experimental import pallas as pl
from jax.experimental.pallas import tpu as pltpu
from jax.sharding import PartitionSpec as P


TERMS = 4
RADIUS = 8
TAPS = RADIUS + 1

HIGHEST = lax.Precision.HIGHEST
F32 = jnp.float32
BF16 = jnp.bfloat16
screening = 0.01
strength = 4.0

BX, BY, BZ = 16, 32, 128
MX, MY, MZ = 8, 16, 64
CX, CY, CZ = 64, 64, 128
EY, EMY = BY + 2 * RADIUS, MY + 2 * RADIUS
GX, GY, GZ = 16, 8, 4
FETCHED, TABLES = 3, 5
ZROWS = 2 * BY + MY
YROWS = BX * 8 + 2 * 8 + 5 * 8
XROWS = 8 * EY + EY + 5 * EMY


def cas_table(count):
    modes = np.arange(count)
    angles = 2.0 * math.pi / count * (np.outer(modes, modes) % count)
    return np.cos(angles) + np.sin(angles)


def constant_tables():
    cas_y, cas_z = cas_table(CY), cas_table(CZ)

    def lam(count):
        return 2.0 - 2.0 * np.cos(2.0 * math.pi / count * np.arange(count))

    total = lam(CX)[:, None, None] + lam(CY)[None, :, None] + lam(CZ)[None, None, :]
    mult = strength * np.exp(-total) / (total + screening)
    mult[0, 0, 0] = 0.0
    shifts = np.arange(CX // 2 + 1)
    cosine = np.cos(2.0 * math.pi / CX * (np.outer(shifts, np.arange(CX)) % CX))
    along_x = np.einsum("dm,myz->dyz", cosine, mult) / (CX * CY * CZ)
    own_z = np.stack([np.tile(cas_z[:, 32 * g : 32 * g + 32], (1, 4)) for g in range(GZ)])

    def split(table):
        table = np.asarray(table, np.float32)
        high = table.astype(BF16)
        return high, (table - high.astype(np.float32)).astype(BF16)

    high, low = split(cas_y)
    tables = [
        np.concatenate([high, high, low], axis=1),
        np.asarray(np.concatenate([cas_y, cas_y], axis=1), np.float32),
        np.stack(split(cas_z)),
        np.stack(split(own_z), axis=1),
        np.asarray(along_x, np.float32),
    ]
    return [jnp.asarray(table) for table in tables]


def lanes(shape):
    return lax.broadcasted_iota(jnp.int32, shape, len(shape) - 1)


def roll(value, shift):
    shift %= 128
    return pltpu.roll(value, shift, 1) if shift else value


def dot(a, b):
    return jnp.dot(a, b, preferred_element_type=F32)


def exact(a, b):
    return jnp.dot(a, b, preferred_element_type=F32, precision=HIGHEST)


def halves(value):
    high = value.astype(BF16)
    return high, (value - high.astype(F32)).astype(BF16)


def weights_kernel(width_ref, weight_ref, *refs):
    fetches = [
        pltpu.make_async_copy(refs[i], refs[TABLES + 7 + i], refs[-1].at[i]) for i in range(TABLES)
    ]
    for fetch in fetches:
        fetch.start()
    gy_ref, gzh_ref, gzl_ref, my_ref, mzh_ref, mzl_ref, cx_ref = refs[TABLES : TABLES + 7]

    def scale(level, term):
        width = jnp.broadcast_to(width_ref[level : level + 1, term : term + 1], (8, 128))
        inverse = 1.0 / (2.0 * width * width)
        offset = lanes((8, 128)) - RADIUS
        values = jnp.exp(-(offset * offset).astype(F32) * inverse)
        values = jnp.where(offset <= RADIUS, values, 0.0)
        norm = 1.0 / jnp.sum(values, axis=1, keepdims=True)
        return inverse[0:1, 0:1], norm[0:1, 0:1]

    def taps(offset, inverse, norm):
        values = jnp.exp(-(offset * offset).astype(F32) * inverse) * norm
        return jnp.where(jnp.abs(offset) <= RADIUS, values, 0.0)

    def along_y(ref, term, inverse, norm, out, ext):
        shape = (out, 3 * ext)
        column = lanes(shape)
        row = lax.broadcasted_iota(jnp.int32, shape, 0)
        part = (column >= ext).astype(jnp.int32) + (column >= 2 * ext).astype(jnp.int32)
        high, low = halves(taps(column - part * ext - RADIUS - row, inverse, norm))
        ref[term * out : (term + 1) * out, :] = jnp.where(part < 2, high.astype(F32), low.astype(F32)).astype(BF16)

    for term in range(TERMS):
        inverse, norm = scale(0, term)
        along_y(gy_ref, term, inverse, norm, BY, EY)
        shape = (256, 128)
        row = lax.broadcasted_iota(jnp.int32, shape, 0)
        slot = row & 15
        place = jnp.where(row < BZ, row, jnp.where(slot < 8, slot - 8, BZ - 8 + slot))
        high, low = halves(taps(place - lanes(shape), inverse, norm))
        gzh_ref[term] = high
        gzl_ref[term] = low
        for offset in range(TAPS):
            value = jnp.exp(-float(offset * offset) * inverse) * norm * weight_ref[0:1, term : term + 1]
            cx_ref[term * TAPS + offset] = jnp.broadcast_to(value, (8, 128))

        inverse, norm = scale(1, term)
        along_y(my_ref, term, inverse, norm, MY, EMY)
        shape = (128, 128)
        row = lax.broadcasted_iota(jnp.int32, shape, 0)
        place = jnp.where(row < MZ, row, jnp.where(row < MZ + 8, row - MZ - 8, row - 8))
        values = taps(place - (lanes(shape) >> 1), inverse, norm)
        high, low = halves(jnp.where(row < MZ + 16, values, 0.0))
        mzh_ref[term] = high
        mzl_ref[term] = low
        for offset in range(TAPS):
            value = jnp.exp(-float(offset * offset) * inverse) * norm * weight_ref[1:2, term : term + 1]
            cx_ref[(TERMS + term) * TAPS + offset] = jnp.broadcast_to(value, (8, 128))
    for fetch in fetches:
        fetch.wait()


def restrict_kernel(*refs):
    sources, (coarse_ref, mid_ref, up_ref, down_ref), copies = refs[:FETCHED], refs[FETCHED : FETCHED + 4], refs[FETCHED + 4 :]
    copies, half_ref, sems = copies[:FETCHED], copies[FETCHED], copies[FETCHED + 1]
    fetches = [pltpu.make_async_copy(a, b, sems.at[i]) for i, (a, b) in enumerate(zip(sources, copies))]
    for fetch in fetches:
        fetch.start()
    f_ref = copies[0]
    fetches[0].wait()
    planes = []
    for x in range(MX):
        total = None
        for plane in (2 * x, 2 * x + 1):
            for odd in (0, 1):
                part = f_ref[plane, pl.ds(odd, MY, stride=2), :]
                total = part if total is None else total + part
        planes.append(total)
    row, column = lax.broadcasted_iota(jnp.int32, (BZ, 128), 0), lanes((BZ, 128))
    pairs = jnp.where((row >> 1) == column, 1.0 / 8.0, jnp.where((row >> 2) == column - 64, 1.0 / 64.0, 0.0))
    half_ref[...] = exact(jnp.concatenate(planes, axis=0), pairs)
    lane = lanes((8, 128))
    coarse = jnp.zeros((8, 128), F32)
    for x in range(4):
        part = None
        for row in (2 * x * MY, 2 * x * MY + 1, (2 * x + 1) * MY, (2 * x + 1) * MY + 1):
            piece = half_ref[pl.ds(row, 8, stride=2), :]
            part = piece if part is None else part + piece
        coarse = jnp.where((lane >> 5) == x, roll(part, x * 32 - 64), coarse)
    for target in range(GY * GZ):
        coarse_ref[target] = coarse

    slot = lanes((BY, 128)) >> 3
    for group in range(2):
        rising = jnp.zeros((BY, 128), F32)
        falling = jnp.zeros((BY, 128), F32)
        for x in range(8):
            plane = f_ref[group * 8 + x]
            rising = jnp.where(slot == 2 * x, roll(plane, x * 16 - 120), rising)
            falling = jnp.where(slot == 2 * x + 1, roll(plane, x * 16 + 8), falling)
        up_ref[group * BY : (group + 1) * BY, :] = rising
        down_ref[group * BY : (group + 1) * BY, :] = falling
    slot = lanes((MY, 128)) >> 3
    rising = jnp.zeros((MY, 128), F32)
    falling = jnp.zeros((MY, 128), F32)
    middle = []
    for x in range(MX):
        plane = half_ref[x * MY : (x + 1) * MY, :]
        middle.append(plane)
        rising = jnp.where(slot == 2 * x, roll(plane, x * 16 - 56), rising)
        falling = jnp.where(slot == 2 * x + 1, roll(plane, x * 16 + 8), falling)
    up_ref[2 * BY : 2 * BY + MY, :] = rising
    down_ref[2 * BY : 2 * BY + MY, :] = falling
    for x in range(4):
        mid_ref[x] = jnp.where(slot < 8, middle[x], roll(middle[x + 4], 64))
    for fetch in fetches[1:]:
        fetch.wait()


def modes_kernel(slab_ref, cas_y_ref, twice_y_ref, cas_z_ref, own_z_ref, along_ref, out_ref, modes_ref, wide_ref):
    rows = [jnp.concatenate([slab_ref[gy * GZ + gz] for gz in range(GZ)], axis=1) for gy in range(GY)]
    high, low = halves(jnp.concatenate(rows, axis=0))
    by_y = dot(cas_y_ref[...], jnp.concatenate([high, low, high], axis=0))
    lane = lanes((CY, 128)) >> 5
    planes = []
    for x in range(4):
        plane = jnp.zeros((CY, 128), F32)
        for gz in range(GZ):
            plane = jnp.where(lane == gz, roll(by_y[:, gz * 128 : (gz + 1) * 128], (gz - x) * 32), plane)
        planes.append(plane)
    high, low = halves(jnp.concatenate(planes, axis=0))
    modes_ref[...] = dot(high, cas_z_ref[0]) + dot(low, cas_z_ref[0]) + dot(high, cas_z_ref[1])

    def tile_step(tile, carry):
        start = pl.multiple_of(tile * 16, 16)
        source = [modes_ref[pl.ds(x * CY + start, 16), :] for x in range(4)]
        table = [along_ref[abs(shift), pl.ds(start, 16), :] for shift in (0, -1, -2, -3)]
        for place in range(CX):
            if place:
                table = [along_ref[min(place, CX - place), pl.ds(start, 16), :]] + table[:3]
            total = table[0] * source[0]
            for x in range(1, 4):
                total = total + table[x] * source[x]
            high, low = halves(total)
            wide_ref[pl.ds(start, 16), place * 128 : (place + 1) * 128] = high
            wide_ref[pl.ds(CY + start, 16), place * 128 : (place + 1) * 128] = low
        return carry

    lax.fori_loop(0, CY // 16, tile_step, 0)
    own_y = twice_y_ref[pl.ds(pl.multiple_of(lax.axis_index("gy") * 8, 8), 8), :]
    high, low = halves(own_y)
    low = jnp.where(lanes((8, 128)) < CY, low.astype(F32), 0.0)
    own_y = jnp.concatenate([high.astype(F32), low], axis=0).astype(BF16)
    back_y = dot(own_y, wide_ref[...])
    back_y = back_y[0:8] + back_y[8:16]
    high, low = halves(jnp.concatenate([back_y[:, x * 128 : (x + 1) * 128] for x in range(CX)], axis=0))
    own_z = own_z_ref.at[lax.axis_index("gz")]
    back_z = dot(high, own_z[0]) + dot(low, own_z[0]) + dot(high, own_z[1])
    me = lax.axis_index("gx")
    lane = lanes((8, 128)) >> 5
    for block in range(GX):
        result = back_z[block * 32 : block * 32 + 8]
        for x in range(1, 4):
            result = jnp.where(lane == x, back_z[block * 32 + x * 8 : block * 32 + (x + 1) * 8], result)
        out_ref[lax.rem(me + block, GX)] = result


def y_message_kernel(f_ref, mid_ref, zlow_ref, zhigh_ref, halo_ref, up_ref, down_ref):
    halo = zlow_ref[...] + zhigh_ref[...]
    halo_ref[...] = halo
    for ref, fine, middle in ((up_ref, BY - 8, MY - 8), (down_ref, 0, 0)):
        for x in range(BX):
            ref[x * 8 : x * 8 + 8, :] = f_ref[x, fine : fine + 8, :]
        for group in range(2):
            ref[128 + group * 8 : 136 + group * 8, :] = halo[group * BY + fine : group * BY + fine + 8]
        for x in range(4):
            ref[144 + x * 8 : 152 + x * 8, :] = mid_ref[x, middle : middle + 8, :]
        ref[176:184, :] = halo[2 * BY + middle : 2 * BY + middle + 8]


def own_extended(f_ref, mid_ref, halo_ref, low_ref, high_ref):
    def joined(row, inner):
        return jnp.concatenate([low_ref[row : row + 8, :], inner, high_ref[row : row + 8, :]], axis=0)

    planes = [lambda x=x: joined(x * 8, f_ref[x]) for x in range(BX)]
    sides = [lambda g=g: joined(128 + g * 8, halo_ref[g * BY : (g + 1) * BY, :]) for g in range(2)]
    middle = [lambda x=x: joined(144 + x * 8, mid_ref[x]) for x in range(4)]
    edge = lambda: joined(176, halo_ref[2 * BY : 2 * BY + MY, :])
    return planes, sides, middle, edge


def x_message_kernel(f_ref, mid_ref, halo_ref, low_ref, high_ref, up_ref, down_ref):
    planes, sides, middle, edge = own_extended(f_ref, mid_ref, halo_ref, low_ref, high_ref)
    for ref, first, group in ((up_ref, 8, 1), (down_ref, 0, 0)):
        for x in range(8):
            ref[x * EY : (x + 1) * EY, :] = planes[first + x]()
        ref[8 * EY : 9 * EY, :] = sides[group]()
        for x in range(4):
            ref[9 * EY + x * EMY : 9 * EY + (x + 1) * EMY, :] = middle[x]()
        ref[9 * EY + 4 * EMY : 9 * EY + 5 * EMY, :] = edge()


def filter_yz(planes, sides, gy, gzh_ref, gzl_ref, out_ref, places):
    for group in range(2):
        data = jnp.concatenate([planes[group * 8 + x]() for x in range(8)] + [sides[group]()], axis=1)
        high, low = halves(data)
        by_y = dot(gy, jnp.concatenate([high, low, high], axis=0))
        slot = lanes((BY, 128)) >> 4
        for term in range(TERMS):
            rows = by_y[term * BY : (term + 1) * BY, :]
            side = rows[:, 8 * 128 :]
            left = jnp.concatenate([rows[:, x * 128 : (x + 1) * 128] for x in range(8)], axis=0)
            right = jnp.concatenate([jnp.where(slot == x, side, 0.0) for x in range(8)], axis=0)
            high, low = halves(jnp.concatenate([left, right], axis=1))
            gzh = gzh_ref[term]
            result = dot(high, gzh) + dot(low, gzh) + dot(high, gzl_ref[term])
            for x in range(8):
                out_ref[term, places[group * 8 + x]] = result[x * BY : (x + 1) * BY]


def filter_middle(middle, edge, my, mzh_ref, mzl_ref, out_ref, place):
    slot = lanes((EMY, 128)) >> 3
    rim = edge()
    planes = []
    for x in range(MX):
        plane = middle[x]() if x < 4 else roll(middle[x - 4](), 64)
        rolled = roll(rim, 64 - 16 * x)
        planes.append(jnp.where(slot < 8, plane, jnp.where(slot < 10, rolled, 0.0)))
    high, low = halves(jnp.concatenate(planes, axis=1))
    by_y = dot(my, jnp.concatenate([high, low, high], axis=0))
    for term in range(TERMS):
        rows = by_y[term * MY : (term + 1) * MY, :]
        left = jnp.concatenate([rows[:, x * 128 : (x + 1) * 128] for x in range(MX)], axis=0)
        high, low = halves(left)
        mzh = mzh_ref[term]
        result = dot(high, mzh) + dot(low, mzh) + dot(high, mzl_ref[term])
        for x in range(MX):
            out_ref[term, place + x] = result[x * MY : (x + 1) * MY]


def own_kernel(
    f_ref, mid_ref, halo_ref, low_ref, high_ref, gy_ref, gzh_ref, gzl_ref, my_ref, mzh_ref, mzl_ref, fine_ref, middle_ref
):
    planes, sides, middle, edge = own_extended(f_ref, mid_ref, halo_ref, low_ref, high_ref)
    filter_yz(planes, sides, gy_ref[...], gzh_ref, gzl_ref, fine_ref, list(range(BX)))
    filter_middle(middle, edge, my_ref[...], mzh_ref, mzl_ref, middle_ref, 0)


def near_kernel(
    low_ref, high_ref, fine_ref, middle_ref, gy_ref, gzh_ref, gzl_ref, my_ref, mzh_ref, mzl_ref, cx_ref,
    out_ref, ring_ref, small_ref, add_ref,
):
    planes, sides = [], []
    for ref in (low_ref, high_ref):
        planes += [lambda ref=ref, x=x: ref[x * EY : (x + 1) * EY, :] for x in range(8)]
        sides.append(lambda ref=ref: ref[8 * EY : 9 * EY, :])
    filter_yz(planes, sides, gy_ref[...], gzh_ref, gzl_ref, ring_ref, list(range(16)))
    for index, ref in enumerate((low_ref, high_ref)):
        middle = [lambda ref=ref, x=x: ref[9 * EY + x * EMY : 9 * EY + (x + 1) * EMY, :] for x in range(4)]
        edge = lambda ref=ref: ref[9 * EY + 4 * EMY : 9 * EY + 5 * EMY, :]
        filter_middle(middle, edge, my_ref[...], mzh_ref, mzl_ref, small_ref, index * MX)

    for tile in range(MY // 8):
        sl = slice(tile * 8, tile * 8 + 8)
        acc = [None] * MX
        for term in range(TERMS):
            for place in range(3 * MX):
                if place < MX:
                    value = small_ref[term, place, sl, :]
                elif place < 2 * MX:
                    value = middle_ref[term, place - MX, sl, :]
                else:
                    value = small_ref[term, place - MX, sl, :]
                for x in range(MX):
                    offset = place - x - RADIUS
                    if abs(offset) <= RADIUS:
                        part = cx_ref[(TERMS + term) * TAPS + abs(offset)] * value
                        acc[x] = part if acc[x] is None else acc[x] + part
        for x in range(MX):
            add_ref[x, pl.ds(tile * 16, 8, stride=2), :] = acc[x]
            add_ref[x, pl.ds(tile * 16 + 1, 8, stride=2), :] = acc[x]

    def tile_step(tile, carry):
        sl = pl.ds(pl.multiple_of(tile * 8, 8), 8)
        acc = [add_ref[x // 2, sl, :] for x in range(BX)]
        for term in range(TERMS):
            for place in range(2 * BX):
                if place < 8:
                    value = ring_ref[term, place, sl, :]
                elif place < 24:
                    value = fine_ref[term, place - 8, sl, :]
                else:
                    value = ring_ref[term, place - 16, sl, :]
                for x in range(BX):
                    offset = place - x - RADIUS
                    if abs(offset) <= RADIUS:
                        acc[x] = acc[x] + cx_ref[term * TAPS + abs(offset)] * value
        for x in range(BX):
            out_ref[x, sl, :] = acc[x]
        return carry

    lax.fori_loop(0, BY // 8, tile_step, 0)


def add_kernel(near_ref, top_ref, out_ref, wide_ref):
    top = top_ref[0]
    for source in range(1, GX):
        top = top + top_ref[source]
    shape = (BZ, 4 * BZ)
    row, column = lax.broadcasted_iota(jnp.int32, shape, 0), lanes(shape)
    spread = jnp.where(row == (column >> 7) * 32 + ((column & 127) >> 2), 1.0, 0.0).astype(BF16)
    high, rest = halves(top)
    rest = top - high.astype(F32)
    mid, low = halves(rest)
    parts = dot(jnp.concatenate([high.astype(F32), mid.astype(F32), low.astype(F32)], axis=0).astype(BF16), spread)
    wide = parts[0:8] + parts[8:16] + parts[16:24]
    for row in range(4):
        wide_ref[pl.ds(row, 8, stride=4), :] = wide[:, :128]
        wide_ref[pl.ds(BY + row, 8, stride=4), :] = wide[:, 128:256]
        wide_ref[pl.ds(2 * BY + row, 8, stride=4), :] = wide[:, 256:384]
        wide_ref[pl.ds(3 * BY + row, 8, stride=4), :] = wide[:, 384:512]
    for x in range(BX):
        out_ref[x] = near_ref[x] + wide_ref[(x // 4) * BY : (x // 4 + 1) * BY, :]


def call(kernel, outs, args, scratch=(), flops=0, hbm=0, limit=4):
    vmem = pl.BlockSpec(memory_space=pltpu.VMEM)
    near = len(args) - hbm
    specs = [vmem] * near + [pl.BlockSpec(memory_space=pltpu.HBM)] * hbm
    args = args[:near] + [pltpu.with_memory_space_constraint(a, pltpu.HBM) for a in args[near:]]
    size = sum(a.size * a.dtype.itemsize for a in args)
    return pl.pallas_call(
        kernel,
        out_shape=[jax.ShapeDtypeStruct(shape, dtype) for shape, dtype in outs],
        in_specs=specs,
        out_specs=[vmem] * len(outs),
        scratch_shapes=list(scratch),
        cost_estimate=pl.CostEstimate(flops=flops, bytes_accessed=size, transcendentals=0),
        compiler_params=pltpu.CompilerParams(vmem_limit_bytes=limit * 1024 * 1024),
    )(*args)


def ring(value, axis, step):
    count = lax.axis_size(axis)
    return lax.ppermute(value, axis, [(i, (i + step) % count) for i in range(count)])


def exchange(value, axis):
    return lax.all_to_all(value, axis, 0, 0, tiled=True)


def potential(charges, term_width, term_weight):
    sources = [charges, term_width, term_weight]
    coarse, mid, z_up, z_down, charges, term_width, term_weight = call(
        restrict_kernel,
        [((GY * GZ, 8, 128), F32), ((4, MY, 128), F32), ((ZROWS, 128), F32), ((ZROWS, 128), F32)]
        + [(a.shape, a.dtype) for a in sources],
        sources,
        [pltpu.VMEM((MX * MY, 128), F32), pltpu.SemaphoreType.DMA((FETCHED,))],
        flops=10**7,
        hbm=3,
    )
    slab = exchange(coarse, ("gy", "gz"))
    z_low, z_high = ring(z_up, "gz", 1), ring(z_down, "gz", -1)
    tables = constant_tables()
    gy, gzh, gzl, my, mzh, mzl, cx, *tables = call(
        weights_kernel,
        [
            ((TERMS * BY, 3 * EY), BF16),
            ((TERMS, 256, 128), BF16),
            ((TERMS, 256, 128), BF16),
            ((TERMS * MY, 3 * EMY), BF16),
            ((TERMS, 128, 128), BF16),
            ((TERMS, 128, 128), BF16),
            ((2 * TERMS * TAPS, 8, 128), F32),
        ]
        + [(a.shape, a.dtype) for a in tables],
        [term_width, term_weight] + tables,
        [pltpu.SemaphoreType.DMA((TABLES,))],
        flops=10**7,
        hbm=TABLES,
    )
    bands = [gy, gzh, gzl, my, mzh, mzl]
    halo, y_up, y_down = call(
        y_message_kernel,
        [((ZROWS, 128), F32), ((YROWS, 128), F32), ((YROWS, 128), F32)],
        [charges, mid, z_low, z_high],
        flops=10**6,
    )
    low, high = ring(y_up, "gy", 1), ring(y_down, "gy", -1)
    (partial,) = call(
        modes_kernel,
        [((GX, 8, 128), F32)],
        [slab] + tables,
        [pltpu.VMEM((4 * CY, 128), F32), pltpu.VMEM((2 * CY, CX * 128), BF16)],
        flops=5 * 10**7,
        limit=8,
    )
    top = exchange(partial, "gx")
    x_up, x_down = call(
        x_message_kernel, [((XROWS, 128), F32), ((XROWS, 128), F32)], [charges, mid, halo, low, high], flops=10**6
    )
    x_low, x_high = ring(x_up, "gx", 1), ring(x_down, "gx", -1)
    fine, middle = call(
        own_kernel,
        [((TERMS, BX, BY, 128), F32), ((TERMS, MX, MY, 128), F32)],
        [charges, mid, halo, low, high] + bands,
        flops=10**8,
        limit=8,
    )
    (near,) = call(
        near_kernel,
        [((BX, BY, BZ), F32)],
        [x_low, x_high, fine, middle] + bands + [cx],
        [
            pltpu.VMEM((TERMS, 16, BY, 128), F32),
            pltpu.VMEM((TERMS, 16, MY, 128), F32),
            pltpu.VMEM((MX, BY, 128), F32),
        ],
        flops=10**8,
        limit=10,
    )
    (result,) = call(add_kernel, [((BX, BY, BZ), F32)], [near, top], [pltpu.VMEM((4 * BY, 128), F32)], flops=10**6)
    return result


def solution(mesh):
    placed = (P("gx", "gy", "gz"), P(), P())
    return jax.shard_map(potential, mesh=mesh, in_specs=placed, out_specs=P("gx", "gy", "gz"), check_vma=False)
```

```python
import math

import jax
import jax.numpy as jnp
import numpy as np
from jax import lax
from jax.experimental import pallas as pl
from jax.experimental.pallas import tpu as pltpu
from jax.sharding import PartitionSpec as P


TERMS = 4
RADIUS = 8
TAPS = RADIUS + 1

HIGHEST = lax.Precision.HIGHEST
F32 = jnp.float32
BF16 = jnp.bfloat16
screening = 0.01
strength = 4.0

BX, BY, BZ = 16, 32, 128
MX, MY, MZ = 8, 16, 64
CX, CY, CZ = 64, 64, 128
EY, EMY = BY + 2 * RADIUS, MY + 2 * RADIUS
GX, GY, GZ = 16, 8, 4
FETCHED, PIECES = 8, 14
ZROWS = 2 * BY + MY
YROWS = BX * 8 + 2 * 8 + 5 * 8
XROWS = 8 * EY + EY + 5 * EMY


def cas_table(count):
    modes = np.arange(count)
    angles = 2.0 * math.pi / count * (np.outer(modes, modes) % count)
    return np.cos(angles) + np.sin(angles)


def constant_tables():
    cas_y, cas_z = cas_table(CY), cas_table(CZ)

    def lam(count):
        return 2.0 - 2.0 * np.cos(2.0 * math.pi / count * np.arange(count))

    total = lam(CX)[:, None, None] + lam(CY)[None, :, None] + lam(CZ)[None, None, :]
    mult = strength * np.exp(-total) / (total + screening)
    mult[0, 0, 0] = 0.0
    shifts = np.arange(CX // 2 + 1)
    cosine = np.cos(2.0 * math.pi / CX * (np.outer(shifts, np.arange(CX)) % CX))
    along_x = np.einsum("dm,myz->dyz", cosine, mult) / (CX * CY * CZ)
    own_z = np.stack([np.tile(cas_z[:, 32 * g : 32 * g + 32], (1, 4)) for g in range(GZ)])

    def split(table):
        table = np.asarray(table, np.float32)
        high = table.astype(BF16)
        return high, (table - high.astype(np.float32)).astype(BF16)

    high, low = split(cas_y)
    tables = [
        np.concatenate([high, high, low], axis=1),
        np.asarray(np.concatenate([cas_y, cas_y], axis=1), np.float32),
        np.stack(split(cas_z)),
        np.stack(split(own_z), axis=1),
        np.asarray(along_x, np.float32),
    ]
    return [jnp.asarray(table) for table in tables]


def lanes(shape):
    return lax.broadcasted_iota(jnp.int32, shape, len(shape) - 1)


def roll(value, shift):
    shift %= 128
    return pltpu.roll(value, shift, 1) if shift else value


def dot(a, b):
    return jnp.dot(a, b, preferred_element_type=F32)


def exact(a, b):
    return jnp.dot(a, b, preferred_element_type=F32, precision=HIGHEST)


def halves(value):
    high = value.astype(BF16)
    return high, (value - high.astype(F32)).astype(BF16)


def weights_kernel(width_ref, weight_ref, gy_ref, gzh_ref, gzl_ref, my_ref, mzh_ref, mzl_ref, cx_ref):
    offset = lanes((8, 128)) - RADIUS
    squares = (offset * offset).astype(F32)

    def scale(level, term):
        width = jnp.broadcast_to(width_ref[level : level + 1, term : term + 1], (8, 128))
        inverse = -1.0 / (2.0 * width * width)
        values = jnp.where(offset <= RADIUS, jnp.exp(squares * inverse), 0.0)
        norm = 1.0 / jnp.broadcast_to(jnp.sum(values, axis=1, keepdims=True), (8, 128))
        weight = jnp.broadcast_to(weight_ref[level : level + 1, term : term + 1], (8, 128))
        for distance in range(TAPS):
            value = jnp.exp(float(distance * distance) * inverse) * norm * weight
            row = (level * TERMS + term) * TAPS + distance
            cx_ref[row : row + 1, :] = value[0:1, :]
        return inverse, norm

    def taps(place, inverse, norm):
        rows, columns = place.shape
        inverse, norm = [
            jnp.concatenate([jnp.concatenate([v] * (columns // 128), axis=1)] * (rows // 8), axis=0) for v in (inverse, norm)
        ]
        values = jnp.exp((place * place).astype(F32) * inverse) * norm
        return jnp.where(jnp.abs(place) <= RADIUS, values, 0.0)

    def along_y(ref, term, inverse, norm, out, ext):
        shape = (out, 256 if 3 * ext > 128 else 128)
        column = lanes(shape)
        row = lax.broadcasted_iota(jnp.int32, shape, 0)
        part = (column >= ext).astype(jnp.int32) + (column >= 2 * ext).astype(jnp.int32)
        high, low = halves(taps(column - part * ext - RADIUS - row, inverse, norm))
        both = jnp.where(part < 2, high.astype(F32), low.astype(F32))
        ref[term * out : (term + 1) * out, :] = both[:, : 3 * ext].astype(BF16)

    for term in range(TERMS):
        inverse, norm = scale(0, term)
        along_y(gy_ref, term, inverse, norm, BY, EY)
        shape = (256, 128)
        row = lax.broadcasted_iota(jnp.int32, shape, 0)
        slot = row & 15
        place = jnp.where(row < BZ, row, jnp.where(slot < 8, slot - 8, BZ - 8 + slot))
        high, low = halves(taps(place - lanes(shape), inverse, norm))
        gzh_ref[term] = high
        gzl_ref[term] = low

        inverse, norm = scale(1, term)
        along_y(my_ref, term, inverse, norm, MY, EMY)
        shape = (128, 128)
        row = lax.broadcasted_iota(jnp.int32, shape, 0)
        place = jnp.where(row < MZ, row, jnp.where(row < MZ + 8, row - MZ - 8, row - 8))
        values = taps(place - (lanes(shape) >> 1), inverse, norm)
        high, low = halves(jnp.where(row < MZ + 16, values, 0.0))
        mzh_ref[term] = high
        mzl_ref[term] = low


def restrict_kernel(*refs):
    sources, (coarse_ref, mid_ref, up_ref, down_ref), copies = refs[:FETCHED], refs[FETCHED : FETCHED + 4], refs[FETCHED + 4 :]
    copies, half_ref, sems = copies[:FETCHED], copies[FETCHED], copies[FETCHED + 1]
    pieces = [(0, x, 4) for x in range(0, BX, 4)] + [(i, 0, None) for i in range(1, FETCHED - 1)]
    pieces += [(FETCHED - 1, x, min(x + 9, CX // 2 + 1) - x) for x in range(0, CX // 2 + 1, 9)]
    fetches = []
    for count, (i, first, size) in enumerate(pieces):
        source, copy = sources[i], copies[i]
        if size:
            source, copy = source.at[pl.ds(first, size)], copy.at[pl.ds(first, size)]
        fetches.append(pltpu.make_async_copy(source, copy, sems.at[count]))
        fetches[-1].start()
    f_ref = copies[0]
    planes = []
    for x in range(MX):
        if x % 2 == 0:
            fetches[x // 2].wait()
        total = None
        for plane in (2 * x, 2 * x + 1):
            for odd in (0, 1):
                part = f_ref[plane, pl.ds(odd, MY, stride=2), :]
                total = part if total is None else total + part
        planes.append(total)
    row, column = lax.broadcasted_iota(jnp.int32, (BZ, 128), 0), lanes((BZ, 128))
    pairs = jnp.where((row >> 1) == column, 1.0 / 8.0, jnp.where((row >> 2) == column - 64, 1.0 / 64.0, 0.0))
    half_ref[...] = exact(jnp.concatenate(planes, axis=0), pairs)
    lane = lanes((8, 128))
    coarse = jnp.zeros((8, 128), F32)
    for x in range(4):
        part = None
        for row in (2 * x * MY, 2 * x * MY + 1, (2 * x + 1) * MY, (2 * x + 1) * MY + 1):
            piece = half_ref[pl.ds(row, 8, stride=2), :]
            part = piece if part is None else part + piece
        coarse = jnp.where((lane >> 5) == x, roll(part, x * 32 - 64), coarse)
    for target in range(GY * GZ):
        coarse_ref[target] = coarse

    slot = lanes((BY, 128)) >> 3
    for group in range(2):
        rising = jnp.zeros((BY, 128), F32)
        falling = jnp.zeros((BY, 128), F32)
        for x in range(8):
            plane = f_ref[group * 8 + x]
            rising = jnp.where(slot == 2 * x, roll(plane, x * 16 - 120), rising)
            falling = jnp.where(slot == 2 * x + 1, roll(plane, x * 16 + 8), falling)
        up_ref[group * BY : (group + 1) * BY, :] = rising
        down_ref[group * BY : (group + 1) * BY, :] = falling
    slot = lanes((MY, 128)) >> 3
    rising = jnp.zeros((MY, 128), F32)
    falling = jnp.zeros((MY, 128), F32)
    middle = []
    for x in range(MX):
        plane = half_ref[x * MY : (x + 1) * MY, :]
        middle.append(plane)
        rising = jnp.where(slot == 2 * x, roll(plane, x * 16 - 56), rising)
        falling = jnp.where(slot == 2 * x + 1, roll(plane, x * 16 + 8), falling)
    up_ref[2 * BY : 2 * BY + MY, :] = rising
    down_ref[2 * BY : 2 * BY + MY, :] = falling
    for x in range(4):
        mid_ref[x] = jnp.where(slot < 8, middle[x], roll(middle[x + 4], 64))
    for fetch in fetches[4:]:
        fetch.wait()


def modes_kernel(slab_ref, cas_y_ref, twice_y_ref, cas_z_ref, own_z_ref, along_ref, out_ref, modes_ref, wide_ref):
    rows = [jnp.concatenate([slab_ref[gy * GZ + gz] for gz in range(GZ)], axis=1) for gy in range(GY)]
    high, low = halves(jnp.concatenate(rows, axis=0))
    by_y = dot(cas_y_ref[...], jnp.concatenate([high, low, high], axis=0))
    lane = lanes((CY, 128)) >> 5
    planes = []
    for x in range(4):
        plane = jnp.zeros((CY, 128), F32)
        for gz in range(GZ):
            plane = jnp.where(lane == gz, roll(by_y[:, gz * 128 : (gz + 1) * 128], (gz - x) * 32), plane)
        planes.append(plane)
    high, low = halves(jnp.concatenate(planes, axis=0))
    modes_ref[...] = dot(high, cas_z_ref[0]) + dot(low, cas_z_ref[0]) + dot(high, cas_z_ref[1])

    def tile_step(tile, carry):
        start = pl.multiple_of(tile * 16, 16)
        source = [modes_ref[pl.ds(x * CY + start, 16), :] for x in range(4)]
        table = [along_ref[abs(shift), pl.ds(start, 16), :] for shift in (0, -1, -2, -3)]
        for place in range(CX):
            if place:
                table = [along_ref[min(place, CX - place), pl.ds(start, 16), :]] + table[:3]
            total = table[0] * source[0]
            for x in range(1, 4):
                total = total + table[x] * source[x]
            high, low = halves(total)
            wide_ref[pl.ds(start, 16), place * 128 : (place + 1) * 128] = high
            wide_ref[pl.ds(CY + start, 16), place * 128 : (place + 1) * 128] = low
        return carry

    lax.fori_loop(0, CY // 16, tile_step, 0)
    own_y = twice_y_ref[pl.ds(pl.multiple_of(lax.axis_index("gy") * 8, 8), 8), :]
    high, low = halves(own_y)
    low = jnp.where(lanes((8, 128)) < CY, low.astype(F32), 0.0)
    own_y = jnp.concatenate([high.astype(F32), low], axis=0).astype(BF16)
    back_y = dot(own_y, wide_ref[...])
    back_y = back_y[0:8] + back_y[8:16]
    high, low = halves(jnp.concatenate([back_y[:, x * 128 : (x + 1) * 128] for x in range(CX)], axis=0))
    own_z = own_z_ref.at[lax.axis_index("gz")]
    back_z = dot(high, own_z[0]) + dot(low, own_z[0]) + dot(high, own_z[1])
    me = lax.axis_index("gx")
    lane = lanes((8, 128)) >> 5
    for block in range(GX):
        result = back_z[block * 32 : block * 32 + 8]
        for x in range(1, 4):
            result = jnp.where(lane == x, back_z[block * 32 + x * 8 : block * 32 + (x + 1) * 8], result)
        out_ref[lax.rem(me + block, GX)] = result


def y_message_kernel(f_ref, mid_ref, zlow_ref, zhigh_ref, halo_ref, up_ref, down_ref):
    halo = zlow_ref[...] + zhigh_ref[...]
    halo_ref[...] = halo
    for ref, fine, middle in ((up_ref, BY - 8, MY - 8), (down_ref, 0, 0)):
        for x in range(BX):
            ref[x * 8 : x * 8 + 8, :] = f_ref[x, fine : fine + 8, :]
        for group in range(2):
            ref[128 + group * 8 : 136 + group * 8, :] = halo[group * BY + fine : group * BY + fine + 8]
        for x in range(4):
            ref[144 + x * 8 : 152 + x * 8, :] = mid_ref[x, middle : middle + 8, :]
        ref[176:184, :] = halo[2 * BY + middle : 2 * BY + middle + 8]


def own_extended(f_ref, mid_ref, halo_ref, low_ref, high_ref):
    def joined(row, inner):
        return jnp.concatenate([low_ref[row : row + 8, :], inner, high_ref[row : row + 8, :]], axis=0)

    planes = [lambda x=x: joined(x * 8, f_ref[x]) for x in range(BX)]
    sides = [lambda g=g: joined(128 + g * 8, halo_ref[g * BY : (g + 1) * BY, :]) for g in range(2)]
    middle = [lambda x=x: joined(144 + x * 8, mid_ref[x]) for x in range(4)]
    edge = lambda: joined(176, halo_ref[2 * BY : 2 * BY + MY, :])
    return planes, sides, middle, edge


def x_message_kernel(f_ref, mid_ref, halo_ref, low_ref, high_ref, up_ref, down_ref):
    planes, sides, middle, edge = own_extended(f_ref, mid_ref, halo_ref, low_ref, high_ref)
    for ref, first, group in ((up_ref, 8, 1), (down_ref, 0, 0)):
        for x in range(8):
            ref[x * EY : (x + 1) * EY, :] = planes[first + x]()
        ref[8 * EY : 9 * EY, :] = sides[group]()
        for x in range(4):
            ref[9 * EY + x * EMY : 9 * EY + (x + 1) * EMY, :] = middle[x]()
        ref[9 * EY + 4 * EMY : 9 * EY + 5 * EMY, :] = edge()


def filter_yz(planes, sides, gy, gzh_ref, gzl_ref, out_ref, places):
    for group in range(2):
        data = jnp.concatenate([planes[group * 8 + x]() for x in range(8)] + [sides[group]()], axis=1)
        high, low = halves(data)
        by_y = dot(gy, jnp.concatenate([high, low, high], axis=0))
        slot = lanes((BY, 128)) >> 4
        for term in range(TERMS):
            rows = by_y[term * BY : (term + 1) * BY, :]
            side = rows[:, 8 * 128 :]
            left = jnp.concatenate([rows[:, x * 128 : (x + 1) * 128] for x in range(8)], axis=0)
            right = jnp.concatenate([jnp.where(slot == x, side, 0.0) for x in range(8)], axis=0)
            high, low = halves(jnp.concatenate([left, right], axis=1))
            gzh = gzh_ref[term]
            result = dot(high, gzh) + dot(low, gzh) + dot(high, gzl_ref[term])
            for x in range(8):
                out_ref[term, places[group * 8 + x]] = result[x * BY : (x + 1) * BY]


def filter_middle(middle, edge, my, mzh_ref, mzl_ref, out_ref, place):
    slot = lanes((EMY, 128)) >> 3
    rim = edge()
    planes = []
    for x in range(MX):
        plane = middle[x]() if x < 4 else roll(middle[x - 4](), 64)
        rolled = roll(rim, 64 - 16 * x)
        planes.append(jnp.where(slot < 8, plane, jnp.where(slot < 10, rolled, 0.0)))
    high, low = halves(jnp.concatenate(planes, axis=1))
    by_y = dot(my, jnp.concatenate([high, low, high], axis=0))
    for term in range(TERMS):
        rows = by_y[term * MY : (term + 1) * MY, :]
        left = jnp.concatenate([rows[:, x * 128 : (x + 1) * 128] for x in range(MX)], axis=0)
        high, low = halves(left)
        mzh = mzh_ref[term]
        result = dot(high, mzh) + dot(low, mzh) + dot(high, mzl_ref[term])
        for x in range(MX):
            out_ref[term, place + x] = result[x * MY : (x + 1) * MY]


def own_kernel(
    f_ref, mid_ref, halo_ref, low_ref, high_ref, gy_ref, gzh_ref, gzl_ref, my_ref, mzh_ref, mzl_ref, fine_ref, middle_ref
):
    planes, sides, middle, edge = own_extended(f_ref, mid_ref, halo_ref, low_ref, high_ref)
    filter_yz(planes, sides, gy_ref[...], gzh_ref, gzl_ref, fine_ref, list(range(BX)))
    filter_middle(middle, edge, my_ref[...], mzh_ref, mzl_ref, middle_ref, 0)


def near_kernel(
    low_ref, high_ref, fine_ref, middle_ref, gy_ref, gzh_ref, gzl_ref, my_ref, mzh_ref, mzl_ref, cx_ref,
    out_ref, ring_ref, small_ref, add_ref,
):
    planes, sides = [], []
    for ref in (low_ref, high_ref):
        planes += [lambda ref=ref, x=x: ref[x * EY : (x + 1) * EY, :] for x in range(8)]
        sides.append(lambda ref=ref: ref[8 * EY : 9 * EY, :])
    filter_yz(planes, sides, gy_ref[...], gzh_ref, gzl_ref, ring_ref, list(range(16)))
    for index, ref in enumerate((low_ref, high_ref)):
        middle = [lambda ref=ref, x=x: ref[9 * EY + x * EMY : 9 * EY + (x + 1) * EMY, :] for x in range(4)]
        edge = lambda ref=ref: ref[9 * EY + 4 * EMY : 9 * EY + 5 * EMY, :]
        filter_middle(middle, edge, my_ref[...], mzh_ref, mzl_ref, small_ref, index * MX)

    def tap_at(row):
        return jnp.broadcast_to(cx_ref[row : row + 1, :], (8, 128))

    for tile in range(MY // 8):
        sl = slice(tile * 8, tile * 8 + 8)
        acc = [None] * MX
        for term in range(TERMS):
            for place in range(3 * MX):
                if place < MX:
                    value = small_ref[term, place, sl, :]
                elif place < 2 * MX:
                    value = middle_ref[term, place - MX, sl, :]
                else:
                    value = small_ref[term, place - MX, sl, :]
                for x in range(MX):
                    offset = place - x - RADIUS
                    if abs(offset) <= RADIUS:
                        part = tap_at((TERMS + term) * TAPS + abs(offset)) * value
                        acc[x] = part if acc[x] is None else acc[x] + part
        for x in range(MX):
            add_ref[x, pl.ds(tile * 16, 8, stride=2), :] = acc[x]
            add_ref[x, pl.ds(tile * 16 + 1, 8, stride=2), :] = acc[x]

    def tile_step(tile, carry):
        sl = pl.ds(pl.multiple_of(tile * 8, 8), 8)
        acc = [add_ref[x // 2, sl, :] for x in range(BX)]
        for term in range(TERMS):
            for place in range(2 * BX):
                if place < 8:
                    value = ring_ref[term, place, sl, :]
                elif place < 24:
                    value = fine_ref[term, place - 8, sl, :]
                else:
                    value = ring_ref[term, place - 16, sl, :]
                for x in range(BX):
                    offset = place - x - RADIUS
                    if abs(offset) <= RADIUS:
                        acc[x] = acc[x] + tap_at(term * TAPS + abs(offset)) * value
        for x in range(BX):
            out_ref[x, sl, :] = acc[x]
        return carry

    lax.fori_loop(0, BY // 8, tile_step, 0)


def add_kernel(near_ref, top_ref, out_ref, wide_ref):
    top = top_ref[0]
    for source in range(1, GX):
        top = top + top_ref[source]
    shape = (BZ, 4 * BZ)
    row, column = lax.broadcasted_iota(jnp.int32, shape, 0), lanes(shape)
    spread = jnp.where(row == (column >> 7) * 32 + ((column & 127) >> 2), 1.0, 0.0).astype(BF16)
    high, rest = halves(top)
    rest = top - high.astype(F32)
    mid, low = halves(rest)
    parts = dot(jnp.concatenate([high.astype(F32), mid.astype(F32), low.astype(F32)], axis=0).astype(BF16), spread)
    wide = parts[0:8] + parts[8:16] + parts[16:24]
    for row in range(4):
        wide_ref[pl.ds(row, 8, stride=4), :] = wide[:, :128]
        wide_ref[pl.ds(BY + row, 8, stride=4), :] = wide[:, 128:256]
        wide_ref[pl.ds(2 * BY + row, 8, stride=4), :] = wide[:, 256:384]
        wide_ref[pl.ds(3 * BY + row, 8, stride=4), :] = wide[:, 384:512]
    for x in range(BX):
        out_ref[x] = near_ref[x] + wide_ref[(x // 4) * BY : (x // 4 + 1) * BY, :]


def call(kernel, outs, args, scratch=(), flops=0, hbm=0, limit=4):
    vmem = pl.BlockSpec(memory_space=pltpu.VMEM)
    near = len(args) - hbm
    specs = [vmem] * near + [pl.BlockSpec(memory_space=pltpu.HBM)] * hbm
    args = args[:near] + [pltpu.with_memory_space_constraint(a, pltpu.HBM) for a in args[near:]]
    size = sum(a.size * a.dtype.itemsize for a in args)
    return pl.pallas_call(
        kernel,
        out_shape=[jax.ShapeDtypeStruct(shape, dtype) for shape, dtype in outs],
        in_specs=specs,
        out_specs=[vmem] * len(outs),
        scratch_shapes=list(scratch),
        cost_estimate=pl.CostEstimate(flops=flops, bytes_accessed=size, transcendentals=0),
        compiler_params=pltpu.CompilerParams(vmem_limit_bytes=limit * 1024 * 1024),
    )(*args)


def ring(value, axis, step):
    count = lax.axis_size(axis)
    return lax.ppermute(value, axis, [(i, (i + step) % count) for i in range(count)])


def exchange(value, axis):
    return lax.all_to_all(value, axis, 0, 0, tiled=True)


def potential(charges, term_width, term_weight):
    sources = [charges, term_width, term_weight] + constant_tables()
    coarse, mid, z_up, z_down, charges, term_width, term_weight, *tables = call(
        restrict_kernel,
        [((GY * GZ, 8, 128), F32), ((4, MY, 128), F32), ((ZROWS, 128), F32), ((ZROWS, 128), F32)]
        + [(a.shape, a.dtype) for a in sources],
        sources,
        [pltpu.VMEM((MX * MY, 128), F32), pltpu.SemaphoreType.DMA((PIECES,))],
        flops=10**7,
        hbm=FETCHED,
    )
    slab = exchange(coarse, ("gy", "gz"))
    z_low, z_high = ring(z_up, "gz", 1), ring(z_down, "gz", -1)
    gy, gzh, gzl, my, mzh, mzl, cx = call(
        weights_kernel,
        [
            ((TERMS * BY, 3 * EY), BF16),
            ((TERMS, 256, 128), BF16),
            ((TERMS, 256, 128), BF16),
            ((TERMS * MY, 3 * EMY), BF16),
            ((TERMS, 128, 128), BF16),
            ((TERMS, 128, 128), BF16),
            ((2 * TERMS * TAPS, 128), F32),
        ],
        [term_width, term_weight],
        flops=10**7,
    )
    bands = [gy, gzh, gzl, my, mzh, mzl]
    halo, y_up, y_down = call(
        y_message_kernel,
        [((ZROWS, 128), F32), ((YROWS, 128), F32), ((YROWS, 128), F32)],
        [charges, mid, z_low, z_high],
        flops=10**6,
    )
    low, high = ring(y_up, "gy", 1), ring(y_down, "gy", -1)
    (partial,) = call(
        modes_kernel,
        [((GX, 8, 128), F32)],
        [slab] + tables,
        [pltpu.VMEM((4 * CY, 128), F32), pltpu.VMEM((2 * CY, CX * 128), BF16)],
        flops=5 * 10**7,
        limit=8,
    )
    top = exchange(partial, "gx")
    x_up, x_down = call(
        x_message_kernel, [((XROWS, 128), F32), ((XROWS, 128), F32)], [charges, mid, halo, low, high], flops=10**6
    )
    x_low, x_high = ring(x_up, "gx", 1), ring(x_down, "gx", -1)
    fine, middle = call(
        own_kernel,
        [((TERMS, BX, BY, 128), F32), ((TERMS, MX, MY, 128), F32)],
        [charges, mid, halo, low, high] + bands,
        flops=10**8,
        limit=8,
    )
    (near,) = call(
        near_kernel,
        [((BX, BY, BZ), F32)],
        [x_low, x_high, fine, middle] + bands + [cx],
        [
            pltpu.VMEM((TERMS, 16, BY, 128), F32),
            pltpu.VMEM((TERMS, 16, MY, 128), F32),
            pltpu.VMEM((MX, BY, 128), F32),
        ],
        flops=10**8,
        limit=10,
    )
    (result,) = call(add_kernel, [((BX, BY, BZ), F32)], [near, top], [pltpu.VMEM((4 * BY, 128), F32)], flops=10**6)
    return result


def solution(mesh):
    placed = (P("gx", "gy", "gz"), P(), P())
    return jax.shard_map(potential, mesh=mesh, in_specs=placed, out_specs=P("gx", "gy", "gz"), check_vma=False)
```

```python
import math

import jax
import jax.numpy as jnp
import numpy as np
from jax import lax
from jax.experimental import pallas as pl
from jax.experimental.pallas import tpu as pltpu
from jax.sharding import PartitionSpec as P


TERMS = 4
RADIUS = 8
TAPS = RADIUS + 1

HIGHEST = lax.Precision.HIGHEST
F32 = jnp.float32
BF16 = jnp.bfloat16
screening = 0.01
strength = 4.0

BX, BY, BZ = 16, 32, 128
MX, MY, MZ = 8, 16, 64
CX, CY, CZ = 64, 64, 128
EY, EMY = BY + 2 * RADIUS, MY + 2 * RADIUS
GX, GY, GZ = 16, 8, 4
FETCHED, PIECES = 8, 14
ZROWS = 2 * BY + MY
YROWS = BX * 8 + 2 * 8 + 5 * 8
XROWS = 8 * EY + EY + 5 * EMY


def cas_table(count):
    modes = np.arange(count)
    angles = 2.0 * math.pi / count * (np.outer(modes, modes) % count)
    return np.cos(angles) + np.sin(angles)


def constant_tables():
    cas_y, cas_z = cas_table(CY), cas_table(CZ)

    def lam(count):
        return 2.0 - 2.0 * np.cos(2.0 * math.pi / count * np.arange(count))

    total = lam(CX)[:, None, None] + lam(CY)[None, :, None] + lam(CZ)[None, None, :]
    mult = strength * np.exp(-total) / (total + screening)
    mult[0, 0, 0] = 0.0
    shifts = np.arange(CX // 2 + 1)
    cosine = np.cos(2.0 * math.pi / CX * (np.outer(shifts, np.arange(CX)) % CX))
    along_x = np.einsum("dm,myz->dyz", cosine, mult) / (CX * CY * CZ)
    own_z = np.stack([np.tile(cas_z[:, 32 * g : 32 * g + 32], (1, 4)) for g in range(GZ)])

    def split(table):
        table = np.asarray(table, np.float32)
        high = table.astype(BF16)
        return high, (table - high.astype(np.float32)).astype(BF16)

    high, low = split(cas_y)
    tables = [
        np.concatenate([high, high, low], axis=1),
        np.asarray(np.concatenate([cas_y, cas_y], axis=1), np.float32),
        np.stack(split(cas_z)),
        np.stack(split(own_z), axis=1),
        np.asarray(along_x, np.float32),
    ]
    return [jnp.asarray(table) for table in tables]


def lanes(shape):
    return lax.broadcasted_iota(jnp.int32, shape, len(shape) - 1)


def roll(value, shift):
    shift %= 128
    return pltpu.roll(value, shift, 1) if shift else value


def dot(a, b):
    return jnp.dot(a, b, preferred_element_type=F32)


def exact(a, b):
    return jnp.dot(a, b, preferred_element_type=F32, precision=HIGHEST)


def halves(value):
    high = value.astype(BF16)
    return high, (value - high.astype(F32)).astype(BF16)


def weights_kernel(width_ref, weight_ref, gy_ref, gzh_ref, gzl_ref, my_ref, mzh_ref, mzl_ref, cx_ref):
    offset = lanes((8, 128)) - RADIUS
    squares = (offset * offset).astype(F32)

    def scale(level, term):
        width = jnp.broadcast_to(width_ref[level : level + 1, term : term + 1], (8, 128))
        inverse = -1.0 / (2.0 * width * width)
        values = jnp.where(offset <= RADIUS, jnp.exp(squares * inverse), 0.0)
        norm = 1.0 / jnp.broadcast_to(jnp.sum(values, axis=1, keepdims=True), (8, 128))
        weight = jnp.broadcast_to(weight_ref[level : level + 1, term : term + 1], (8, 128))
        for distance in range(TAPS):
            value = jnp.exp(float(distance * distance) * inverse) * norm * weight
            row = (level * TERMS + term) * TAPS + distance
            cx_ref[row : row + 1, :] = value[0:1, :]
        return inverse, norm

    def taps(place, inverse, norm):
        rows, columns = place.shape
        inverse, norm = [
            jnp.concatenate([jnp.concatenate([v] * (columns // 128), axis=1)] * (rows // 8), axis=0) for v in (inverse, norm)
        ]
        values = jnp.exp((place * place).astype(F32) * inverse) * norm
        return jnp.where(jnp.abs(place) <= RADIUS, values, 0.0)

    def along_y(ref, term, inverse, norm, out, ext):
        shape = (out, 256 if 3 * ext > 128 else 128)
        column = lanes(shape)
        row = lax.broadcasted_iota(jnp.int32, shape, 0)
        part = (column >= ext).astype(jnp.int32) + (column >= 2 * ext).astype(jnp.int32)
        high, low = halves(taps(column - part * ext - RADIUS - row, inverse, norm))
        both = jnp.where(part < 2, high.astype(F32), low.astype(F32))
        ref[term * out : (term + 1) * out, :] = both[:, : 3 * ext].astype(BF16)

    for term in range(TERMS):
        inverse, norm = scale(0, term)
        along_y(gy_ref, term, inverse, norm, BY, EY)
        shape = (256, 128)
        row = lax.broadcasted_iota(jnp.int32, shape, 0)
        slot = row & 15
        place = jnp.where(row < BZ, row, jnp.where(slot < 8, slot - 8, BZ - 8 + slot))
        high, low = halves(taps(place - lanes(shape), inverse, norm))
        gzh_ref[term] = high
        gzl_ref[term] = low

        inverse, norm = scale(1, term)
        along_y(my_ref, term, inverse, norm, MY, EMY)
        shape = (128, 128)
        row = lax.broadcasted_iota(jnp.int32, shape, 0)
        place = jnp.where(row < MZ, row, jnp.where(row < MZ + 8, row - MZ - 8, row - 8))
        values = taps(place - (lanes(shape) >> 1), inverse, norm)
        high, low = halves(jnp.where(row < MZ + 16, values, 0.0))
        mzh_ref[term] = high
        mzl_ref[term] = low


def restrict_kernel(*refs):
    sources, (coarse_ref, mid_ref, up_ref, down_ref), copies = refs[:FETCHED], refs[FETCHED : FETCHED + 4], refs[FETCHED + 4 :]
    copies, half_ref, many_ref, sems = copies[:FETCHED], *copies[FETCHED:]
    pieces = [(0, x, 4) for x in range(0, BX, 4)] + [(i, 0, None) for i in range(1, FETCHED - 1)]
    pieces += [(FETCHED - 1, x, min(x + 9, CX // 2 + 1) - x) for x in range(0, CX // 2 + 1, 9)]
    fetches = []
    for count, (i, first, size) in enumerate(pieces):
        source, copy = sources[i], copies[i]
        if size:
            source, copy = source.at[pl.ds(first, size)], copy.at[pl.ds(first, size)]
        fetches.append(pltpu.make_async_copy(source, copy, sems.at[count]))
        fetches[-1].start()
    f_ref = copies[0]
    planes = []
    for x in range(MX):
        if x % 2 == 0:
            fetches[x // 2].wait()
        total = None
        for plane in (2 * x, 2 * x + 1):
            for odd in (0, 1):
                part = f_ref[plane, pl.ds(odd, MY, stride=2), :]
                total = part if total is None else total + part
        planes.append(total)
    row, column = lax.broadcasted_iota(jnp.int32, (BZ, 128), 0), lanes((BZ, 128))
    pairs = jnp.where((row >> 1) == column, 1.0 / 8.0, jnp.where((row >> 2) == column - 64, 1.0 / 64.0, 0.0))
    half_ref[...] = exact(jnp.concatenate(planes, axis=0), pairs)
    lane = lanes((8, 128))
    coarse = jnp.zeros((8, 128), F32)
    for x in range(4):
        part = None
        for row in (2 * x * MY, 2 * x * MY + 1, (2 * x + 1) * MY, (2 * x + 1) * MY + 1):
            piece = half_ref[pl.ds(row, 8, stride=2), :]
            part = piece if part is None else part + piece
        coarse = jnp.where((lane >> 5) == x, roll(part, x * 32 - 64), coarse)
    for target in range(GY * GZ):
        many_ref[target] = coarse
    send = pltpu.make_async_copy(many_ref, coarse_ref, sems.at[PIECES])
    send.start()

    slot = lanes((BY, 128)) >> 3
    for group in range(2):
        rising = jnp.zeros((BY, 128), F32)
        falling = jnp.zeros((BY, 128), F32)
        for x in range(8):
            plane = f_ref[group * 8 + x]
            rising = jnp.where(slot == 2 * x, roll(plane, x * 16 - 120), rising)
            falling = jnp.where(slot == 2 * x + 1, roll(plane, x * 16 + 8), falling)
        up_ref[group * BY : (group + 1) * BY, :] = rising
        down_ref[group * BY : (group + 1) * BY, :] = falling
    slot = lanes((MY, 128)) >> 3
    rising = jnp.zeros((MY, 128), F32)
    falling = jnp.zeros((MY, 128), F32)
    middle = []
    for x in range(MX):
        plane = half_ref[x * MY : (x + 1) * MY, :]
        middle.append(plane)
        rising = jnp.where(slot == 2 * x, roll(plane, x * 16 - 56), rising)
        falling = jnp.where(slot == 2 * x + 1, roll(plane, x * 16 + 8), falling)
    up_ref[2 * BY : 2 * BY + MY, :] = rising
    down_ref[2 * BY : 2 * BY + MY, :] = falling
    for x in range(4):
        mid_ref[x] = jnp.where(slot < 8, middle[x], roll(middle[x + 4], 64))
    for fetch in fetches[4:]:
        fetch.wait()
    send.wait()


def modes_kernel(slab_ref, cas_y_ref, twice_y_ref, cas_z_ref, own_z_ref, along_ref, out_ref, modes_ref, wide_ref):
    rows = [jnp.concatenate([slab_ref[gy * GZ + gz] for gz in range(GZ)], axis=1) for gy in range(GY)]
    high, low = halves(jnp.concatenate(rows, axis=0))
    by_y = dot(cas_y_ref[...], jnp.concatenate([high, low, high], axis=0))
    lane = lanes((CY, 128)) >> 5
    planes = []
    for x in range(4):
        plane = jnp.zeros((CY, 128), F32)
        for gz in range(GZ):
            plane = jnp.where(lane == gz, roll(by_y[:, gz * 128 : (gz + 1) * 128], (gz - x) * 32), plane)
        planes.append(plane)
    high, low = halves(jnp.concatenate(planes, axis=0))
    modes_ref[...] = dot(high, cas_z_ref[0]) + dot(low, cas_z_ref[0]) + dot(high, cas_z_ref[1])

    own_y = twice_y_ref[pl.ds(pl.multiple_of(lax.axis_index("gy") * 8, 8), 8), :]
    high, low = halves(own_y)
    low = jnp.where(lanes((8, 128)) < CY, low.astype(F32), 0.0)
    own_y = jnp.concatenate([high.astype(F32), low], axis=0).astype(BF16)
    parts = []
    for first in range(0, CX, 16):
        for start in range(0, CY, 16):
            rows = slice(start, start + 16)
            source = [modes_ref[x * CY + start : x * CY + start + 16, :] for x in range(4)]
            table = [None] + [along_ref[min(abs(first - x), CX - abs(first - x)), rows, :] for x in (1, 2, 3)]
            for place in range(first, first + 16):
                table = [along_ref[min(place, CX - place), rows, :]] + (table[1:] if place == first else table[:3])
                total = table[0] * source[0]
                for x in range(1, 4):
                    total = total + table[x] * source[x]
                high, low = halves(total)
                wide_ref[rows, place * 128 : (place + 1) * 128] = high
                wide_ref[CY + start : CY + start + 16, place * 128 : (place + 1) * 128] = low
        part = dot(own_y, wide_ref[:, first * 128 : (first + 16) * 128])
        parts.append(part[0:8] + part[8:16])
    rows = [part[:, x * 128 : (x + 1) * 128] for part in parts for x in range(16)]
    high, low = halves(jnp.concatenate(rows, axis=0))
    own_z = own_z_ref.at[lax.axis_index("gz")]
    back_z = dot(high, own_z[0]) + dot(low, own_z[0]) + dot(high, own_z[1])
    me = lax.axis_index("gx")
    lane = lanes((8, 128)) >> 5
    for block in range(GX):
        result = back_z[block * 32 : block * 32 + 8]
        for x in range(1, 4):
            result = jnp.where(lane == x, back_z[block * 32 + x * 8 : block * 32 + (x + 1) * 8], result)
        out_ref[lax.rem(me + block, GX)] = result


def y_message_kernel(f_ref, mid_ref, zlow_ref, zhigh_ref, halo_ref, up_ref, down_ref):
    halo = zlow_ref[...] + zhigh_ref[...]
    halo_ref[...] = halo
    for ref, fine, middle in ((up_ref, BY - 8, MY - 8), (down_ref, 0, 0)):
        for x in range(BX):
            ref[x * 8 : x * 8 + 8, :] = f_ref[x, fine : fine + 8, :]
        for group in range(2):
            ref[128 + group * 8 : 136 + group * 8, :] = halo[group * BY + fine : group * BY + fine + 8]
        for x in range(4):
            ref[144 + x * 8 : 152 + x * 8, :] = mid_ref[x, middle : middle + 8, :]
        ref[176:184, :] = halo[2 * BY + middle : 2 * BY + middle + 8]


def own_extended(f_ref, mid_ref, halo_ref, low_ref, high_ref):
    def joined(row, inner):
        return jnp.concatenate([low_ref[row : row + 8, :], inner, high_ref[row : row + 8, :]], axis=0)

    planes = [lambda x=x: joined(x * 8, f_ref[x]) for x in range(BX)]
    sides = [lambda g=g: joined(128 + g * 8, halo_ref[g * BY : (g + 1) * BY, :]) for g in range(2)]
    middle = [lambda x=x: joined(144 + x * 8, mid_ref[x]) for x in range(4)]
    edge = lambda: joined(176, halo_ref[2 * BY : 2 * BY + MY, :])
    return planes, sides, middle, edge


def x_message_kernel(f_ref, mid_ref, halo_ref, low_ref, high_ref, up_ref, down_ref):
    planes, sides, middle, edge = own_extended(f_ref, mid_ref, halo_ref, low_ref, high_ref)
    for ref, first, group in ((up_ref, 8, 1), (down_ref, 0, 0)):
        for x in range(8):
            ref[x * EY : (x + 1) * EY, :] = planes[first + x]()
        ref[8 * EY : 9 * EY, :] = sides[group]()
        for x in range(4):
            ref[9 * EY + x * EMY : 9 * EY + (x + 1) * EMY, :] = middle[x]()
        ref[9 * EY + 4 * EMY : 9 * EY + 5 * EMY, :] = edge()


def filter_yz(planes, sides, gy, gzh_ref, gzl_ref, out_ref, places):
    for group in range(2):
        data = jnp.concatenate([planes[group * 8 + x]() for x in range(8)] + [sides[group]()], axis=1)
        high, low = halves(data)
        by_y = dot(gy, jnp.concatenate([high, low, high], axis=0))
        slot = lanes((BY, 128)) >> 4
        for term in range(TERMS):
            rows = by_y[term * BY : (term + 1) * BY, :]
            side = rows[:, 8 * 128 :]
            left = jnp.concatenate([rows[:, x * 128 : (x + 1) * 128] for x in range(8)], axis=0)
            right = jnp.concatenate([jnp.where(slot == x, side, 0.0) for x in range(8)], axis=0)
            high, low = halves(jnp.concatenate([left, right], axis=1))
            gzh = gzh_ref[term]
            result = dot(high, gzh) + dot(low, gzh) + dot(high, gzl_ref[term])
            for x in range(8):
                out_ref[term, places[group * 8 + x]] = result[x * BY : (x + 1) * BY]


def filter_middle(middle, edge, my, mzh_ref, mzl_ref, out_ref, place):
    slot = lanes((EMY, 128)) >> 3
    rim = edge()
    planes = []
    for x in range(MX):
        plane = middle[x]() if x < 4 else roll(middle[x - 4](), 64)
        rolled = roll(rim, 64 - 16 * x)
        planes.append(jnp.where(slot < 8, plane, jnp.where(slot < 10, rolled, 0.0)))
    high, low = halves(jnp.concatenate(planes, axis=1))
    by_y = dot(my, jnp.concatenate([high, low, high], axis=0))
    for term in range(TERMS):
        rows = by_y[term * MY : (term + 1) * MY, :]
        left = jnp.concatenate([rows[:, x * 128 : (x + 1) * 128] for x in range(MX)], axis=0)
        high, low = halves(left)
        mzh = mzh_ref[term]
        result = dot(high, mzh) + dot(low, mzh) + dot(high, mzl_ref[term])
        for x in range(MX):
            out_ref[term, place + x] = result[x * MY : (x + 1) * MY]


def own_kernel(
    f_ref, mid_ref, halo_ref, low_ref, high_ref, gy_ref, gzh_ref, gzl_ref, my_ref, mzh_ref, mzl_ref, fine_ref, middle_ref
):
    planes, sides, middle, edge = own_extended(f_ref, mid_ref, halo_ref, low_ref, high_ref)
    filter_yz(planes, sides, gy_ref[...], gzh_ref, gzl_ref, fine_ref, list(range(BX)))
    filter_middle(middle, edge, my_ref[...], mzh_ref, mzl_ref, middle_ref, 0)


def near_kernel(
    low_ref, high_ref, fine_ref, middle_ref, gy_ref, gzh_ref, gzl_ref, my_ref, mzh_ref, mzl_ref, cx_ref,
    out_ref, ring_ref, small_ref, add_ref,
):
    planes, sides = [], []
    for ref in (low_ref, high_ref):
        planes += [lambda ref=ref, x=x: ref[x * EY : (x + 1) * EY, :] for x in range(8)]
        sides.append(lambda ref=ref: ref[8 * EY : 9 * EY, :])
    filter_yz(planes, sides, gy_ref[...], gzh_ref, gzl_ref, ring_ref, list(range(16)))
    for index, ref in enumerate((low_ref, high_ref)):
        middle = [lambda ref=ref, x=x: ref[9 * EY + x * EMY : 9 * EY + (x + 1) * EMY, :] for x in range(4)]
        edge = lambda ref=ref: ref[9 * EY + 4 * EMY : 9 * EY + 5 * EMY, :]
        filter_middle(middle, edge, my_ref[...], mzh_ref, mzl_ref, small_ref, index * MX)

    def tap_at(row):
        return jnp.broadcast_to(cx_ref[row : row + 1, :], (8, 128))

    for tile in range(MY // 8):
        sl = slice(tile * 8, tile * 8 + 8)
        acc = [None] * MX
        for term in range(TERMS):
            for place in range(3 * MX):
                if place < MX:
                    value = small_ref[term, place, sl, :]
                elif place < 2 * MX:
                    value = middle_ref[term, place - MX, sl, :]
                else:
                    value = small_ref[term, place - MX, sl, :]
                for x in range(MX):
                    offset = place - x - RADIUS
                    if abs(offset) <= RADIUS:
                        part = tap_at((TERMS + term) * TAPS + abs(offset)) * value
                        acc[x] = part if acc[x] is None else acc[x] + part
        for x in range(MX):
            add_ref[x, pl.ds(tile * 16, 8, stride=2), :] = acc[x]
            add_ref[x, pl.ds(tile * 16 + 1, 8, stride=2), :] = acc[x]

    def tile_step(tile, carry):
        sl = pl.ds(pl.multiple_of(tile * 8, 8), 8)
        acc = [add_ref[x // 2, sl, :] for x in range(BX)]
        for term in range(TERMS):
            for place in range(2 * BX):
                if place < 8:
                    value = ring_ref[term, place, sl, :]
                elif place < 24:
                    value = fine_ref[term, place - 8, sl, :]
                else:
                    value = ring_ref[term, place - 16, sl, :]
                for x in range(BX):
                    offset = place - x - RADIUS
                    if abs(offset) <= RADIUS:
                        acc[x] = acc[x] + tap_at(term * TAPS + abs(offset)) * value
        for x in range(BX):
            out_ref[x, sl, :] = acc[x]
        return carry

    lax.fori_loop(0, BY // 8, tile_step, 0)


def add_kernel(near_ref, top_ref, out_ref, wide_ref, sum_ref, sems):
    top = top_ref[0]
    for source in range(1, GX):
        top = top + top_ref[source]
    shape = (BZ, 4 * BZ)
    row, column = lax.broadcasted_iota(jnp.int32, shape, 0), lanes(shape)
    spread = jnp.where(row == (column >> 7) * 32 + ((column & 127) >> 2), 1.0, 0.0).astype(BF16)
    high, rest = halves(top)
    rest = top - high.astype(F32)
    mid, low = halves(rest)
    parts = dot(jnp.concatenate([high.astype(F32), mid.astype(F32), low.astype(F32)], axis=0).astype(BF16), spread)
    wide = parts[0:8] + parts[8:16] + parts[16:24]
    for row in range(4):
        wide_ref[pl.ds(row, 8, stride=4), :] = wide[:, :128]
        wide_ref[pl.ds(BY + row, 8, stride=4), :] = wide[:, 128:256]
        wide_ref[pl.ds(2 * BY + row, 8, stride=4), :] = wide[:, 256:384]
        wide_ref[pl.ds(3 * BY + row, 8, stride=4), :] = wide[:, 384:512]
    sends = []
    for block in range(4):
        for x in range(4 * block, 4 * block + 4):
            sum_ref[x] = near_ref[x] + wide_ref[block * BY : (block + 1) * BY, :]
        place = pl.ds(4 * block, 4)
        sends.append(pltpu.make_async_copy(sum_ref.at[place], out_ref.at[place], sems.at[block]))
        sends[-1].start()
    for send in sends:
        send.wait()


def call(kernel, outs, args, scratch=(), flops=0, hbm=0, written=0, limit=4):
    vmem = pl.BlockSpec(memory_space=pltpu.VMEM)
    near = len(args) - hbm
    specs = [vmem] * near + [pl.BlockSpec(memory_space=pltpu.HBM)] * hbm
    args = args[:near] + [pltpu.with_memory_space_constraint(a, pltpu.HBM) for a in args[near:]]
    size = sum(a.size * a.dtype.itemsize for a in args)
    return pl.pallas_call(
        kernel,
        out_shape=[jax.ShapeDtypeStruct(shape, dtype) for shape, dtype in outs],
        in_specs=specs,
        out_specs=[pl.BlockSpec(memory_space=pl.ANY)] * written + [vmem] * (len(outs) - written),
        scratch_shapes=list(scratch),
        cost_estimate=pl.CostEstimate(flops=flops, bytes_accessed=size, transcendentals=0),
        compiler_params=pltpu.CompilerParams(vmem_limit_bytes=limit * 1024 * 1024),
    )(*args)


def ring(value, axis, step):
    count = lax.axis_size(axis)
    return lax.ppermute(value, axis, [(i, (i + step) % count) for i in range(count)])


def exchange(value, axis):
    return lax.all_to_all(value, axis, 0, 0, tiled=True)


def potential(charges, term_width, term_weight):
    sources = [charges, term_width, term_weight] + constant_tables()
    coarse, mid, z_up, z_down, charges, term_width, term_weight, *tables = call(
        restrict_kernel,
        [((GY * GZ, 8, 128), F32), ((4, MY, 128), F32), ((ZROWS, 128), F32), ((ZROWS, 128), F32)]
        + [(a.shape, a.dtype) for a in sources],
        sources,
        [
            pltpu.VMEM((MX * MY, 128), F32),
            pltpu.VMEM((GY * GZ, 8, 128), F32),
            pltpu.SemaphoreType.DMA((PIECES + 1,)),
        ],
        flops=10**7,
        hbm=FETCHED,
        written=1,
    )
    slab = exchange(coarse, ("gy", "gz"))
    z_low, z_high = ring(z_up, "gz", 1), ring(z_down, "gz", -1)
    gy, gzh, gzl, my, mzh, mzl, cx = call(
        weights_kernel,
        [
            ((TERMS * BY, 3 * EY), BF16),
            ((TERMS, 256, 128), BF16),
            ((TERMS, 256, 128), BF16),
            ((TERMS * MY, 3 * EMY), BF16),
            ((TERMS, 128, 128), BF16),
            ((TERMS, 128, 128), BF16),
            ((2 * TERMS * TAPS, 128), F32),
        ],
        [term_width, term_weight],
        flops=10**7,
    )
    bands = [gy, gzh, gzl, my, mzh, mzl]
    halo, y_up, y_down = call(
        y_message_kernel,
        [((ZROWS, 128), F32), ((YROWS, 128), F32), ((YROWS, 128), F32)],
        [charges, mid, z_low, z_high],
        flops=10**6,
    )
    low, high = ring(y_up, "gy", 1), ring(y_down, "gy", -1)
    (partial,) = call(
        modes_kernel,
        [((GX, 8, 128), F32)],
        [slab] + tables,
        [pltpu.VMEM((4 * CY, 128), F32), pltpu.VMEM((2 * CY, CX * 128), BF16)],
        flops=5 * 10**7,
        limit=8,
    )
    top = exchange(partial, "gx")
    x_up, x_down = call(
        x_message_kernel, [((XROWS, 128), F32), ((XROWS, 128), F32)], [charges, mid, halo, low, high], flops=10**6
    )
    x_low, x_high = ring(x_up, "gx", 1), ring(x_down, "gx", -1)
    fine, middle = call(
        own_kernel,
        [((TERMS, BX, BY, 128), F32), ((TERMS, MX, MY, 128), F32)],
        [charges, mid, halo, low, high] + bands,
        flops=10**8,
        limit=8,
    )
    (near,) = call(
        near_kernel,
        [((BX, BY, BZ), F32)],
        [x_low, x_high, fine, middle] + bands + [cx],
        [
            pltpu.VMEM((TERMS, 16, BY, 128), F32),
            pltpu.VMEM((TERMS, 16, MY, 128), F32),
            pltpu.VMEM((MX, BY, 128), F32),
        ],
        flops=10**8,
        limit=10,
    )
    (result,) = call(
        add_kernel,
        [((BX, BY, BZ), F32)],
        [near, top],
        [pltpu.VMEM((4 * BY, 128), F32), pltpu.VMEM((BX, BY, BZ), F32), pltpu.SemaphoreType.DMA((4,))],
        flops=10**6,
        written=1,
    )
    return result


def solution(mesh):
    placed = (P("gx", "gy", "gz"), P(), P())
    return jax.shard_map(potential, mesh=mesh, in_specs=placed, out_specs=P("gx", "gy", "gz"), check_vma=False)
```

```python
import math

import jax
import jax.numpy as jnp
import numpy as np
from jax import lax
from jax.experimental import pallas as pl
from jax.experimental.pallas import tpu as pltpu
from jax.sharding import PartitionSpec as P


TERMS = 4
RADIUS = 8
TAPS = RADIUS + 1

HIGHEST = lax.Precision.HIGHEST
F32 = jnp.float32
BF16 = jnp.bfloat16
screening = 0.01
strength = 4.0

BX, BY, BZ = 16, 32, 128
MX, MY, MZ = 8, 16, 64
CX, CY, CZ = 64, 64, 128
EY, EMY = BY + 2 * RADIUS, MY + 2 * RADIUS
GX, GY, GZ = 16, 8, 4
FETCHED, PIECES = 8, 14
ZROWS = 2 * BY + MY
YROWS = BX * 8 + 2 * 8 + 5 * 8
XROWS = 8 * EY + EY + 5 * EMY


def cas_table(count):
    modes = np.arange(count)
    angles = 2.0 * math.pi / count * (np.outer(modes, modes) % count)
    return np.cos(angles) + np.sin(angles)


def constant_tables():
    cas_y, cas_z = cas_table(CY), cas_table(CZ)

    def lam(count):
        return 2.0 - 2.0 * np.cos(2.0 * math.pi / count * np.arange(count))

    total = lam(CX)[:, None, None] + lam(CY)[None, :, None] + lam(CZ)[None, None, :]
    mult = strength * np.exp(-total) / (total + screening)
    mult[0, 0, 0] = 0.0
    shifts = np.arange(CX // 2 + 1)
    cosine = np.cos(2.0 * math.pi / CX * (np.outer(shifts, np.arange(CX)) % CX))
    along_x = np.einsum("dm,myz->dyz", cosine, mult) / (CX * CY * CZ)
    own_z = np.stack([np.tile(cas_z[32 * g : 32 * g + 32], (4, 1)) for g in range(GZ)])
    own_y = np.stack([cas_y[:, 8 * g : 8 * g + 8] for g in range(GY)])

    def split(table):
        table = np.asarray(table, np.float32)
        high = table.astype(BF16)
        return high, (table - high.astype(np.float32)).astype(BF16)

    high, low = split(cas_y)
    own_high, own_low = split(own_y)
    tables = [
        np.concatenate([high, high, low], axis=1),
        np.concatenate([own_high, own_high, own_low, np.zeros_like(own_low)], axis=2),
        np.stack(split(cas_z)),
        np.stack(split(own_z), axis=1),
        np.asarray(along_x, np.float32),
    ]
    return [jnp.asarray(table) for table in tables]


def lanes(shape):
    return lax.broadcasted_iota(jnp.int32, shape, len(shape) - 1)


def roll(value, shift):
    shift %= 128
    return pltpu.roll(value, shift, 1) if shift else value


def dot(a, b):
    return jnp.dot(a, b, preferred_element_type=F32)


def exact(a, b):
    return jnp.dot(a, b, preferred_element_type=F32, precision=HIGHEST)


def halves(value):
    high = value.astype(BF16)
    return high, (value - high.astype(F32)).astype(BF16)


def weights_kernel(width_ref, weight_ref, gy_ref, gzh_ref, gzl_ref, my_ref, mzh_ref, mzl_ref, cx_ref):
    offset = lanes((8, 128)) - RADIUS
    squares = (offset * offset).astype(F32)

    def scale(level, term):
        width = jnp.broadcast_to(width_ref[level : level + 1, term : term + 1], (8, 128))
        inverse = -1.0 / (2.0 * width * width)
        values = jnp.where(offset <= RADIUS, jnp.exp(squares * inverse), 0.0)
        norm = 1.0 / jnp.broadcast_to(jnp.sum(values, axis=1, keepdims=True), (8, 128))
        weight = jnp.broadcast_to(weight_ref[level : level + 1, term : term + 1], (8, 128))
        for distance in range(TAPS):
            value = jnp.exp(float(distance * distance) * inverse) * norm * weight
            row = (level * TERMS + term) * TAPS + distance
            cx_ref[row : row + 1, :] = value[0:1, :]
        return inverse, norm

    def taps(place, inverse, norm):
        rows, columns = place.shape
        inverse, norm = [
            jnp.concatenate([jnp.concatenate([v] * (columns // 128), axis=1)] * (rows // 8), axis=0) for v in (inverse, norm)
        ]
        values = jnp.exp((place * place).astype(F32) * inverse) * norm
        return jnp.where(jnp.abs(place) <= RADIUS, values, 0.0)

    def along_y(ref, term, inverse, norm, out, ext):
        shape = (out, 256 if 3 * ext > 128 else 128)
        column = lanes(shape)
        row = lax.broadcasted_iota(jnp.int32, shape, 0)
        part = (column >= ext).astype(jnp.int32) + (column >= 2 * ext).astype(jnp.int32)
        high, low = halves(taps(column - part * ext - RADIUS - row, inverse, norm))
        both = jnp.where(part < 2, high.astype(F32), low.astype(F32))
        ref[term * out : (term + 1) * out, :] = both[:, : 3 * ext].astype(BF16)

    for term in range(TERMS):
        inverse, norm = scale(0, term)
        along_y(gy_ref, term, inverse, norm, BY, EY)
        shape = (256, 128)
        row = lax.broadcasted_iota(jnp.int32, shape, 0)
        slot = row & 15
        place = jnp.where(row < BZ, row, jnp.where(slot < 8, slot - 8, BZ - 8 + slot))
        high, low = halves(taps(place - lanes(shape), inverse, norm))
        gzh_ref[term] = high
        gzl_ref[term] = low

        inverse, norm = scale(1, term)
        along_y(my_ref, term, inverse, norm, MY, EMY)
        shape = (128, 128)
        row = lax.broadcasted_iota(jnp.int32, shape, 0)
        place = jnp.where(row < MZ, row, jnp.where(row < MZ + 8, row - MZ - 8, row - 8))
        values = taps(place - (lanes(shape) >> 1), inverse, norm)
        high, low = halves(jnp.where(row < MZ + 16, values, 0.0))
        mzh_ref[term] = high
        mzl_ref[term] = low


def restrict_kernel(*refs):
    sources, (coarse_ref, mid_ref, up_ref, down_ref), copies = refs[:FETCHED], refs[FETCHED : FETCHED + 4], refs[FETCHED + 4 :]
    copies, half_ref, many_ref, sems = copies[:FETCHED], *copies[FETCHED:]
    pieces = [(0, x, 4) for x in range(0, BX, 4)] + [(i, 0, None) for i in range(1, FETCHED - 1)]
    pieces += [(FETCHED - 1, x, min(x + 9, CX // 2 + 1) - x) for x in range(0, CX // 2 + 1, 9)]
    fetches = []
    for count, (i, first, size) in enumerate(pieces):
        source, copy = sources[i], copies[i]
        if size:
            source, copy = source.at[pl.ds(first, size)], copy.at[pl.ds(first, size)]
        fetches.append(pltpu.make_async_copy(source, copy, sems.at[count]))
        fetches[-1].start()
    f_ref = copies[0]
    planes = []
    for x in range(MX):
        if x % 2 == 0:
            fetches[x // 2].wait()
        total = None
        for plane in (2 * x, 2 * x + 1):
            for odd in (0, 1):
                part = f_ref[plane, pl.ds(odd, MY, stride=2), :]
                total = part if total is None else total + part
        planes.append(total)
    row, column = lax.broadcasted_iota(jnp.int32, (BZ, 128), 0), lanes((BZ, 128))
    pairs = jnp.where((row >> 1) == column, 1.0 / 8.0, jnp.where((row >> 2) == column - 64, 1.0 / 64.0, 0.0))
    half_ref[...] = exact(jnp.concatenate(planes, axis=0), pairs)
    lane = lanes((8, 128))
    coarse = jnp.zeros((8, 128), F32)
    for x in range(4):
        part = None
        for row in (2 * x * MY, 2 * x * MY + 1, (2 * x + 1) * MY, (2 * x + 1) * MY + 1):
            piece = half_ref[pl.ds(row, 8, stride=2), :]
            part = piece if part is None else part + piece
        coarse = jnp.where((lane >> 5) == x, roll(part, x * 32 - 64), coarse)
    for target in range(GX):
        many_ref[target] = coarse
    send = pltpu.make_async_copy(many_ref, coarse_ref, sems.at[PIECES])
    send.start()

    slot = lanes((BY, 128)) >> 3
    for group in range(2):
        rising = jnp.zeros((BY, 128), F32)
        falling = jnp.zeros((BY, 128), F32)
        for x in range(8):
            plane = f_ref[group * 8 + x]
            rising = jnp.where(slot == 2 * x, roll(plane, x * 16 - 120), rising)
            falling = jnp.where(slot == 2 * x + 1, roll(plane, x * 16 + 8), falling)
        up_ref[group * BY : (group + 1) * BY, :] = rising
        down_ref[group * BY : (group + 1) * BY, :] = falling
    slot = lanes((MY, 128)) >> 3
    rising = jnp.zeros((MY, 128), F32)
    falling = jnp.zeros((MY, 128), F32)
    middle = []
    for x in range(MX):
        plane = half_ref[x * MY : (x + 1) * MY, :]
        middle.append(plane)
        rising = jnp.where(slot == 2 * x, roll(plane, x * 16 - 56), rising)
        falling = jnp.where(slot == 2 * x + 1, roll(plane, x * 16 + 8), falling)
    up_ref[2 * BY : 2 * BY + MY, :] = rising
    down_ref[2 * BY : 2 * BY + MY, :] = falling
    for x in range(4):
        mid_ref[x] = jnp.where(slot < 8, middle[x], roll(middle[x + 4], 64))
    for fetch in fetches[4:]:
        fetch.wait()
    send.wait()


def modes_kernel(columns_ref, cas_y_ref, own_y_ref, cas_z_ref, own_z_ref, along_ref, out_ref, modes_ref):
    me = lax.axis_index("gx")
    rows = jnp.concatenate([columns_ref[lax.rem(me + block, GX)] for block in range(GX)], axis=0)
    lane = lanes((GX * 8, 128)) >> 5
    high, low = halves(jnp.concatenate([jnp.where(lane == x, rows, 0.0) for x in range(4)], axis=0))
    own_z = own_z_ref.at[lax.axis_index("gz")]
    by_z = dot(high, own_z[0]) + dot(low, own_z[0]) + dot(high, own_z[1])
    ordered = [by_z[(x * GX + block) * 8 : (x * GX + block + 1) * 8] for block in range(GX) for x in range(4)]
    own_y = own_y_ref[lax.axis_index("gy")]
    for first in range(0, CX, 16):
        data = jnp.concatenate(ordered[first : first + 16], axis=1)
        high = data.astype(BF16).astype(F32)
        stacked = jnp.concatenate([high, data - high, high, jnp.zeros_like(high)], axis=0).astype(BF16)
        modes_ref[:, first * 128 : (first + 16) * 128] = dot(own_y, stacked)

    outs = [[] for _ in range(4)]
    for start in range(0, CY, 8):
        rows = slice(start, start + 8)
        total = [None] * 4
        table = [along_ref[shift, rows, :] for shift in (0, 1, 2, 3)]
        for place in range(CX):
            if place:
                table = [along_ref[min(place, CX - place), rows, :]] + table[:3]
            value = modes_ref[rows, place * 128 : (place + 1) * 128]
            for x in range(4):
                part = table[x] * value
                total[x] = part if total[x] is None else total[x] + part
        for x in range(4):
            outs[x].append(total[x])
    high, low = halves(jnp.concatenate([tile for x in range(4) for tile in outs[x]], axis=0))
    back_z = dot(high, cas_z_ref[0]) + dot(low, cas_z_ref[0]) + dot(high, cas_z_ref[1])
    high, low = halves(jnp.concatenate([back_z[x * CY : (x + 1) * CY] for x in range(4)], axis=1))
    back_y = dot(cas_y_ref[...], jnp.concatenate([high, low, high], axis=0))
    lane = lanes((CY, 128)) >> 5
    for gz in range(GZ):
        result = jnp.zeros((CY, 128), F32)
        for x in range(4):
            result = jnp.where(lane == x, roll(back_y[:, x * 128 : (x + 1) * 128], (x - gz) * 32), result)
        for gy in range(GY):
            out_ref[gy * GZ + gz] = result[gy * 8 : gy * 8 + 8]


def y_message_kernel(f_ref, mid_ref, zlow_ref, zhigh_ref, halo_ref, up_ref, down_ref):
    halo = zlow_ref[...] + zhigh_ref[...]
    halo_ref[...] = halo
    for ref, fine, middle in ((up_ref, BY - 8, MY - 8), (down_ref, 0, 0)):
        for x in range(BX):
            ref[x * 8 : x * 8 + 8, :] = f_ref[x, fine : fine + 8, :]
        for group in range(2):
            ref[128 + group * 8 : 136 + group * 8, :] = halo[group * BY + fine : group * BY + fine + 8]
        for x in range(4):
            ref[144 + x * 8 : 152 + x * 8, :] = mid_ref[x, middle : middle + 8, :]
        ref[176:184, :] = halo[2 * BY + middle : 2 * BY + middle + 8]


def own_extended(f_ref, mid_ref, halo_ref, low_ref, high_ref):
    def joined(row, inner):
        return jnp.concatenate([low_ref[row : row + 8, :], inner, high_ref[row : row + 8, :]], axis=0)

    planes = [lambda x=x: joined(x * 8, f_ref[x]) for x in range(BX)]
    sides = [lambda g=g: joined(128 + g * 8, halo_ref[g * BY : (g + 1) * BY, :]) for g in range(2)]
    middle = [lambda x=x: joined(144 + x * 8, mid_ref[x]) for x in range(4)]
    edge = lambda: joined(176, halo_ref[2 * BY : 2 * BY + MY, :])
    return planes, sides, middle, edge


def x_message_kernel(f_ref, mid_ref, halo_ref, low_ref, high_ref, up_ref, down_ref):
    planes, sides, middle, edge = own_extended(f_ref, mid_ref, halo_ref, low_ref, high_ref)
    for ref, first, group in ((up_ref, 8, 1), (down_ref, 0, 0)):
        for x in range(8):
            ref[x * EY : (x + 1) * EY, :] = planes[first + x]()
        ref[8 * EY : 9 * EY, :] = sides[group]()
        for x in range(4):
            ref[9 * EY + x * EMY : 9 * EY + (x + 1) * EMY, :] = middle[x]()
        ref[9 * EY + 4 * EMY : 9 * EY + 5 * EMY, :] = edge()


def filter_yz(planes, sides, gy, gzh_ref, gzl_ref, out_ref, places):
    for group in range(2):
        data = jnp.concatenate([planes[group * 8 + x]() for x in range(8)] + [sides[group]()], axis=1)
        high, low = halves(data)
        by_y = dot(gy, jnp.concatenate([high, low, high], axis=0))
        slot = lanes((BY, 128)) >> 4
        for term in range(TERMS):
            rows = by_y[term * BY : (term + 1) * BY, :]
            side = rows[:, 8 * 128 :]
            left = jnp.concatenate([rows[:, x * 128 : (x + 1) * 128] for x in range(8)], axis=0)
            right = jnp.concatenate([jnp.where(slot == x, side, 0.0) for x in range(8)], axis=0)
            high, low = halves(jnp.concatenate([left, right], axis=1))
            gzh = gzh_ref[term]
            result = dot(high, gzh) + dot(low, gzh) + dot(high, gzl_ref[term])
            for x in range(8):
                out_ref[term, places[group * 8 + x]] = result[x * BY : (x + 1) * BY]


def filter_middle(middle, edge, my, mzh_ref, mzl_ref, out_ref, place):
    slot = lanes((EMY, 128)) >> 3
    rim = edge()
    planes = []
    for x in range(MX):
        plane = middle[x]() if x < 4 else roll(middle[x - 4](), 64)
        rolled = roll(rim, 64 - 16 * x)
        planes.append(jnp.where(slot < 8, plane, jnp.where(slot < 10, rolled, 0.0)))
    high, low = halves(jnp.concatenate(planes, axis=1))
    by_y = dot(my, jnp.concatenate([high, low, high], axis=0))
    for term in range(TERMS):
        rows = by_y[term * MY : (term + 1) * MY, :]
        left = jnp.concatenate([rows[:, x * 128 : (x + 1) * 128] for x in range(MX)], axis=0)
        high, low = halves(left)
        mzh = mzh_ref[term]
        result = dot(high, mzh) + dot(low, mzh) + dot(high, mzl_ref[term])
        for x in range(MX):
            out_ref[term, place + x] = result[x * MY : (x + 1) * MY]


def own_kernel(
    f_ref, mid_ref, halo_ref, low_ref, high_ref, gy_ref, gzh_ref, gzl_ref, my_ref, mzh_ref, mzl_ref, fine_ref, middle_ref
):
    planes, sides, middle, edge = own_extended(f_ref, mid_ref, halo_ref, low_ref, high_ref)
    filter_yz(planes, sides, gy_ref[...], gzh_ref, gzl_ref, fine_ref, list(range(BX)))
    filter_middle(middle, edge, my_ref[...], mzh_ref, mzl_ref, middle_ref, 0)


def near_kernel(
    low_ref, high_ref, fine_ref, middle_ref, gy_ref, gzh_ref, gzl_ref, my_ref, mzh_ref, mzl_ref, cx_ref,
    out_ref, ring_ref, small_ref, add_ref,
):
    planes, sides = [], []
    for ref in (low_ref, high_ref):
        planes += [lambda ref=ref, x=x: ref[x * EY : (x + 1) * EY, :] for x in range(8)]
        sides.append(lambda ref=ref: ref[8 * EY : 9 * EY, :])
    filter_yz(planes, sides, gy_ref[...], gzh_ref, gzl_ref, ring_ref, list(range(16)))
    for index, ref in enumerate((low_ref, high_ref)):
        middle = [lambda ref=ref, x=x: ref[9 * EY + x * EMY : 9 * EY + (x + 1) * EMY, :] for x in range(4)]
        edge = lambda ref=ref: ref[9 * EY + 4 * EMY : 9 * EY + 5 * EMY, :]
        filter_middle(middle, edge, my_ref[...], mzh_ref, mzl_ref, small_ref, index * MX)

    def tap_at(row):
        return jnp.broadcast_to(cx_ref[row : row + 1, :], (8, 128))

    for tile in range(MY // 8):
        sl = slice(tile * 8, tile * 8 + 8)
        acc = [None] * MX
        for term in range(TERMS):
            for place in range(3 * MX):
                if place < MX:
                    value = small_ref[term, place, sl, :]
                elif place < 2 * MX:
                    value = middle_ref[term, place - MX, sl, :]
                else:
                    value = small_ref[term, place - MX, sl, :]
                for x in range(MX):
                    offset = place - x - RADIUS
                    if abs(offset) <= RADIUS:
                        part = tap_at((TERMS + term) * TAPS + abs(offset)) * value
                        acc[x] = part if acc[x] is None else acc[x] + part
        for x in range(MX):
            add_ref[x, pl.ds(tile * 16, 8, stride=2), :] = acc[x]
            add_ref[x, pl.ds(tile * 16 + 1, 8, stride=2), :] = acc[x]

    def tile_step(tile, carry):
        sl = pl.ds(pl.multiple_of(tile * 8, 8), 8)
        acc = [add_ref[x // 2, sl, :] for x in range(BX)]
        for term in range(TERMS):
            for place in range(2 * BX):
                if place < 8:
                    value = ring_ref[term, place, sl, :]
                elif place < 24:
                    value = fine_ref[term, place - 8, sl, :]
                else:
                    value = ring_ref[term, place - 16, sl, :]
                for x in range(BX):
                    offset = place - x - RADIUS
                    if abs(offset) <= RADIUS:
                        acc[x] = acc[x] + tap_at(term * TAPS + abs(offset)) * value
        for x in range(BX):
            out_ref[x, sl, :] = acc[x]
        return carry

    lax.fori_loop(0, BY // 8, tile_step, 0)


def add_kernel(near_ref, top_ref, out_ref, wide_ref, sum_ref, sems):
    top = top_ref[0]
    for source in range(1, GY * GZ):
        top = top + top_ref[source]
    shape = (BZ, 4 * BZ)
    row, column = lax.broadcasted_iota(jnp.int32, shape, 0), lanes(shape)
    spread = jnp.where(row == (column >> 7) * 32 + ((column & 127) >> 2), 1.0, 0.0).astype(BF16)
    high, rest = halves(top)
    rest = top - high.astype(F32)
    mid, low = halves(rest)
    parts = dot(jnp.concatenate([high.astype(F32), mid.astype(F32), low.astype(F32)], axis=0).astype(BF16), spread)
    wide = parts[0:8] + parts[8:16] + parts[16:24]
    for row in range(4):
        wide_ref[pl.ds(row, 8, stride=4), :] = wide[:, :128]
        wide_ref[pl.ds(BY + row, 8, stride=4), :] = wide[:, 128:256]
        wide_ref[pl.ds(2 * BY + row, 8, stride=4), :] = wide[:, 256:384]
        wide_ref[pl.ds(3 * BY + row, 8, stride=4), :] = wide[:, 384:512]
    sends = []
    for block in range(4):
        for x in range(4 * block, 4 * block + 4):
            sum_ref[x] = near_ref[x] + wide_ref[block * BY : (block + 1) * BY, :]
        place = pl.ds(4 * block, 4)
        sends.append(pltpu.make_async_copy(sum_ref.at[place], out_ref.at[place], sems.at[block]))
        sends[-1].start()
    for send in sends:
        send.wait()


def call(kernel, outs, args, scratch=(), flops=0, hbm=0, written=0, limit=4):
    vmem = pl.BlockSpec(memory_space=pltpu.VMEM)
    near = len(args) - hbm
    specs = [vmem] * near + [pl.BlockSpec(memory_space=pltpu.HBM)] * hbm
    args = args[:near] + [pltpu.with_memory_space_constraint(a, pltpu.HBM) for a in args[near:]]
    size = sum(a.size * a.dtype.itemsize for a in args)
    return pl.pallas_call(
        kernel,
        out_shape=[jax.ShapeDtypeStruct(shape, dtype) for shape, dtype in outs],
        in_specs=specs,
        out_specs=[pl.BlockSpec(memory_space=pl.ANY)] * written + [vmem] * (len(outs) - written),
        scratch_shapes=list(scratch),
        cost_estimate=pl.CostEstimate(flops=flops, bytes_accessed=size, transcendentals=0),
        compiler_params=pltpu.CompilerParams(vmem_limit_bytes=limit * 1024 * 1024),
    )(*args)


def ring(value, axis, step):
    count = lax.axis_size(axis)
    return lax.ppermute(value, axis, [(i, (i + step) % count) for i in range(count)])


def exchange(value, axis):
    return lax.all_to_all(value, axis, 0, 0, tiled=True)


def potential(charges, term_width, term_weight):
    sources = [charges, term_width, term_weight] + constant_tables()
    coarse, mid, z_up, z_down, charges, term_width, term_weight, *tables = call(
        restrict_kernel,
        [((GX, 8, 128), F32), ((4, MY, 128), F32), ((ZROWS, 128), F32), ((ZROWS, 128), F32)]
        + [(a.shape, a.dtype) for a in sources],
        sources,
        [
            pltpu.VMEM((MX * MY, 128), F32),
            pltpu.VMEM((GX, 8, 128), F32),
            pltpu.SemaphoreType.DMA((PIECES + 1,)),
        ],
        flops=10**7,
        hbm=FETCHED,
        written=1,
    )
    columns = exchange(coarse, "gx")
    z_low, z_high = ring(z_up, "gz", 1), ring(z_down, "gz", -1)
    gy, gzh, gzl, my, mzh, mzl, cx = call(
        weights_kernel,
        [
            ((TERMS * BY, 3 * EY), BF16),
            ((TERMS, 256, 128), BF16),
            ((TERMS, 256, 128), BF16),
            ((TERMS * MY, 3 * EMY), BF16),
            ((TERMS, 128, 128), BF16),
            ((TERMS, 128, 128), BF16),
            ((2 * TERMS * TAPS, 128), F32),
        ],
        [term_width, term_weight],
        flops=10**7,
    )
    bands = [gy, gzh, gzl, my, mzh, mzl]
    halo, y_up, y_down = call(
        y_message_kernel,
        [((ZROWS, 128), F32), ((YROWS, 128), F32), ((YROWS, 128), F32)],
        [charges, mid, z_low, z_high],
        flops=10**6,
    )
    low, high = ring(y_up, "gy", 1), ring(y_down, "gy", -1)
    (partial,) = call(
        modes_kernel,
        [((GY * GZ, 8, 128), F32)],
        [columns] + tables,
        [pltpu.VMEM((CY, CX * 128), F32)],
        flops=5 * 10**7,
        limit=8,
    )
    top = exchange(partial, ("gy", "gz"))
    x_up, x_down = call(
        x_message_kernel, [((XROWS, 128), F32), ((XROWS, 128), F32)], [charges, mid, halo, low, high], flops=10**6
    )
    x_low, x_high = ring(x_up, "gx", 1), ring(x_down, "gx", -1)
    fine, middle = call(
        own_kernel,
        [((TERMS, BX, BY, 128), F32), ((TERMS, MX, MY, 128), F32)],
        [charges, mid, halo, low, high] + bands,
        flops=10**8,
        limit=8,
    )
    (near,) = call(
        near_kernel,
        [((BX, BY, BZ), F32)],
        [x_low, x_high, fine, middle] + bands + [cx],
        [
            pltpu.VMEM((TERMS, 16, BY, 128), F32),
            pltpu.VMEM((TERMS, 16, MY, 128), F32),
            pltpu.VMEM((MX, BY, 128), F32),
        ],
        flops=10**8,
        limit=10,
    )
    (result,) = call(
        add_kernel,
        [((BX, BY, BZ), F32)],
        [near, top],
        [pltpu.VMEM((4 * BY, 128), F32), pltpu.VMEM((BX, BY, BZ), F32), pltpu.SemaphoreType.DMA((4,))],
        flops=10**6,
        written=1,
    )
    return result


def solution(mesh):
    placed = (P("gx", "gy", "gz"), P(), P())
    return jax.shard_map(potential, mesh=mesh, in_specs=placed, out_specs=P("gx", "gy", "gz"), check_vma=False)
```

```python
import math

import jax
import jax.numpy as jnp
import numpy as np
from jax import lax
from jax.experimental import pallas as pl
from jax.experimental.pallas import tpu as pltpu
from jax.sharding import PartitionSpec as P


TERMS = 4
RADIUS = 8
TAPS = RADIUS + 1

HIGHEST = lax.Precision.HIGHEST
F32 = jnp.float32
BF16 = jnp.bfloat16
screening = 0.01
strength = 4.0

BX, BY, BZ = 16, 32, 128
MX, MY, MZ = 8, 16, 64
CX, CY, CZ = 64, 64, 128
EY, EMY = BY + 2 * RADIUS, MY + 2 * RADIUS
GX, GY, GZ = 16, 8, 4
FETCHED, PIECES = 8, 14
ZROWS = 2 * BY + MY
YROWS = BX * 8 + 2 * 8 + 5 * 8
XROWS = 8 * EY + EY + 5 * EMY


def cas_table(count):
    modes = np.arange(count)
    angles = 2.0 * math.pi / count * (np.outer(modes, modes) % count)
    return np.cos(angles) + np.sin(angles)


def constant_tables():
    cas_y, cas_z = cas_table(CY), cas_table(CZ)

    def lam(count):
        return 2.0 - 2.0 * np.cos(2.0 * math.pi / count * np.arange(count))

    total = lam(CX)[:, None, None] + lam(CY)[None, :, None] + lam(CZ)[None, None, :]
    mult = strength * np.exp(-total) / (total + screening)
    mult[0, 0, 0] = 0.0
    shifts = np.arange(CX // 2 + 1)
    cosine = np.cos(2.0 * math.pi / CX * (np.outer(shifts, np.arange(CX)) % CX))
    along_x = np.einsum("dm,myz->dyz", cosine, mult) / (CX * CY * CZ)
    own_z = np.stack([np.tile(cas_z[32 * g : 32 * g + 32], (4, 1)) for g in range(GZ)])
    own_y = np.stack([cas_y[:, 8 * g : 8 * g + 8] for g in range(GY)])

    def split(table):
        table = np.asarray(table, np.float32)
        high = table.astype(BF16)
        return high, (table - high.astype(np.float32)).astype(BF16)

    high, low = split(cas_y)
    own_high, own_low = split(own_y)
    tables = [
        np.concatenate([high, high, low], axis=1),
        np.concatenate([own_high, own_high, own_low, np.zeros_like(own_low)], axis=2),
        np.stack(split(cas_z)),
        np.stack(split(own_z), axis=1),
        np.asarray(along_x, np.float32),
    ]
    return [jnp.asarray(table) for table in tables]


def lanes(shape):
    return lax.broadcasted_iota(jnp.int32, shape, len(shape) - 1)


def roll(value, shift):
    shift %= 128
    return pltpu.roll(value, shift, 1) if shift else value


def dot(a, b):
    return jnp.dot(a, b, preferred_element_type=F32)


def exact(a, b):
    return jnp.dot(a, b, preferred_element_type=F32, precision=HIGHEST)


def halves(value):
    high = value.astype(BF16)
    return high, (value - high.astype(F32)).astype(BF16)


def weights_kernel(width_ref, weight_ref, gy_ref, gzh_ref, gzl_ref, my_ref, mzh_ref, mzl_ref, cx_ref):
    offset = lanes((8, 128)) - RADIUS
    squares = (offset * offset).astype(F32)

    def scale(level, term):
        width = jnp.broadcast_to(width_ref[level : level + 1, term : term + 1], (8, 128))
        inverse = -1.0 / (2.0 * width * width)
        values = jnp.where(offset <= RADIUS, jnp.exp(squares * inverse), 0.0)
        norm = 1.0 / jnp.broadcast_to(jnp.sum(values, axis=1, keepdims=True), (8, 128))
        weight = jnp.broadcast_to(weight_ref[level : level + 1, term : term + 1], (8, 128))
        for distance in range(TAPS):
            value = jnp.exp(float(distance * distance) * inverse) * norm * weight
            row = (level * TERMS + term) * TAPS + distance
            cx_ref[row : row + 1, :] = value[0:1, :]
        return inverse, norm

    def taps(place, inverse, norm):
        rows, columns = place.shape
        inverse, norm = [
            jnp.concatenate([jnp.concatenate([v] * (columns // 128), axis=1)] * (rows // 8), axis=0) for v in (inverse, norm)
        ]
        values = jnp.exp((place * place).astype(F32) * inverse) * norm
        return jnp.where(jnp.abs(place) <= RADIUS, values, 0.0)

    def along_y(ref, term, inverse, norm, out, ext):
        shape = (out, 256 if 3 * ext > 128 else 128)
        column = lanes(shape)
        row = lax.broadcasted_iota(jnp.int32, shape, 0)
        part = (column >= ext).astype(jnp.int32) + (column >= 2 * ext).astype(jnp.int32)
        high, low = halves(taps(column - part * ext - RADIUS - row, inverse, norm))
        both = jnp.where(part < 2, high.astype(F32), low.astype(F32))
        ref[term * out : (term + 1) * out, :] = both[:, : 3 * ext].astype(BF16)

    for term in range(TERMS):
        inverse, norm = scale(0, term)
        along_y(gy_ref, term, inverse, norm, BY, EY)
        shape = (256, 128)
        row = lax.broadcasted_iota(jnp.int32, shape, 0)
        slot = row & 15
        place = jnp.where(row < BZ, row, jnp.where(slot < 8, slot - 8, BZ - 8 + slot))
        high, low = halves(taps(place - lanes(shape), inverse, norm))
        gzh_ref[term] = high
        gzl_ref[term] = low

        inverse, norm = scale(1, term)
        along_y(my_ref, term, inverse, norm, MY, EMY)
        shape = (128, 128)
        row = lax.broadcasted_iota(jnp.int32, shape, 0)
        place = jnp.where(row < MZ, row, jnp.where(row < MZ + 8, row - MZ - 8, row - 8))
        values = taps(place - (lanes(shape) >> 1), inverse, norm)
        high, low = halves(jnp.where(row < MZ + 16, values, 0.0))
        mzh_ref[term] = high
        mzl_ref[term] = low


def restrict_kernel(*refs):
    sources, (coarse_ref, mid_ref, up_ref, down_ref), copies = refs[:FETCHED], refs[FETCHED : FETCHED + 4], refs[FETCHED + 4 :]
    copies, half_ref, many_ref, sems = copies[:FETCHED], *copies[FETCHED:]
    pieces = [(0, x, 4) for x in range(0, BX, 4)] + [(i, 0, None) for i in range(1, FETCHED - 1)]
    pieces += [(FETCHED - 1, x, min(x + 9, CX // 2 + 1) - x) for x in range(0, CX // 2 + 1, 9)]
    fetches = []
    for count, (i, first, size) in enumerate(pieces):
        source, copy = sources[i], copies[i]
        if size:
            source, copy = source.at[pl.ds(first, size)], copy.at[pl.ds(first, size)]
        fetches.append(pltpu.make_async_copy(source, copy, sems.at[count]))
        fetches[-1].start()
    f_ref = copies[0]
    planes = []
    for x in range(MX):
        if x % 2 == 0:
            fetches[x // 2].wait()
        total = None
        for plane in (2 * x, 2 * x + 1):
            for odd in (0, 1):
                part = f_ref[plane, pl.ds(odd, MY, stride=2), :]
                total = part if total is None else total + part
        planes.append(total)
    row, column = lax.broadcasted_iota(jnp.int32, (BZ, 128), 0), lanes((BZ, 128))
    pairs = jnp.where((row >> 1) == column, 1.0 / 8.0, jnp.where((row >> 2) == column - 64, 1.0 / 64.0, 0.0))
    half_ref[...] = exact(jnp.concatenate(planes, axis=0), pairs)
    lane = lanes((8, 128))
    coarse = jnp.zeros((8, 128), F32)
    for x in range(4):
        part = None
        for row in (2 * x * MY, 2 * x * MY + 1, (2 * x + 1) * MY, (2 * x + 1) * MY + 1):
            piece = half_ref[pl.ds(row, 8, stride=2), :]
            part = piece if part is None else part + piece
        coarse = jnp.where((lane >> 5) == x, roll(part, x * 32 - 64), coarse)
    for target in range(GX):
        many_ref[target] = coarse
    send = pltpu.make_async_copy(many_ref, coarse_ref, sems.at[PIECES])
    send.start()

    slot = lanes((BY, 128)) >> 3
    for group in range(2):
        rising = jnp.zeros((BY, 128), F32)
        falling = jnp.zeros((BY, 128), F32)
        for x in range(8):
            plane = f_ref[group * 8 + x]
            rising = jnp.where(slot == 2 * x, roll(plane, x * 16 - 120), rising)
            falling = jnp.where(slot == 2 * x + 1, roll(plane, x * 16 + 8), falling)
        up_ref[group * BY : (group + 1) * BY, :] = rising
        down_ref[group * BY : (group + 1) * BY, :] = falling
    slot = lanes((MY, 128)) >> 3
    rising = jnp.zeros((MY, 128), F32)
    falling = jnp.zeros((MY, 128), F32)
    middle = []
    for x in range(MX):
        plane = half_ref[x * MY : (x + 1) * MY, :]
        middle.append(plane)
        rising = jnp.where(slot == 2 * x, roll(plane, x * 16 - 56), rising)
        falling = jnp.where(slot == 2 * x + 1, roll(plane, x * 16 + 8), falling)
    up_ref[2 * BY : 2 * BY + MY, :] = rising
    down_ref[2 * BY : 2 * BY + MY, :] = falling
    for x in range(4):
        mid_ref[x] = jnp.where(slot < 8, middle[x], roll(middle[x + 4], 64))
    for fetch in fetches[4:]:
        fetch.wait()
    send.wait()


def modes_kernel(columns_ref, cas_y_ref, own_y_ref, cas_z_ref, own_z_ref, along_ref, out_ref, modes_ref):
    me = lax.axis_index("gx")
    rows = jnp.concatenate([columns_ref[lax.rem(me + block, GX)] for block in range(GX)], axis=0)
    lane = lanes((GX * 8, 128)) >> 5
    high, low = halves(jnp.concatenate([jnp.where(lane == x, rows, 0.0) for x in range(4)], axis=0))
    own_z = own_z_ref.at[lax.axis_index("gz")]
    by_z = dot(high, own_z[0]) + dot(low, own_z[0]) + dot(high, own_z[1])
    ordered = [by_z[(x * GX + block) * 8 : (x * GX + block + 1) * 8] for block in range(GX) for x in range(4)]
    own_y = own_y_ref[lax.axis_index("gy")]
    for first in range(0, CX, 16):
        data = jnp.concatenate(ordered[first : first + 16], axis=1)
        high = data.astype(BF16).astype(F32)
        stacked = jnp.concatenate([high, data - high, high, jnp.zeros_like(high)], axis=0).astype(BF16)
        modes_ref[:, first * 128 : (first + 16) * 128] = dot(own_y, stacked)

    outs = [[] for _ in range(4)]
    for start in range(0, CY, 8):
        rows = slice(start, start + 8)
        total = [None] * 4
        table = [along_ref[shift, rows, :] for shift in (0, 1, 2, 3)]
        for place in range(CX):
            if place:
                table = [along_ref[min(place, CX - place), rows, :]] + table[:3]
            value = modes_ref[rows, place * 128 : (place + 1) * 128]
            for x in range(4):
                part = table[x] * value
                total[x] = part if total[x] is None else total[x] + part
        for x in range(4):
            outs[x].append(total[x])
    high, low = halves(jnp.concatenate([tile for x in range(4) for tile in outs[x]], axis=0))
    back_z = dot(high, cas_z_ref[0]) + dot(low, cas_z_ref[0]) + dot(high, cas_z_ref[1])
    high, low = halves(jnp.concatenate([back_z[x * CY : (x + 1) * CY] for x in range(4)], axis=1))
    back_y = dot(cas_y_ref[...], jnp.concatenate([high, low, high], axis=0))
    lane = lanes((CY, 128)) >> 5
    for gz in range(GZ):
        result = jnp.zeros((CY, 128), F32)
        for x in range(4):
            result = jnp.where(lane == x, roll(back_y[:, x * 128 : (x + 1) * 128], (x - gz) * 32), result)
        for gy in range(GY):
            out_ref[gy * GZ + gz] = result[gy * 8 : gy * 8 + 8]


def y_message_kernel(f_ref, mid_ref, zlow_ref, zhigh_ref, halo_ref, up_ref, down_ref):
    halo = zlow_ref[...] + zhigh_ref[...]
    halo_ref[...] = halo
    for ref, fine, middle in ((up_ref, BY - 8, MY - 8), (down_ref, 0, 0)):
        for x in range(BX):
            ref[x * 8 : x * 8 + 8, :] = f_ref[x, fine : fine + 8, :]
        for group in range(2):
            ref[128 + group * 8 : 136 + group * 8, :] = halo[group * BY + fine : group * BY + fine + 8]
        for x in range(4):
            ref[144 + x * 8 : 152 + x * 8, :] = mid_ref[x, middle : middle + 8, :]
        ref[176:184, :] = halo[2 * BY + middle : 2 * BY + middle + 8]


def own_extended(f_ref, mid_ref, halo_ref, low_ref, high_ref):
    def joined(row, inner):
        return jnp.concatenate([low_ref[row : row + 8, :], inner, high_ref[row : row + 8, :]], axis=0)

    planes = [lambda x=x: joined(x * 8, f_ref[x]) for x in range(BX)]
    sides = [lambda g=g: joined(128 + g * 8, halo_ref[g * BY : (g + 1) * BY, :]) for g in range(2)]
    middle = [lambda x=x: joined(144 + x * 8, mid_ref[x]) for x in range(4)]
    edge = lambda: joined(176, halo_ref[2 * BY : 2 * BY + MY, :])
    return planes, sides, middle, edge


def x_message_kernel(f_ref, mid_ref, halo_ref, low_ref, high_ref, up_ref, down_ref):
    planes, sides, middle, edge = own_extended(f_ref, mid_ref, halo_ref, low_ref, high_ref)
    for ref, first, group in ((up_ref, 8, 1), (down_ref, 0, 0)):
        for x in range(8):
            ref[x * EY : (x + 1) * EY, :] = planes[first + x]()
        ref[8 * EY : 9 * EY, :] = sides[group]()
        for x in range(4):
            ref[9 * EY + x * EMY : 9 * EY + (x + 1) * EMY, :] = middle[x]()
        ref[9 * EY + 4 * EMY : 9 * EY + 5 * EMY, :] = edge()


def filter_yz(planes, sides, gy, gzh_ref, gzl_ref, out_ref, places):
    for group in range(2):
        data = jnp.concatenate([planes[group * 8 + x]() for x in range(8)] + [sides[group]()], axis=1)
        high, low = halves(data)
        by_y = dot(gy, jnp.concatenate([high, low, high], axis=0))
        slot = lanes((BY, 128)) >> 4
        for term in range(TERMS):
            rows = by_y[term * BY : (term + 1) * BY, :]
            side = rows[:, 8 * 128 :]
            left = jnp.concatenate([rows[:, x * 128 : (x + 1) * 128] for x in range(8)], axis=0)
            right = jnp.concatenate([jnp.where(slot == x, side, 0.0) for x in range(8)], axis=0)
            high, low = halves(jnp.concatenate([left, right], axis=1))
            gzh = gzh_ref[term]
            result = dot(high, gzh) + dot(low, gzh) + dot(high, gzl_ref[term])
            for x in range(8):
                out_ref[term, places[group * 8 + x]] = result[x * BY : (x + 1) * BY]


def filter_middle(middle, edge, my, mzh_ref, mzl_ref, out_ref, place):
    slot = lanes((EMY, 128)) >> 3
    rim = edge()
    planes = []
    for x in range(MX):
        plane = middle[x]() if x < 4 else roll(middle[x - 4](), 64)
        rolled = roll(rim, 64 - 16 * x)
        planes.append(jnp.where(slot < 8, plane, jnp.where(slot < 10, rolled, 0.0)))
    high, low = halves(jnp.concatenate(planes, axis=1))
    by_y = dot(my, jnp.concatenate([high, low, high], axis=0))
    for term in range(TERMS):
        rows = by_y[term * MY : (term + 1) * MY, :]
        left = jnp.concatenate([rows[:, x * 128 : (x + 1) * 128] for x in range(MX)], axis=0)
        high, low = halves(left)
        mzh = mzh_ref[term]
        result = dot(high, mzh) + dot(low, mzh) + dot(high, mzl_ref[term])
        for x in range(MX):
            out_ref[term, place + x] = result[x * MY : (x + 1) * MY]


def tap_rows(cx_ref):
    return lambda row: jnp.broadcast_to(cx_ref[row : row + 1, :], (8, 128))


def along_x(acc, tap_at, level, places, load):
    for term in range(TERMS):
        for index, place in places:
            value = load(term, index)
            for x in range(len(acc)):
                if abs(place - x) <= RADIUS:
                    part = tap_at((level * TERMS + term) * TAPS + abs(place - x)) * value
                    acc[x] = part if acc[x] is None else acc[x] + part
    return acc


def own_kernel(
    f_ref, mid_ref, halo_ref, low_ref, high_ref, gy_ref, gzh_ref, gzl_ref, my_ref, mzh_ref, mzl_ref, cx_ref,
    fine_ref, middle_ref, planes_ref, small_ref,
):
    planes, sides, middle, edge = own_extended(f_ref, mid_ref, halo_ref, low_ref, high_ref)
    filter_yz(planes, sides, gy_ref[...], gzh_ref, gzl_ref, planes_ref, list(range(BX)))
    filter_middle(middle, edge, my_ref[...], mzh_ref, mzl_ref, small_ref, 0)
    tap_at = tap_rows(cx_ref)
    for tile in range(MY // 8):
        sl = slice(tile * 8, tile * 8 + 8)
        places = [(x, x) for x in range(MX)]
        acc = along_x([None] * MX, tap_at, 1, places, lambda term, i, sl=sl: small_ref[term, i, sl, :])
        for x in range(MX):
            middle_ref[x, sl, :] = acc[x]

    def tile_step(tile, carry):
        sl = pl.ds(pl.multiple_of(tile * 8, 8), 8)
        places = [(x, x) for x in range(BX)]
        acc = along_x([None] * BX, tap_at, 0, places, lambda term, i: planes_ref[term, i, sl, :])
        for x in range(BX):
            fine_ref[x, sl, :] = acc[x]
        return carry

    lax.fori_loop(0, BY // 8, tile_step, 0)


def near_kernel(
    low_ref, high_ref, fine_ref, middle_ref, gy_ref, gzh_ref, gzl_ref, my_ref, mzh_ref, mzl_ref, cx_ref,
    out_ref, ring_ref, small_ref, add_ref,
):
    planes, sides = [], []
    for ref in (low_ref, high_ref):
        planes += [lambda ref=ref, x=x: ref[x * EY : (x + 1) * EY, :] for x in range(8)]
        sides.append(lambda ref=ref: ref[8 * EY : 9 * EY, :])
    filter_yz(planes, sides, gy_ref[...], gzh_ref, gzl_ref, ring_ref, list(range(16)))
    for index, ref in enumerate((low_ref, high_ref)):
        middle = [lambda ref=ref, x=x: ref[9 * EY + x * EMY : 9 * EY + (x + 1) * EMY, :] for x in range(4)]
        edge = lambda ref=ref: ref[9 * EY + 4 * EMY : 9 * EY + 5 * EMY, :]
        filter_middle(middle, edge, my_ref[...], mzh_ref, mzl_ref, small_ref, index * MX)

    tap_at = tap_rows(cx_ref)
    for tile in range(MY // 8):
        sl = slice(tile * 8, tile * 8 + 8)
        acc = [middle_ref[x, sl, :] for x in range(MX)]
        places = [(i, i - MX if i < MX else i) for i in range(2 * MX)]
        acc = along_x(acc, tap_at, 1, places, lambda term, i, sl=sl: small_ref[term, i, sl, :])
        for x in range(MX):
            add_ref[x, pl.ds(tile * 16, 8, stride=2), :] = acc[x]
            add_ref[x, pl.ds(tile * 16 + 1, 8, stride=2), :] = acc[x]

    def tile_step(tile, carry):
        sl = pl.ds(pl.multiple_of(tile * 8, 8), 8)
        acc = [fine_ref[x, sl, :] + add_ref[x // 2, sl, :] for x in range(BX)]
        places = [(i, i - 8 if i < 8 else i + 8) for i in range(16)]
        acc = along_x(acc, tap_at, 0, places, lambda term, i: ring_ref[term, i, sl, :])
        for x in range(BX):
            out_ref[x, sl, :] = acc[x]
        return carry

    lax.fori_loop(0, BY // 8, tile_step, 0)


def add_kernel(near_ref, top_ref, out_ref, wide_ref, sum_ref, sems):
    top = top_ref[0]
    for source in range(1, GY * GZ):
        top = top + top_ref[source]
    shape = (BZ, 4 * BZ)
    row, column = lax.broadcasted_iota(jnp.int32, shape, 0), lanes(shape)
    spread = jnp.where(row == (column >> 7) * 32 + ((column & 127) >> 2), 1.0, 0.0).astype(BF16)
    high, rest = halves(top)
    rest = top - high.astype(F32)
    mid, low = halves(rest)
    parts = dot(jnp.concatenate([high.astype(F32), mid.astype(F32), low.astype(F32)], axis=0).astype(BF16), spread)
    wide = parts[0:8] + parts[8:16] + parts[16:24]
    for row in range(4):
        wide_ref[pl.ds(row, 8, stride=4), :] = wide[:, :128]
        wide_ref[pl.ds(BY + row, 8, stride=4), :] = wide[:, 128:256]
        wide_ref[pl.ds(2 * BY + row, 8, stride=4), :] = wide[:, 256:384]
        wide_ref[pl.ds(3 * BY + row, 8, stride=4), :] = wide[:, 384:512]
    sends = []
    for block in range(4):
        for x in range(4 * block, 4 * block + 4):
            sum_ref[x] = near_ref[x] + wide_ref[block * BY : (block + 1) * BY, :]
        place = pl.ds(4 * block, 4)
        sends.append(pltpu.make_async_copy(sum_ref.at[place], out_ref.at[place], sems.at[block]))
        sends[-1].start()
    for send in sends:
        send.wait()


def call(kernel, outs, args, scratch=(), flops=0, hbm=0, written=0, limit=4):
    vmem = pl.BlockSpec(memory_space=pltpu.VMEM)
    near = len(args) - hbm
    specs = [vmem] * near + [pl.BlockSpec(memory_space=pltpu.HBM)] * hbm
    args = args[:near] + [pltpu.with_memory_space_constraint(a, pltpu.HBM) for a in args[near:]]
    size = sum(a.size * a.dtype.itemsize for a in args)
    return pl.pallas_call(
        kernel,
        out_shape=[jax.ShapeDtypeStruct(shape, dtype) for shape, dtype in outs],
        in_specs=specs,
        out_specs=[pl.BlockSpec(memory_space=pl.ANY)] * written + [vmem] * (len(outs) - written),
        scratch_shapes=list(scratch),
        cost_estimate=pl.CostEstimate(flops=flops, bytes_accessed=size, transcendentals=0),
        compiler_params=pltpu.CompilerParams(vmem_limit_bytes=limit * 1024 * 1024),
    )(*args)


def ring(value, axis, step):
    count = lax.axis_size(axis)
    return lax.ppermute(value, axis, [(i, (i + step) % count) for i in range(count)])


def exchange(value, axis):
    return lax.all_to_all(value, axis, 0, 0, tiled=True)


def potential(charges, term_width, term_weight):
    sources = [charges, term_width, term_weight] + constant_tables()
    coarse, mid, z_up, z_down, charges, term_width, term_weight, *tables = call(
        restrict_kernel,
        [((GX, 8, 128), F32), ((4, MY, 128), F32), ((ZROWS, 128), F32), ((ZROWS, 128), F32)]
        + [(a.shape, a.dtype) for a in sources],
        sources,
        [
            pltpu.VMEM((MX * MY, 128), F32),
            pltpu.VMEM((GX, 8, 128), F32),
            pltpu.SemaphoreType.DMA((PIECES + 1,)),
        ],
        flops=10**7,
        hbm=FETCHED,
        written=1,
    )
    columns = exchange(coarse, "gx")
    z_low, z_high = ring(z_up, "gz", 1), ring(z_down, "gz", -1)
    gy, gzh, gzl, my, mzh, mzl, cx = call(
        weights_kernel,
        [
            ((TERMS * BY, 3 * EY), BF16),
            ((TERMS, 256, 128), BF16),
            ((TERMS, 256, 128), BF16),
            ((TERMS * MY, 3 * EMY), BF16),
            ((TERMS, 128, 128), BF16),
            ((TERMS, 128, 128), BF16),
            ((2 * TERMS * TAPS, 128), F32),
        ],
        [term_width, term_weight],
        flops=10**7,
    )
    bands = [gy, gzh, gzl, my, mzh, mzl]
    halo, y_up, y_down = call(
        y_message_kernel,
        [((ZROWS, 128), F32), ((YROWS, 128), F32), ((YROWS, 128), F32)],
        [charges, mid, z_low, z_high],
        flops=10**6,
    )
    low, high = ring(y_up, "gy", 1), ring(y_down, "gy", -1)
    (partial,) = call(
        modes_kernel,
        [((GY * GZ, 8, 128), F32)],
        [columns] + tables,
        [pltpu.VMEM((CY, CX * 128), F32)],
        flops=5 * 10**7,
        limit=8,
    )
    top = exchange(partial, ("gy", "gz"))
    x_up, x_down = call(
        x_message_kernel, [((XROWS, 128), F32), ((XROWS, 128), F32)], [charges, mid, halo, low, high], flops=10**6
    )
    x_low, x_high = ring(x_up, "gx", 1), ring(x_down, "gx", -1)
    fine, middle = call(
        own_kernel,
        [((BX, BY, BZ), F32), ((MX, MY, 128), F32)],
        [charges, mid, halo, low, high] + bands + [cx],
        [pltpu.VMEM((TERMS, BX, BY, 128), F32), pltpu.VMEM((TERMS, MX, MY, 128), F32)],
        flops=10**8,
        limit=10,
    )
    (near,) = call(
        near_kernel,
        [((BX, BY, BZ), F32)],
        [x_low, x_high, fine, middle] + bands + [cx],
        [
            pltpu.VMEM((TERMS, 16, BY, 128), F32),
            pltpu.VMEM((TERMS, 16, MY, 128), F32),
            pltpu.VMEM((MX, BY, 128), F32),
        ],
        flops=10**8,
        limit=10,
    )
    (result,) = call(
        add_kernel,
        [((BX, BY, BZ), F32)],
        [near, top],
        [pltpu.VMEM((4 * BY, 128), F32), pltpu.VMEM((BX, BY, BZ), F32), pltpu.SemaphoreType.DMA((4,))],
        flops=10**6,
        written=1,
    )
    return result


def solution(mesh):
    placed = (P("gx", "gy", "gz"), P(), P())
    return jax.shard_map(potential, mesh=mesh, in_specs=placed, out_specs=P("gx", "gy", "gz"), check_vma=False)
```

```python
import math

import jax
import jax.numpy as jnp
import numpy as np
from jax import lax
from jax.experimental import pallas as pl
from jax.experimental.pallas import tpu as pltpu
from jax.sharding import PartitionSpec as P


TERMS = 4
RADIUS = 8
TAPS = RADIUS + 1

HIGHEST = lax.Precision.HIGHEST
F32 = jnp.float32
BF16 = jnp.bfloat16
screening = 0.01
strength = 4.0

BX, BY, BZ = 16, 32, 128
MX, MY, MZ = 8, 16, 64
CX, CY, CZ = 64, 64, 128
EY, EMY = BY + 2 * RADIUS, MY + 2 * RADIUS
GX, GY, GZ = 16, 8, 4
FETCHED, PIECES = 8, 14
ZROWS = 2 * BY + MY
YROWS = BX * 8 + 2 * 8 + 5 * 8
XROWS = 8 * EY + EY + 5 * EMY


def cas_table(count):
    modes = np.arange(count)
    angles = 2.0 * math.pi / count * (np.outer(modes, modes) % count)
    return np.cos(angles) + np.sin(angles)


def constant_tables():
    cas_y, cas_z = cas_table(CY), cas_table(CZ)

    def lam(count):
        return 2.0 - 2.0 * np.cos(2.0 * math.pi / count * np.arange(count))

    total = lam(CX)[:, None, None] + lam(CY)[None, :, None] + lam(CZ)[None, None, :]
    mult = strength * np.exp(-total) / (total + screening)
    mult[0, 0, 0] = 0.0
    shifts = np.arange(CX // 2 + 1)
    cosine = np.cos(2.0 * math.pi / CX * (np.outer(shifts, np.arange(CX)) % CX))
    along_x = np.einsum("dm,myz->dyz", cosine, mult) / (CX * CY * CZ)
    own_z = np.stack([np.tile(cas_z[32 * g : 32 * g + 32], (4, 1)) for g in range(GZ)])
    own_y = np.stack([cas_y[:, 8 * g : 8 * g + 8] for g in range(GY)])

    def split(table):
        table = np.asarray(table, np.float32)
        high = table.astype(BF16)
        return high, (table - high.astype(np.float32)).astype(BF16)

    high, low = split(cas_y)
    own_high, own_low = split(own_y)
    tables = [
        np.concatenate([high, high, low], axis=1),
        np.concatenate([own_high, own_high, own_low, np.zeros_like(own_low)], axis=2),
        np.stack(split(cas_z)),
        np.stack(split(own_z), axis=1),
        np.asarray(along_x, np.float32),
    ]
    return [jnp.asarray(table) for table in tables]


def lanes(shape):
    return lax.broadcasted_iota(jnp.int32, shape, len(shape) - 1)


def roll(value, shift):
    shift %= 128
    return pltpu.roll(value, shift, 1) if shift else value


def dot(a, b):
    return jnp.dot(a, b, preferred_element_type=F32)


def exact(a, b):
    return jnp.dot(a, b, preferred_element_type=F32, precision=HIGHEST)


def halves(value):
    high = value.astype(BF16)
    return high, (value - high.astype(F32)).astype(BF16)


def weights_kernel(width_ref, weight_ref, gy_ref, gzh_ref, gzl_ref, my_ref, mzh_ref, mzl_ref, cx_ref):
    offset = lanes((8, 128)) - RADIUS
    squares = (offset * offset).astype(F32)

    def scale(level, term):
        width = jnp.broadcast_to(width_ref[level : level + 1, term : term + 1], (8, 128))
        inverse = -1.0 / (2.0 * width * width)
        values = jnp.where(offset <= RADIUS, jnp.exp(squares * inverse), 0.0)
        norm = 1.0 / jnp.broadcast_to(jnp.sum(values, axis=1, keepdims=True), (8, 128))
        weight = jnp.broadcast_to(weight_ref[level : level + 1, term : term + 1], (8, 128))
        for distance in range(TAPS):
            value = jnp.exp(float(distance * distance) * inverse) * norm * weight
            row = (level * TERMS + term) * TAPS + distance
            cx_ref[row : row + 1, :] = value[0:1, :]
        return inverse, norm

    def taps(place, inverse, norm):
        rows, columns = place.shape
        inverse, norm = [
            jnp.concatenate([jnp.concatenate([v] * (columns // 128), axis=1)] * (rows // 8), axis=0) for v in (inverse, norm)
        ]
        values = jnp.exp((place * place).astype(F32) * inverse) * norm
        return jnp.where(jnp.abs(place) <= RADIUS, values, 0.0)

    def along_y(ref, term, inverse, norm, out, ext):
        shape = (out, 256 if 3 * ext > 128 else 128)
        column = lanes(shape)
        row = lax.broadcasted_iota(jnp.int32, shape, 0)
        part = (column >= ext).astype(jnp.int32) + (column >= 2 * ext).astype(jnp.int32)
        high, low = halves(taps(column - part * ext - RADIUS - row, inverse, norm))
        both = jnp.where(part < 2, high.astype(F32), low.astype(F32))
        ref[term * out : (term + 1) * out, :] = both[:, : 3 * ext].astype(BF16)

    for term in range(TERMS):
        inverse, norm = scale(0, term)
        along_y(gy_ref, term, inverse, norm, BY, EY)
        shape = (256, 128)
        row = lax.broadcasted_iota(jnp.int32, shape, 0)
        slot = row & 15
        place = jnp.where(row < BZ, row, jnp.where(slot < 8, slot - 8, BZ - 8 + slot))
        high, low = halves(taps(place - lanes(shape), inverse, norm))
        gzh_ref[term] = high
        gzl_ref[term] = low

        inverse, norm = scale(1, term)
        along_y(my_ref, term, inverse, norm, MY, EMY)
        shape = (128, 128)
        row = lax.broadcasted_iota(jnp.int32, shape, 0)
        place = jnp.where(row < MZ, row, jnp.where(row < MZ + 8, row - MZ - 8, row - 8))
        values = taps(place - (lanes(shape) >> 1), inverse, norm)
        high, low = halves(jnp.where(row < MZ + 16, values, 0.0))
        mzh_ref[term] = high
        mzl_ref[term] = low


def restrict_kernel(*refs):
    sources, (coarse_ref, mid_ref, up_ref, down_ref), copies = refs[:FETCHED], refs[FETCHED : FETCHED + 4], refs[FETCHED + 4 :]
    copies, half_ref, many_ref, sems = copies[:FETCHED], *copies[FETCHED:]
    pieces = [(0, x, 4) for x in range(0, BX, 4)] + [(i, 0, None) for i in range(1, FETCHED - 1)]
    pieces += [(FETCHED - 1, x, min(x + 9, CX // 2 + 1) - x) for x in range(0, CX // 2 + 1, 9)]
    fetches = []
    for count, (i, first, size) in enumerate(pieces):
        source, copy = sources[i], copies[i]
        if size:
            source, copy = source.at[pl.ds(first, size)], copy.at[pl.ds(first, size)]
        fetches.append(pltpu.make_async_copy(source, copy, sems.at[count]))
        fetches[-1].start()
    f_ref = copies[0]
    planes = []
    for x in range(MX):
        if x % 2 == 0:
            fetches[x // 2].wait()
        total = None
        for plane in (2 * x, 2 * x + 1):
            for odd in (0, 1):
                part = f_ref[plane, pl.ds(odd, MY, stride=2), :]
                total = part if total is None else total + part
        planes.append(total)
    row, column = lax.broadcasted_iota(jnp.int32, (BZ, 128), 0), lanes((BZ, 128))
    pairs = jnp.where((row >> 1) == column, 1.0 / 8.0, jnp.where((row >> 2) == column - 64, 1.0 / 64.0, 0.0))
    half_ref[...] = exact(jnp.concatenate(planes, axis=0), pairs)
    lane = lanes((8, 128))
    coarse = jnp.zeros((8, 128), F32)
    for x in range(4):
        part = None
        for row in (2 * x * MY, 2 * x * MY + 1, (2 * x + 1) * MY, (2 * x + 1) * MY + 1):
            piece = half_ref[pl.ds(row, 8, stride=2), :]
            part = piece if part is None else part + piece
        coarse = jnp.where((lane >> 5) == x, roll(part, x * 32 - 64), coarse)
    for target in range(GX):
        many_ref[target] = coarse
    send = pltpu.make_async_copy(many_ref, coarse_ref, sems.at[PIECES])
    send.start()

    slot = lanes((BY, 128)) >> 3
    for group in range(2):
        rising = jnp.zeros((BY, 128), F32)
        falling = jnp.zeros((BY, 128), F32)
        for x in range(8):
            plane = f_ref[group * 8 + x]
            rising = jnp.where(slot == 2 * x, roll(plane, x * 16 - 120), rising)
            falling = jnp.where(slot == 2 * x + 1, roll(plane, x * 16 + 8), falling)
        up_ref[group * BY : (group + 1) * BY, :] = rising
        down_ref[group * BY : (group + 1) * BY, :] = falling
    slot = lanes((MY, 128)) >> 3
    rising = jnp.zeros((MY, 128), F32)
    falling = jnp.zeros((MY, 128), F32)
    middle = []
    for x in range(MX):
        plane = half_ref[x * MY : (x + 1) * MY, :]
        middle.append(plane)
        rising = jnp.where(slot == 2 * x, roll(plane, x * 16 - 56), rising)
        falling = jnp.where(slot == 2 * x + 1, roll(plane, x * 16 + 8), falling)
    up_ref[2 * BY : 2 * BY + MY, :] = rising
    down_ref[2 * BY : 2 * BY + MY, :] = falling
    for x in range(4):
        mid_ref[x] = jnp.where(slot < 8, middle[x], roll(middle[x + 4], 64))
    for fetch in fetches[4:]:
        fetch.wait()
    send.wait()


def modes_kernel(columns_ref, cas_y_ref, own_y_ref, cas_z_ref, own_z_ref, along_ref, out_ref, modes_ref):
    me = lax.axis_index("gx")
    rows = jnp.concatenate([columns_ref[lax.rem(me + block, GX)] for block in range(GX)], axis=0)
    lane = lanes((GX * 8, 128)) >> 5
    high, low = halves(jnp.concatenate([jnp.where(lane == x, rows, 0.0) for x in range(4)], axis=0))
    own_z = own_z_ref.at[lax.axis_index("gz")]
    by_z = dot(high, own_z[0]) + dot(low, own_z[0]) + dot(high, own_z[1])
    ordered = [by_z[(x * GX + block) * 8 : (x * GX + block + 1) * 8] for block in range(GX) for x in range(4)]
    own_y = own_y_ref[lax.axis_index("gy")]
    for first in range(0, CX, 16):
        data = jnp.concatenate(ordered[first : first + 16], axis=1)
        high = data.astype(BF16).astype(F32)
        stacked = jnp.concatenate([high, data - high, high, jnp.zeros_like(high)], axis=0).astype(BF16)
        modes_ref[:, first * 128 : (first + 16) * 128] = dot(own_y, stacked)

    outs = [[] for _ in range(4)]
    for start in range(0, CY, 8):
        rows = slice(start, start + 8)
        total = [None] * 4
        table = [along_ref[shift, rows, :] for shift in (0, 1, 2, 3)]
        for place in range(CX):
            if place:
                table = [along_ref[min(place, CX - place), rows, :]] + table[:3]
            value = modes_ref[rows, place * 128 : (place + 1) * 128]
            for x in range(4):
                part = table[x] * value
                total[x] = part if total[x] is None else total[x] + part
        for x in range(4):
            outs[x].append(total[x])
    high, low = halves(jnp.concatenate([tile for x in range(4) for tile in outs[x]], axis=0))
    back_z = dot(high, cas_z_ref[0]) + dot(low, cas_z_ref[0]) + dot(high, cas_z_ref[1])
    high, low = halves(jnp.concatenate([back_z[x * CY : (x + 1) * CY] for x in range(4)], axis=1))
    back_y = dot(cas_y_ref[...], jnp.concatenate([high, low, high], axis=0))
    lane = lanes((CY, 128)) >> 5
    for gz in range(GZ):
        result = jnp.zeros((CY, 128), F32)
        for x in range(4):
            result = jnp.where(lane == x, roll(back_y[:, x * 128 : (x + 1) * 128], (x - gz) * 32), result)
        for gy in range(GY):
            out_ref[gy * GZ + gz] = result[gy * 8 : gy * 8 + 8]


def y_message_kernel(f_ref, mid_ref, zlow_ref, zhigh_ref, halo_ref, up_ref, down_ref):
    halo = zlow_ref[...] + zhigh_ref[...]
    halo_ref[...] = halo
    for ref, fine, middle in ((up_ref, BY - 8, MY - 8), (down_ref, 0, 0)):
        for x in range(BX):
            ref[x * 8 : x * 8 + 8, :] = f_ref[x, fine : fine + 8, :]
        for group in range(2):
            ref[128 + group * 8 : 136 + group * 8, :] = halo[group * BY + fine : group * BY + fine + 8]
        for x in range(4):
            ref[144 + x * 8 : 152 + x * 8, :] = mid_ref[x, middle : middle + 8, :]
        ref[176:184, :] = halo[2 * BY + middle : 2 * BY + middle + 8]


def own_extended(f_ref, mid_ref, halo_ref, low_ref, high_ref):
    def joined(row, inner):
        return jnp.concatenate([low_ref[row : row + 8, :], inner, high_ref[row : row + 8, :]], axis=0)

    planes = [lambda x=x: joined(x * 8, f_ref[x]) for x in range(BX)]
    sides = [lambda g=g: joined(128 + g * 8, halo_ref[g * BY : (g + 1) * BY, :]) for g in range(2)]
    middle = [lambda x=x: joined(144 + x * 8, mid_ref[x]) for x in range(4)]
    edge = lambda: joined(176, halo_ref[2 * BY : 2 * BY + MY, :])
    return planes, sides, middle, edge


def x_message_kernel(f_ref, mid_ref, halo_ref, low_ref, high_ref, up_ref, down_ref):
    planes, sides, middle, edge = own_extended(f_ref, mid_ref, halo_ref, low_ref, high_ref)
    for ref, first, group in ((up_ref, 8, 1), (down_ref, 0, 0)):
        for x in range(8):
            ref[x * EY : (x + 1) * EY, :] = planes[first + x]()
        ref[8 * EY : 9 * EY, :] = sides[group]()
        for x in range(4):
            ref[9 * EY + x * EMY : 9 * EY + (x + 1) * EMY, :] = middle[x]()
        ref[9 * EY + 4 * EMY : 9 * EY + 5 * EMY, :] = edge()


def filter_yz(planes, sides, gy, gzh_ref, gzl_ref, out_ref, places):
    for group in range(len(sides)):
        data = jnp.concatenate([planes[group * 8 + x]() for x in range(8)] + [sides[group]()], axis=1)
        high, low = halves(data)
        by_y = dot(gy, jnp.concatenate([high, low, high], axis=0))
        slot = lanes((BY, 128)) >> 4
        for term in range(TERMS):
            rows = by_y[term * BY : (term + 1) * BY, :]
            side = rows[:, 8 * 128 :]
            left = jnp.concatenate([rows[:, x * 128 : (x + 1) * 128] for x in range(8)], axis=0)
            right = jnp.concatenate([jnp.where(slot == x, side, 0.0) for x in range(8)], axis=0)
            high, low = halves(jnp.concatenate([left, right], axis=1))
            gzh = gzh_ref[term]
            result = dot(high, gzh) + dot(low, gzh) + dot(high, gzl_ref[term])
            for x in range(8):
                out_ref[term, places[group * 8 + x]] = result[x * BY : (x + 1) * BY]


def filter_middle(middle, edge, my, mzh_ref, mzl_ref, out_ref, place):
    slot = lanes((EMY, 128)) >> 3
    rim = edge()
    planes = []
    for x in range(MX):
        plane = middle[x]() if x < 4 else roll(middle[x - 4](), 64)
        rolled = roll(rim, 64 - 16 * x)
        planes.append(jnp.where(slot < 8, plane, jnp.where(slot < 10, rolled, 0.0)))
    high, low = halves(jnp.concatenate(planes, axis=1))
    by_y = dot(my, jnp.concatenate([high, low, high], axis=0))
    for term in range(TERMS):
        rows = by_y[term * MY : (term + 1) * MY, :]
        left = jnp.concatenate([rows[:, x * 128 : (x + 1) * 128] for x in range(MX)], axis=0)
        high, low = halves(left)
        mzh = mzh_ref[term]
        result = dot(high, mzh) + dot(low, mzh) + dot(high, mzl_ref[term])
        for x in range(MX):
            out_ref[term, place + x] = result[x * MY : (x + 1) * MY]


def tap_rows(cx_ref):
    return lambda row: jnp.broadcast_to(cx_ref[row : row + 1, :], (8, 128))


def along_x(acc, tap_at, level, places, load):
    for term in range(TERMS):
        for index, place in places:
            value = load(term, index)
            for x in range(len(acc)):
                if abs(place - x) <= RADIUS:
                    part = tap_at((level * TERMS + term) * TAPS + abs(place - x)) * value
                    acc[x] = part if acc[x] is None else acc[x] + part
    return acc


def own_kernel(
    f_ref, mid_ref, halo_ref, low_ref, high_ref, gy_ref, gzh_ref, gzl_ref, my_ref, mzh_ref, mzl_ref, cx_ref,
    fine_ref, middle_ref, planes_ref, small_ref,
):
    planes, sides, middle, edge = own_extended(f_ref, mid_ref, halo_ref, low_ref, high_ref)
    filter_yz(planes, sides, gy_ref[...], gzh_ref, gzl_ref, planes_ref, list(range(BX)))
    filter_middle(middle, edge, my_ref[...], mzh_ref, mzl_ref, small_ref, 0)
    tap_at = tap_rows(cx_ref)
    for tile in range(MY // 8):
        sl = slice(tile * 8, tile * 8 + 8)
        places = [(x, x) for x in range(MX)]
        acc = along_x([None] * MX, tap_at, 1, places, lambda term, i, sl=sl: small_ref[term, i, sl, :])
        for x in range(MX):
            middle_ref[x, sl, :] = acc[x]

    def tile_step(tile, carry):
        sl = pl.ds(pl.multiple_of(tile * 8, 8), 8)
        places = [(x, x) for x in range(BX)]
        acc = along_x([None] * BX, tap_at, 0, places, lambda term, i: planes_ref[term, i, sl, :])
        for x in range(BX):
            fine_ref[x, sl, :] = acc[x]
        return carry

    lax.fori_loop(0, BY // 8, tile_step, 0)


def ring_planes(ref, high, gy, gzh_ref, gzl_ref, my, mzh_ref, mzl_ref, ring_ref, small_ref):
    planes = [lambda x=x: ref[x * EY : (x + 1) * EY, :] for x in range(8)]
    filter_yz(planes, [lambda: ref[8 * EY : 9 * EY, :]], gy, gzh_ref, gzl_ref, ring_ref, list(range(8)))
    middle = [lambda x=x: ref[9 * EY + x * EMY : 9 * EY + (x + 1) * EMY, :] for x in range(4)]
    edge = lambda: ref[9 * EY + 4 * EMY : 9 * EY + 5 * EMY, :]
    filter_middle(middle, edge, my, mzh_ref, mzl_ref, small_ref, 0)
    return [(i, BX + i if high else i - 8) for i in range(8)], [(i, MX + i if high else i - MX) for i in range(MX)]


def low_kernel(
    low_ref, fine_ref, middle_ref, gy_ref, gzh_ref, gzl_ref, my_ref, mzh_ref, mzl_ref, cx_ref,
    out_ref, outm_ref, ring_ref, small_ref,
):
    fine, middle = ring_planes(
        low_ref, False, gy_ref[...], gzh_ref, gzl_ref, my_ref[...], mzh_ref, mzl_ref, ring_ref, small_ref
    )
    tap_at = tap_rows(cx_ref)
    for tile in range(MY // 8):
        sl = slice(tile * 8, tile * 8 + 8)
        acc = [middle_ref[x, sl, :] for x in range(MX)]
        acc = along_x(acc, tap_at, 1, middle, lambda term, i, sl=sl: small_ref[term, i, sl, :])
        for x in range(MX):
            outm_ref[x, sl, :] = acc[x]

    def tile_step(tile, carry):
        sl = pl.ds(pl.multiple_of(tile * 8, 8), 8)
        acc = [fine_ref[x, sl, :] for x in range(BX)]
        acc = along_x(acc, tap_at, 0, fine, lambda term, i: ring_ref[term, i, sl, :])
        for x in range(BX):
            out_ref[x, sl, :] = acc[x]
        return carry

    lax.fori_loop(0, BY // 8, tile_step, 0)


def near_kernel(
    high_ref, fine_ref, middle_ref, gy_ref, gzh_ref, gzl_ref, my_ref, mzh_ref, mzl_ref, cx_ref,
    out_ref, ring_ref, small_ref, add_ref,
):
    fine, middle = ring_planes(
        high_ref, True, gy_ref[...], gzh_ref, gzl_ref, my_ref[...], mzh_ref, mzl_ref, ring_ref, small_ref
    )
    tap_at = tap_rows(cx_ref)
    for tile in range(MY // 8):
        sl = slice(tile * 8, tile * 8 + 8)
        acc = [middle_ref[x, sl, :] for x in range(MX)]
        acc = along_x(acc, tap_at, 1, middle, lambda term, i, sl=sl: small_ref[term, i, sl, :])
        for x in range(MX):
            add_ref[x, pl.ds(tile * 16, 8, stride=2), :] = acc[x]
            add_ref[x, pl.ds(tile * 16 + 1, 8, stride=2), :] = acc[x]

    def tile_step(tile, carry):
        sl = pl.ds(pl.multiple_of(tile * 8, 8), 8)
        acc = [fine_ref[x, sl, :] + add_ref[x // 2, sl, :] for x in range(BX)]
        acc = along_x(acc, tap_at, 0, fine, lambda term, i: ring_ref[term, i, sl, :])
        for x in range(BX):
            out_ref[x, sl, :] = acc[x]
        return carry

    lax.fori_loop(0, BY // 8, tile_step, 0)


def add_kernel(near_ref, top_ref, out_ref, wide_ref, sum_ref, sems):
    top = top_ref[0]
    for source in range(1, GY * GZ):
        top = top + top_ref[source]
    shape = (BZ, 4 * BZ)
    row, column = lax.broadcasted_iota(jnp.int32, shape, 0), lanes(shape)
    spread = jnp.where(row == (column >> 7) * 32 + ((column & 127) >> 2), 1.0, 0.0).astype(BF16)
    high, rest = halves(top)
    rest = top - high.astype(F32)
    mid, low = halves(rest)
    parts = dot(jnp.concatenate([high.astype(F32), mid.astype(F32), low.astype(F32)], axis=0).astype(BF16), spread)
    wide = parts[0:8] + parts[8:16] + parts[16:24]
    for row in range(4):
        wide_ref[pl.ds(row, 8, stride=4), :] = wide[:, :128]
        wide_ref[pl.ds(BY + row, 8, stride=4), :] = wide[:, 128:256]
        wide_ref[pl.ds(2 * BY + row, 8, stride=4), :] = wide[:, 256:384]
        wide_ref[pl.ds(3 * BY + row, 8, stride=4), :] = wide[:, 384:512]
    sends = []
    for block in range(4):
        for x in range(4 * block, 4 * block + 4):
            sum_ref[x] = near_ref[x] + wide_ref[block * BY : (block + 1) * BY, :]
        place = pl.ds(4 * block, 4)
        sends.append(pltpu.make_async_copy(sum_ref.at[place], out_ref.at[place], sems.at[block]))
        sends[-1].start()
    for send in sends:
        send.wait()


def call(kernel, outs, args, scratch=(), flops=0, hbm=0, written=0, limit=4):
    vmem = pl.BlockSpec(memory_space=pltpu.VMEM)
    near = len(args) - hbm
    specs = [vmem] * near + [pl.BlockSpec(memory_space=pltpu.HBM)] * hbm
    args = args[:near] + [pltpu.with_memory_space_constraint(a, pltpu.HBM) for a in args[near:]]
    size = sum(a.size * a.dtype.itemsize for a in args)
    return pl.pallas_call(
        kernel,
        out_shape=[jax.ShapeDtypeStruct(shape, dtype) for shape, dtype in outs],
        in_specs=specs,
        out_specs=[pl.BlockSpec(memory_space=pl.ANY)] * written + [vmem] * (len(outs) - written),
        scratch_shapes=list(scratch),
        cost_estimate=pl.CostEstimate(flops=flops, bytes_accessed=size, transcendentals=0),
        compiler_params=pltpu.CompilerParams(vmem_limit_bytes=limit * 1024 * 1024),
    )(*args)


def ring(value, axis, step):
    count = lax.axis_size(axis)
    return lax.ppermute(value, axis, [(i, (i + step) % count) for i in range(count)])


def exchange(value, axis):
    return lax.all_to_all(value, axis, 0, 0, tiled=True)


def potential(charges, term_width, term_weight):
    sources = [charges, term_width, term_weight] + constant_tables()
    coarse, mid, z_up, z_down, charges, term_width, term_weight, *tables = call(
        restrict_kernel,
        [((GX, 8, 128), F32), ((4, MY, 128), F32), ((ZROWS, 128), F32), ((ZROWS, 128), F32)]
        + [(a.shape, a.dtype) for a in sources],
        sources,
        [
            pltpu.VMEM((MX * MY, 128), F32),
            pltpu.VMEM((GX, 8, 128), F32),
            pltpu.SemaphoreType.DMA((PIECES + 1,)),
        ],
        flops=10**7,
        hbm=FETCHED,
        written=1,
    )
    columns = exchange(coarse, "gx")
    z_low, z_high = ring(z_up, "gz", 1), ring(z_down, "gz", -1)
    gy, gzh, gzl, my, mzh, mzl, cx = call(
        weights_kernel,
        [
            ((TERMS * BY, 3 * EY), BF16),
            ((TERMS, 256, 128), BF16),
            ((TERMS, 256, 128), BF16),
            ((TERMS * MY, 3 * EMY), BF16),
            ((TERMS, 128, 128), BF16),
            ((TERMS, 128, 128), BF16),
            ((2 * TERMS * TAPS, 128), F32),
        ],
        [term_width, term_weight],
        flops=10**7,
    )
    bands = [gy, gzh, gzl, my, mzh, mzl]
    halo, y_up, y_down = call(
        y_message_kernel,
        [((ZROWS, 128), F32), ((YROWS, 128), F32), ((YROWS, 128), F32)],
        [charges, mid, z_low, z_high],
        flops=10**6,
    )
    low, high = ring(y_up, "gy", 1), ring(y_down, "gy", -1)
    (partial,) = call(
        modes_kernel,
        [((GY * GZ, 8, 128), F32)],
        [columns] + tables,
        [pltpu.VMEM((CY, CX * 128), F32)],
        flops=5 * 10**7,
        limit=8,
    )
    top = exchange(partial, ("gy", "gz"))
    x_up, x_down = call(
        x_message_kernel, [((XROWS, 128), F32), ((XROWS, 128), F32)], [charges, mid, halo, low, high], flops=10**6
    )
    x_low, x_high = ring(x_up, "gx", 1), ring(x_down, "gx", -1)
    fine, middle = call(
        own_kernel,
        [((BX, BY, BZ), F32), ((MX, MY, 128), F32)],
        [charges, mid, halo, low, high] + bands + [cx],
        [pltpu.VMEM((TERMS, BX, BY, 128), F32), pltpu.VMEM((TERMS, MX, MY, 128), F32)],
        flops=10**8,
        limit=10,
    )
    scratch = [pltpu.VMEM((TERMS, 8, BY, 128), F32), pltpu.VMEM((TERMS, MX, MY, 128), F32)]
    fine, middle = call(
        low_kernel,
        [((BX, BY, BZ), F32), ((MX, MY, 128), F32)],
        [x_low, fine, middle] + bands + [cx],
        scratch,
        flops=10**8,
        limit=8,
    )
    (near,) = call(
        near_kernel,
        [((BX, BY, BZ), F32)],
        [x_high, fine, middle] + bands + [cx],
        scratch + [pltpu.VMEM((MX, BY, 128), F32)],
        flops=10**8,
        limit=8,
    )
    (result,) = call(
        add_kernel,
        [((BX, BY, BZ), F32)],
        [near, top],
        [pltpu.VMEM((4 * BY, 128), F32), pltpu.VMEM((BX, BY, BZ), F32), pltpu.SemaphoreType.DMA((4,))],
        flops=10**6,
        written=1,
    )
    return result


def solution(mesh):
    placed = (P("gx", "gy", "gz"), P(), P())
    return jax.shard_map(potential, mesh=mesh, in_specs=placed, out_specs=P("gx", "gy", "gz"), check_vma=False)
```
